128 devices in a mesh: leaf: 32 (over z, y, core), front: 4 (over x).
Axes of the slice: x: 4, y: 4, z: 4, core: 2. Of those that a mesh axis runs over, the one named last changes fastest.
Arguments:
- right_side: float32 [32, 4, 96, 512], P('leaf', 'front'), may hold values from -6 to 6
- factor_inverse: float32 [32, 4, 128, 7680], P('leaf', 'front'), may hold values from -1 to 1, as said below
- update_panel: float32 [32, 4, 128, 1792], P('leaf', 'front'), may hold values from -0.09375 to 0.09375
- update_targets: int32 [32, 14], P('leaf'), may hold values from 0 to 31, as said below
- pivot_pairs: int32 [32, 4, 256], P('leaf', 'front'), may hold values 0 or 1
- pivot_diagonal: float32 [32, 4, 512], P('leaf', 'front'), may hold values from 0.5 to 2
- pivot_coupling: float32 [32, 4, 256], P('leaf', 'front'), may hold values from 3 to 5
Outputs:
- solution: float32 [32, 4, 96, 512], P('leaf', 'front')
The draws below stay inside these ranges and needn't reach their ends.
Inputs may be any that keep to these rules, and one draw needn't show every extreme that they name: `factor_inverse`: each front's inverse factor is lower triangular in the front's row order with ones on its diagonal. `update_targets`: each front's list names distinct blocks of its parent's pivot rows in rising order, and is repeated in the row of every leaf index of the front's group.
All inputs are finite; a program needn't handle non-finite values. No bound on the sum of `pivot_pairs` on one device may be relied on, other than what follows from the above.
Results may differ from the reference program's by a relative error of at most 0.0001.
Values sent between devices are 32-bit elements; how exact they have to be, the bound alone decides.
No kernel may reach another device: no remote copies, remote signals or barrier semaphores. Data moves between devices by JAX's collectives and lax.ppermute only.
A program may use at most 64 MiB of HBM per device.

```python
import math
import jax
import jax.numpy as jnp
from jax import lax

PB = 128
R = 96
LEVELS = 4
BLOCK = 128
UCOLS = 1792
N_LEAF = 32
N_FRONT = 4


def draw_factor_inverse(key, part):
    leaf_ids = jnp.arange(N_LEAF, dtype=jnp.int32)[:, None, None, None]
    front_ids = jnp.arange(N_FRONT, dtype=jnp.int32)[None, :, None, None]
    row_ids = jnp.arange(PB, dtype=jnp.int32)[None, None, :, None]
    pieces = []
    for level_index in range(LEVELS):
        group_width = 2 ** level_index
        front_span = N_FRONT * PB * group_width
        column = jnp.arange(front_span, dtype=jnp.int32)[None, None, None, :]
        row_order = (front_ids * group_width + leaf_ids % group_width) * PB + row_ids
        level_key = jax.random.fold_in(key, 11 + level_index)
        shape_all = (N_LEAF, N_FRONT, PB, front_span)
        noise_part = jax.random.normal(level_key, shape_all, jnp.float32)
        noise_part = noise_part * (0.5 / math.sqrt(front_span))
        level_block = jnp.where(column < row_order, noise_part, 0.0) + jnp.where(column == row_order, 1.0, 0.0)
        pieces.append(level_block.astype(jnp.float32))
    return jnp.concatenate(pieces, axis=-1)


def draw_update_targets(key, part):
    target_lists = []
    for level_index in range(LEVELS - 1):
        group_width = 2 ** level_index
        node_count = N_LEAF // group_width
        block_count = 2 * PB * group_width // BLOCK
        parent_blocks = N_FRONT * PB * 2 * group_width // BLOCK
        scores = jax.random.randint(jax.random.fold_in(key, 31 + level_index), (node_count, parent_blocks), 0, 1 << 20)
        scores = scores * parent_blocks + jnp.arange(parent_blocks, dtype=jnp.int32)[None, :]
        node_ids = jnp.arange(node_count, dtype=jnp.int32)[:, None]
        block_ids = jnp.arange(parent_blocks, dtype=jnp.int32)[None, :]
        forced = (node_ids == 0) & (block_ids == parent_blocks - 1) | (node_ids == node_count - 1) & (block_ids == 0)
        scores = jnp.where(forced, -1, scores)
        chosen = jnp.sort(jnp.argsort(scores, axis=1)[:, :block_count].astype(jnp.int32), axis=1)
        target_lists.append(jnp.repeat(chosen, group_width, axis=0))
    return jnp.concatenate(target_lists, axis=1)


def touch_ends(entries, stream_key, least, high):
    dims = entries.shape
    index_at = [jax.random.randint(jax.random.fold_in(stream_key, axis), (), 0, dims[axis]) for axis in range(len(dims))]
    entries = entries.at[tuple(index_at)].set(least)
    longest = dims.index(max(dims))
    index_at[longest] = (index_at[longest] + 1) % dims[longest]
    return entries.at[tuple(index_at)].set(high)


def block_levels(stream_key, extent, split, least, high):
    def one(position, parts):
        heights = jax.random.uniform(jax.random.fold_in(jax.random.fold_in(stream_key, 6), position), (parts,), jnp.float32, least / len(split), high / len(split))
        return jnp.repeat(jnp.exp(heights), extent[position] // parts).reshape((-1,) + (1,) * (len(extent) - position - 1))

    factor_of = one(*split[0])
    for cut in split[1:]:
        factor_of = factor_of * one(*cut)
    return factor_of


def noise(key, dims, deviation, most, shards=(), kind=jnp.bfloat16):
    values = deviation * jax.random.normal(key, dims, jnp.float32)
    if shards:
        values = values * block_levels(key, dims, shards, -0.22, 0.18)
    return jnp.clip(values, -most, most).astype(kind)


def setup_inputs(seed: int = 0) -> dict:
    keys = jax.random.split(jax.random.key(seed), 8)
    right_side = noise(keys[0], (N_LEAF, N_FRONT, R, LEVELS * PB), 1.0, 6.0, ((0, 32), (1, 4)), jnp.float32)
    factor_inverse = draw_factor_inverse(jax.random.fold_in(keys[7], 71), 0)
    update_panel = noise(keys[2], (N_LEAF, N_FRONT, PB, UCOLS), (N_FRONT * PB * 2 ** (LEVELS - 1)) ** -0.5, 0.09375, ((0, 32), (1, 4)), jnp.float32)
    update_targets = draw_update_targets(jax.random.fold_in(keys[7], 71), 0)
    pivot_pairs = touch_ends((jax.random.randint(keys[4], (N_LEAF, N_FRONT, LEVELS * PB // 2), 0, 2) < 1).astype(jnp.int32), jax.random.fold_in(keys[4], 1), 0, 1)
    pivot_diagonal = jnp.clip(jnp.exp(math.log(2.0) - 1.3862944 * jax.random.uniform(keys[5], (N_LEAF, N_FRONT, LEVELS * PB), jnp.float32) ** block_levels(keys[5], (N_LEAF, N_FRONT, LEVELS * PB), ((0, 32), (1, 4)), -0.2, 0.2)), 0.5, 2.0)
    pivot_coupling = jnp.clip(3.0 + 2.0 * jax.random.uniform(keys[6], (N_LEAF, N_FRONT, LEVELS * PB // 2), jnp.float32) ** block_levels(keys[6], (N_LEAF, N_FRONT, LEVELS * PB // 2), ((0, 32), (1, 4)), -0.2, 0.2), 3.0, 5.0)
    return dict(right_side=right_side, factor_inverse=factor_inverse, update_panel=update_panel, update_targets=update_targets, pivot_pairs=pivot_pairs, pivot_diagonal=pivot_diagonal, pivot_coupling=pivot_coupling)


exact_mode = lax.Precision.HIGHEST


def front_of(values, level_index):
    group_width = 2 ** level_index
    node_count = N_LEAF // group_width
    side_count = values.shape[2]
    shaped = values.reshape(node_count, group_width, N_FRONT, side_count, PB)
    return shaped.transpose(0, 3, 2, 1, 4).reshape(node_count, side_count, N_FRONT * group_width * PB)


def spread_rows(front_values, level_index):
    group_width = 2 ** level_index
    node_count = N_LEAF // group_width
    side_count = front_values.shape[1]
    shaped = front_values.reshape(node_count, side_count, N_FRONT, group_width, PB)
    return shaped.transpose(0, 3, 2, 1, 4).reshape(N_LEAF, N_FRONT, side_count, PB)


def pivot_solve(solved, pivot_diag, couple, pivot_kinds):
    pair_first = solved[..., 0::2]
    second = solved[..., 1::2]
    diag_first = pivot_diag[..., 0::2][:, :, None, :]
    diag_second = pivot_diag[..., 1::2][:, :, None, :]
    coupling = couple[:, :, None, :]
    pair_flag = (pivot_kinds == 1)[:, :, None, :]
    determinant = diag_first * diag_second - coupling * coupling
    two_first = (diag_second * pair_first - coupling * second) / determinant
    two_second = (diag_first * second - coupling * pair_first) / determinant
    result_first = jnp.where(pair_flag, two_first, pair_first / diag_first)
    result_second = jnp.where(pair_flag, two_second, second / diag_second)
    return jnp.stack([result_first, result_second], axis=-1).reshape(solved.shape)


def target_table(update_targets, level_index):
    group_width = 2 ** level_index
    block_count = 2 * PB * group_width // BLOCK
    target_start = 2 * PB * (group_width - 1) // BLOCK
    parent_blocks = N_FRONT * PB * 2 * group_width // BLOCK
    target_lists = update_targets[::group_width, target_start:target_start + block_count]
    ids = jnp.arange(parent_blocks, dtype=jnp.int32)
    return (target_lists[:, :, None] == ids[None, None, :]).astype(jnp.float32)


def reference(right_side, factor_inverse, update_panel, update_targets, pivot_pairs, pivot_diagonal, pivot_coupling):
    side_count = right_side.shape[2]
    carried = jnp.zeros((N_LEAF, N_FRONT, side_count, PB), jnp.float32)
    weighted = []
    half_pb = PB // 2
    for level_index in range(LEVELS):
        group_width = 2 ** level_index
        node_count = N_LEAF // group_width
        front_span = N_FRONT * PB * group_width
        column_start = N_FRONT * PB * (group_width - 1)
        inverse_rows = factor_inverse[..., column_start:column_start + front_span]
        own_side = right_side[..., level_index * PB:(level_index + 1) * PB] - carried
        gathered = jnp.repeat(front_of(own_side, level_index), group_width, axis=0)
        solved = jnp.einsum("dqpc,drc->dqrp", inverse_rows, gathered, precision=exact_mode)
        weighted.append(pivot_solve(solved,
                                    pivot_diagonal[..., level_index * PB:(level_index + 1) * PB],
                                    pivot_coupling[..., level_index * half_pb:(level_index + 1) * half_pb],
                                    pivot_pairs[..., level_index * half_pb:(level_index + 1) * half_pb]))
        if level_index + 1 < LEVELS:
            update_len = 2 * PB * group_width
            update_start = 2 * PB * (group_width - 1)
            update_part = jnp.einsum("dqrp,dqpu->dqru", solved,
                                     update_panel[..., update_start:update_start + update_len], precision=exact_mode)
            summed = update_part.reshape(node_count, group_width, N_FRONT, side_count, update_len).sum(axis=(1, 2))
            onehot_table = target_table(update_targets, level_index)
            placed = jnp.einsum("nrkc,nkt->nrtc", summed.reshape(node_count, side_count, update_len // BLOCK, BLOCK),
                                onehot_table, precision=exact_mode)
            placed = placed.reshape(node_count // 2, 2, side_count, 2 * front_span).sum(axis=1)
            carried = spread_rows(placed, level_index + 1)
    answers = [None] * LEVELS
    for level_index in reversed(range(LEVELS)):
        group_width = 2 ** level_index
        node_count = N_LEAF // group_width
        front_span = N_FRONT * PB * group_width
        column_start = N_FRONT * PB * (group_width - 1)
        inverse_rows = factor_inverse[..., column_start:column_start + front_span]
        target = weighted[level_index]
        if level_index + 1 < LEVELS:
            update_len = 2 * PB * group_width
            update_start = 2 * PB * (group_width - 1)
            parent = jnp.repeat(front_of(answers[level_index + 1], level_index + 1), 2, axis=0)
            onehot_table = target_table(update_targets, level_index)
            chosen = jnp.einsum("nrtc,nkt->nrkc", parent.reshape(node_count, side_count, -1, BLOCK),
                                onehot_table, precision=exact_mode).reshape(node_count, side_count, update_len)
            chosen = jnp.repeat(chosen, group_width, axis=0)
            target = target - jnp.einsum("dru,dqpu->dqrp", chosen,
                                         update_panel[..., update_start:update_start + update_len], precision=exact_mode)
        partial_terms = jnp.einsum("dqrp,dqpc->dqrc", target, inverse_rows, precision=exact_mode)
        summed = partial_terms.reshape(node_count, group_width, N_FRONT, side_count, front_span).sum(axis=(1, 2))
        answers[level_index] = spread_rows(summed, level_index)
    return jnp.concatenate(answers, axis=-1)
```

```python
import jax
import jax.numpy as jnp
import numpy as np
from jax import lax
from jax.experimental import pallas as pl
from jax.experimental.pallas import tpu as pltpu
from jax.sharding import Mesh, PartitionSpec as P

LEVELS = 4
BLOCK = 128
PIVOTS = 128
SIDES = 96
HALF = SIDES // 2
AXES = ("z", "y1", "y0", "c", "x")

exact_mode = lax.Precision.HIGHEST


def dot_rows(left, right):
    return lax.dot_general(
        left, right, (((1,), (1,)), ((), ())), precision=exact_mode, preferred_element_type=jnp.float32
    )


def dot_cols(left, right):
    return lax.dot_general(
        left, right, (((1,), (0,)), ((), ())), precision=exact_mode, preferred_element_type=jnp.float32
    )


def exchange(value, axes):
    return lax.all_to_all(value, axes, 0, 0, tiled=True)


def with_partner(value):
    return lax.ppermute(value, "c", [(0, 1), (1, 0)])


def block_at(index):
    return pl.ds(pl.multiple_of(index * BLOCK, BLOCK), BLOCK)


def call(body, out_shapes, operands, specs, scratch=()):
    return pl.pallas_call(
        body,
        grid=(1,),
        in_specs=specs,
        out_specs=[pl.BlockSpec(s, lambda i, n=len(s): (0,) * n) for s in out_shapes],
        out_shape=[jax.ShapeDtypeStruct(s, jnp.float32) for s in out_shapes],
        scratch_shapes=list(scratch),
        compiler_params=pltpu.CompilerParams(vmem_limit_bytes=60 * 1024 * 1024),
    )(*operands)


class Inputs:
    def __init__(self):
        self.operands, self.specs = [], []

    def whole(self, value):
        shape = value.shape
        self.operands.append(value)
        self.specs.append(pl.BlockSpec(shape, lambda i, n=len(shape): (0,) * n))

    def scalars(self, value):
        self.operands.append(value)
        self.specs.append(pl.BlockSpec(memory_space=pltpu.SMEM))

    def columns(self, value, start, width, step):
        for k in range(width // step):
            self.operands.append(value)
            self.specs.append(
                pl.BlockSpec((value.shape[0], step), lambda i, at=start // step + k: (0, at))
            )


def pivot_apply(solved, own, swapped):
    lane = lax.broadcasted_iota(jnp.int32, solved.shape, 1)
    beside = jnp.where(lane % 2 == 0, pltpu.roll(solved, PIVOTS - 1, 1), pltpu.roll(solved, 1, 1))
    return own * solved + swapped * beside


def pivot_factors(kinds, diagonal, coupling):
    def body(kinds_ref, diagonal_ref, coupling_ref, out_ref):
        width = diagonal_ref.shape[1]
        row = lax.broadcasted_iota(jnp.int32, (width // 2, width), 0)
        col = lax.broadcasted_iota(jnp.int32, (width // 2, width), 1)
        widen = (col // 2 == row).astype(jnp.float32)
        pair = jnp.concatenate(
            [kinds_ref[...].astype(jnp.float32), coupling_ref[...], jnp.zeros((6, width // 2), jnp.float32)], 0
        )
        wide = dot_cols(pair, widen)
        is_pair = wide[0:1] > 0.5
        couple = wide[1:2]
        own = jnp.broadcast_to(diagonal_ref[...], (8, width))
        lane = lax.broadcasted_iota(jnp.int32, (8, width), 1)
        other = jnp.where(lane % 2 == 0, pltpu.roll(own, width - 1, 1), pltpu.roll(own, 1, 1))[0:1]
        own = own[0:1]
        determinant = own * other - couple * couple
        out_ref[0:1, :] = jnp.where(is_pair, other / determinant, 1.0 / own)
        out_ref[1:2, :] = jnp.where(is_pair, -couple / determinant, 0.0)

    args = Inputs()
    args.whole(kinds)
    args.whole(diagonal)
    args.whole(coupling)
    return call(body, [(2, diagonal.shape[1])], args.operands, args.specs)[0]


def level_zero_forward(first, inverse, update, factors):
    def body(first_ref, *refs):
        inverse_ref, update_ref, factors_ref, sent_ref, weighted_ref = refs
        inverse_rows = inverse_ref[...]
        solved = dot_rows(first_ref[0, :, :PIVOTS], inverse_rows[:, :PIVOTS])
        for q in range(1, 4):
            solved += dot_rows(first_ref[q, :, :PIVOTS], inverse_rows[:, q * PIVOTS : (q + 1) * PIVOTS])
        weighted_ref[...] = pivot_apply(solved, factors_ref[0:1, :], factors_ref[1:2, :])
        part = dot_cols(solved, update_ref[...])
        for c in range(2):
            for x in range(4):
                sent_ref[c * 4 + x] = part[c * HALF : (c + 1) * HALF]

    args = Inputs()
    args.whole(first)
    args.columns(inverse, 0, 512, 512)
    args.columns(update, 0, 256, 256)
    args.columns(factors, 0, PIVOTS, PIVOTS)
    return call(body, [(8, HALF, 256), (SIDES, PIVOTS)], args.operands, args.specs)


def forward(level, received, sides, targets, inverse, partner_inverse, update, partner_update, factors, partner_factors):
    width = 1 << level
    span = 4 * PIVOTS * width
    chunks = span // 512
    start = 4 * PIVOTS * (width - 1)
    update_len = 2 * PIVOTS * width
    update_start = 2 * PIVOTS * (width - 1)
    update_step = 256
    update_chunks = update_len // update_step if level < 3 else 0
    blocks = (2, 4, 8)[level - 1]
    table_at = (0, 4, 12)[level - 1]

    def body(*refs):
        refs = list(refs)
        targets_ref, received_ref, sides_ref = refs[:3]
        at = 3
        own_inverse = refs[at : at + chunks]
        at += chunks
        other_inverse = refs[at : at + chunks]
        at += chunks
        own_update = refs[at : at + update_chunks]
        at += update_chunks
        other_update = refs[at : at + update_chunks]
        at += update_chunks
        own_factors, other_factors = refs[at : at + 2]
        outs = refs[at + 2 : -1]
        b_ref = refs[-1]
        for i in range(span // 256):
            if level == 1:
                b_ref[:, i * 256 : i * 256 + 128] = sides_ref[i, 0:HALF, PIVOTS:]
                b_ref[:, i * 256 + 128 : i * 256 + 256] = sides_ref[i, HALF:, PIVOTS:]
            else:
                b_ref[:, i * 256 : (i + 1) * 256] = sides_ref[i]
        for child in range(2):
            if level < 3:
                if level == 1:
                    total = sum(received_ref[child * 4 + x] for x in range(4))
                else:
                    total = sum(received_ref[x * 2 + child] for x in range(4))
            for k in range(blocks):
                if level < 3:
                    piece = total[:, k * BLOCK : (k + 1) * BLOCK]
                else:
                    piece = received_ref[(k // 2) * 4 + child * 2 + k % 2]
                where = block_at(targets_ref[table_at + child * blocks + k])
                b_ref[:, where] = b_ref[:, where] - piece
        own = jnp.zeros((HALF, PIVOTS), jnp.float32)
        other = jnp.zeros((HALF, PIVOTS), jnp.float32)
        for k in range(chunks):
            rows = b_ref[:, k * 512 : (k + 1) * 512]
            own += dot_rows(rows, own_inverse[k][...])
            other += dot_rows(rows, other_inverse[k][...])
        own_weighted = pivot_apply(own, own_factors[0:1, :], own_factors[1:2, :])
        other_weighted = pivot_apply(other, other_factors[0:1, :], other_factors[1:2, :])
        if level < 3:
            sent_ref, weighted_ref = outs
            weighted_ref[0] = own_weighted
            weighted_ref[1] = other_weighted
            for k in range(update_chunks):
                part = dot_cols(own, own_update[k][...]) + dot_cols(other, other_update[k][...])
                if level == 1:
                    for i in range(8):
                        sent_ref[i, :, k * 256 : (k + 1) * 256] = part
                else:
                    sent_ref[2 * k] = part[:, :BLOCK]
                    sent_ref[2 * k + 1] = part[:, BLOCK:]
        else:
            sent_ref, full_ref = outs
            for k in range(chunks):
                part = dot_cols(own_weighted, own_inverse[k][...]) + dot_cols(other_weighted, other_inverse[k][...])
                b_ref[:, k * 512 : (k + 1) * 512] = part
                full_ref[2 * k] = part[:, :256]
                full_ref[2 * k + 1] = part[:, 256:]
            for child in range(2):
                for k in range(8):
                    where = block_at(targets_ref[table_at + child * 8 + k])
                    sent_ref[(k // 2) * 4 + child * 2 + k % 2] = b_ref[:, where]

    args = Inputs()
    args.scalars(targets)
    args.whole(received)
    args.whole(sides)
    args.columns(inverse, start, span, 512)
    args.columns(partner_inverse, start, span, 512)
    if level < 3:
        args.columns(update, update_start, update_len, update_step)
        args.columns(partner_update, update_start, update_len, update_step)
    args.columns(factors, level * PIVOTS, PIVOTS, PIVOTS)
    args.columns(partner_factors, level * PIVOTS, PIVOTS, PIVOTS)
    outs = {
        1: [(8, HALF, 512), (2, HALF, PIVOTS)],
        2: [(8, HALF, BLOCK), (2, HALF, PIVOTS)],
        3: [(16, HALF, BLOCK), (16, HALF, 256)],
    }[level]
    return call(body, outs, args.operands, args.specs, [pltpu.VMEM((HALF, span), jnp.float32)])


def backward(level, received, weighted, targets, inverse, partner_inverse, update, partner_update):
    width = 1 << level
    span = 4 * PIVOTS * width
    chunks = span // 512
    start = 4 * PIVOTS * (width - 1)
    update_len = 2 * PIVOTS * width
    update_start = 2 * PIVOTS * (width - 1)
    update_chunks = update_len // 256
    blocks = (2, 4)[level - 1]
    table_at = (0, 4)[level - 1]

    def body(*refs):
        refs = list(refs)
        targets_ref, received_ref, weighted_ref = refs[:3]
        at = 3
        own_inverse = refs[at : at + chunks]
        at += chunks
        other_inverse = refs[at : at + chunks]
        at += chunks
        own_update = refs[at : at + update_chunks]
        at += update_chunks
        other_update = refs[at : at + update_chunks]
        sent_ref, full_ref, x_ref = refs[-3:]
        own = weighted_ref[0]
        other = weighted_ref[1]
        if level == 1:
            total = sum(received_ref[i] for i in range(8))
        for k in range(update_chunks):
            if level == 1:
                chosen = total[:, k * 256 : (k + 1) * 256]
            else:
                chosen = jnp.concatenate([received_ref[2 * k], received_ref[2 * k + 1]], 1)
            own -= dot_rows(chosen, own_update[k][...])
            other -= dot_rows(chosen, other_update[k][...])
        for k in range(chunks):
            part = dot_cols(own, own_inverse[k][...]) + dot_cols(other, other_inverse[k][...])
            x_ref[:, k * 512 : (k + 1) * 512] = part
            full_ref[2 * k] = part[:, :256]
            full_ref[2 * k + 1] = part[:, 256:]
        for child in range(2):
            for k in range(blocks):
                where = block_at(targets_ref[table_at + child * blocks + k])
                piece = x_ref[:, where]
                for x in range(4):
                    sent_ref[x * 2 + child, :, k * BLOCK : (k + 1) * BLOCK] = piece

    args = Inputs()
    args.scalars(targets)
    args.whole(received)
    args.whole(weighted)
    args.columns(inverse, start, span, 512)
    args.columns(partner_inverse, start, span, 512)
    args.columns(update, update_start, update_len, 256)
    args.columns(partner_update, update_start, update_len, 256)
    outs = [(8, HALF, blocks * BLOCK), (span // 256, HALF, 256)]
    return call(body, outs, args.operands, args.specs, [pltpu.VMEM((HALF, span), jnp.float32)])


def level_zero_backward(received, weighted, inverse, update, upper):
    def body(received_ref, weighted_ref, inverse_ref, update_ref, upper_ref, sent_ref):
        update_rows = update_ref[...]
        inverse_rows = inverse_ref[...]
        for c in range(2):
            half = slice(c * HALF, (c + 1) * HALF)
            chosen = sum(received_ref[x * 2 + c] for x in range(4))
            target = weighted_ref[half] - dot_rows(chosen, update_rows)
            part = dot_cols(target, inverse_rows)
            for q in range(4):
                sent_ref[q, half, :PIVOTS] = part[:, q * PIVOTS : (q + 1) * PIVOTS]
                sent_ref[q, half, PIVOTS:] = upper_ref[q, :, c * PIVOTS : (c + 1) * PIVOTS]

    args = Inputs()
    args.whole(received)
    args.whole(weighted)
    args.columns(inverse, 0, 512, 512)
    args.columns(update, 0, 256, 256)
    args.whole(upper)
    return call(body, [(4, SIDES, 256)], args.operands, args.specs)[0]


def copies(value, count):
    return jnp.broadcast_to(value[None], (count, *value.shape))


def sibling_targets(targets):
    pairs = []
    for y1 in range(2):
        for y0 in range(2):
            here = y1 * 4 + y0 * 2
            pairs.append((here, y1 * 4 + (1 - y0) * 2))
            pairs.append((here + 1, (1 - y1) * 4 + y0 * 2 + 1))
    received = lax.ppermute(targets, ("y1", "y0", "c"), pairs)
    both = jnp.stack([targets, received])
    other = with_partner(both)
    c, y0, y1 = lax.axis_index("c"), lax.axis_index("y0"), lax.axis_index("y1")

    def ordered(own, sibling, bit):
        return jnp.where(bit == 0, jnp.concatenate([own, sibling]), jnp.concatenate([sibling, own]))

    side = jnp.where(c == 0, received, other[1])
    above = jnp.where(c == 0, other[1], received)
    return jnp.concatenate(
        [
            ordered(targets[0:2], other[0, 0:2], c),
            ordered(targets[2:6], side[2:6], y0),
            ordered(targets[6:14], above[6:14], y1),
        ]
    )


def per_device(right_side, factor_inverse, update_panel, update_targets, pivot_pairs, pivot_diagonal, pivot_coupling):
    sides = right_side[0, 0]
    inverse = factor_inverse[0, 0]
    update = update_panel[0, 0]
    c = lax.axis_index("c")
    targets = sibling_targets(update_targets[0])
    factors = pivot_factors(pivot_pairs[0], pivot_diagonal[0], pivot_coupling[0])
    partner_factors = with_partner(factors)
    partner_inverse = with_partner(inverse)
    partner_update = with_partner(update)

    upper = sides[:, PIVOTS:]
    kept = lax.dynamic_slice_in_dim(upper, c * HALF, HALF, 0)
    swapped = with_partner(lax.dynamic_slice_in_dim(upper, (1 - c) * HALF, HALF, 0))
    low = jnp.where(c == 0, kept, swapped)
    high = jnp.where(c == 0, swapped, kept)
    rows = [jnp.concatenate([low[:, i : i + PIVOTS], high[:, i : i + PIVOTS]], 1) for i in (0, 128, 256)]

    first = jnp.concatenate(
        [sides[:, :PIVOTS], jnp.concatenate([rows[0][:, :PIVOTS], rows[0][:, PIVOTS:]], 0)], 1
    )
    first = exchange(copies(first, 4), ("x",))
    sides2 = exchange(copies(rows[1], 8), ("x", "y0"))
    sides3 = exchange(copies(rows[2], 16), ("x", "y1", "y0"))

    sent, weighted0 = level_zero_forward(first, inverse, update, factors)
    received = exchange(sent, ("c", "x"))
    sent, weighted1 = forward(
        1, received, first, targets, inverse, partner_inverse, update, partner_update, factors, partner_factors
    )
    received = exchange(sent, ("x", "y0"))
    sent, weighted2 = forward(
        2, received, sides2, targets, inverse, partner_inverse, update, partner_update, factors, partner_factors
    )
    received = jnp.sum(exchange(sent, ("x", "y0")), 0)
    received = exchange(copies(received, 16), ("x", "y1", "y0"))
    sent, full3 = forward(
        3, received, sides3, targets, inverse, partner_inverse, update, partner_update, factors, partner_factors
    )
    received = jnp.sum(exchange(sent, ("x", "y1", "y0")), 0)
    received = exchange(copies(received, 8), ("x", "y0"))
    answer3 = exchange(full3, ("x", "y1", "y0"))
    sent, full2 = backward(2, received, weighted2, targets, inverse, partner_inverse, update, partner_update)
    received = exchange(sent, ("x", "y0"))
    answer2 = exchange(full2, ("x", "y0"))
    sent, full1 = backward(1, received, weighted1, targets, inverse, partner_inverse, update, partner_update)
    received = exchange(sent, ("x", "c"))
    sent = level_zero_backward(received, weighted0, inverse, update, full1)
    last = jnp.sum(exchange(sent, ("x",)), 0)

    answer1 = jnp.concatenate([last[:HALF, PIVOTS:], last[HALF:, PIVOTS:]], 1)
    answers = [answer1, jnp.sum(answer2, 0), jnp.sum(answer3, 0)]
    low = jnp.concatenate([a[:, :PIVOTS] for a in answers], 1)
    high = jnp.concatenate([a[:, PIVOTS:] for a in answers], 1)
    kept = jnp.where(c == 0, low, high)
    swapped = with_partner(jnp.where(c == 0, high, low))
    upper = jnp.where(c == 0, jnp.concatenate([kept, swapped], 0), jnp.concatenate([swapped, kept], 0))
    return jnp.concatenate([last[:, :PIVOTS], upper], 1)[None, None]


def solution(mesh):
    grid = np.array(mesh.devices).reshape(4, 2, 2, 2, 4)
    fine = Mesh(grid, AXES)
    leaf = ("z", "y1", "y0", "c")
    in_specs = (
        P(leaf, "x", None, None),
        P(leaf, "x", None, None),
        P(leaf, "x", None, None),
        P(leaf, None),
        P(leaf, "x", None),
        P(leaf, "x", None),
        P(leaf, "x", None),
    )
    out_specs = P(leaf, "x", None, None)
    return jax.shard_map(per_device, mesh=fine, in_specs=in_specs, out_specs=out_specs, check_vma=False)
```

```python
import jax
import jax.numpy as jnp
import numpy as np
from jax import lax
from jax.experimental import pallas as pl
from jax.experimental.pallas import tpu as pltpu
from jax.sharding import Mesh, PartitionSpec as P

LEVELS = 4
BLOCK = 128
PIVOTS = 128
SIDES = 96
HALF = SIDES // 2
AXES = ("z", "y1", "y0", "c", "x")

exact_mode = lax.Precision.HIGHEST


def dot_rows(left, right):
    return lax.dot_general(
        left, right, (((1,), (1,)), ((), ())), precision=exact_mode, preferred_element_type=jnp.float32
    )


def dot_cols(left, right):
    return lax.dot_general(
        left, right, (((1,), (0,)), ((), ())), precision=exact_mode, preferred_element_type=jnp.float32
    )


def dot_full(left, right):
    return lax.dot_general(
        left, right, (((1,), (0,)), ((), ())), precision=exact_mode, preferred_element_type=jnp.float32
    )


def exchange(value, axes):
    return lax.all_to_all(value, axes, 0, 0, tiled=True)


def with_partner(value):
    return lax.ppermute(value, "c", [(0, 1), (1, 0)])


def across(value, axis):
    return lax.ppermute(value, axis, [(0, 1), (1, 0)])


def block_at(index, size=BLOCK):
    return pl.ds(pl.multiple_of(index * size, size), size)


WHOLE = pl.BlockSpec(memory_space=pltpu.VMEM)
SCALARS = pl.BlockSpec(memory_space=pltpu.SMEM)
FAR = pl.BlockSpec(memory_space=pltpu.HBM)


def call(body, out_shapes, operands, specs, scratch=(), limit=16):
    return pl.pallas_call(
        body,
        in_specs=specs,
        out_specs=[WHOLE] * len(out_shapes),
        out_shape=[jax.ShapeDtypeStruct(s, jnp.float32) for s in out_shapes],
        scratch_shapes=list(scratch),
        compiler_params=pltpu.CompilerParams(vmem_limit_bytes=limit * 1024 * 1024),
    )(*operands)


class Stream:
    def __init__(self, pair, start, width, step, buffer, semaphores):
        self.step, self.buffer, self.moves = step, buffer, []
        for k in range(width // step):
            both = []
            for side, source in enumerate(pair):
                both.append(
                    pltpu.make_async_copy(
                        source.at[:, pl.ds(start + k * step, step)],
                        buffer.at[pl.ds(side * PIVOTS, PIVOTS), pl.ds(k * step, step)],
                        semaphores.at[k, side],
                    )
                )
            self.moves.append(both)

    def start(self):
        for both in self.moves:
            for move in both:
                move.start()

    def wait(self, k):
        for move in self.moves[k]:
            move.wait()

    def at(self, k):
        return self.buffer[:, k * self.step : (k + 1) * self.step]


def stream_scratch(pair, width, step):
    return [pltpu.VMEM((pair * PIVOTS, width), jnp.float32), pltpu.SemaphoreType.DMA((width // step, pair))]


def pivot_apply(solved, own, swapped):
    lane = lax.broadcasted_iota(jnp.int32, solved.shape, 1)
    width = solved.shape[1]
    beside = jnp.where(lane % 2 == 0, pltpu.roll(solved, width - 1, 1), pltpu.roll(solved, 1, 1))
    return own * solved + swapped * beside


def pivot_factors(kinds, diagonal, coupling):
    def body(kinds_ref, diagonal_ref, coupling_ref, out_ref):
        width = diagonal_ref.shape[1]
        row = lax.broadcasted_iota(jnp.int32, (width // 2, width), 0)
        col = lax.broadcasted_iota(jnp.int32, (width // 2, width), 1)
        widen = (col // 2 == row).astype(jnp.float32)
        pair = jnp.concatenate(
            [kinds_ref[...].astype(jnp.float32), coupling_ref[...], jnp.zeros((6, width // 2), jnp.float32)], 0
        )
        wide = dot_full(pair, widen)
        is_pair = wide[0:1] > 0.5
        couple = wide[1:2]
        own = jnp.broadcast_to(diagonal_ref[...], (8, width))
        lane = lax.broadcasted_iota(jnp.int32, (8, width), 1)
        other = jnp.where(lane % 2 == 0, pltpu.roll(own, width - 1, 1), pltpu.roll(own, 1, 1))[0:1]
        own = own[0:1]
        determinant = own * other - couple * couple
        out_ref[0:1, :] = jnp.where(is_pair, other / determinant, 1.0 / own)
        out_ref[1:2, :] = jnp.where(is_pair, -couple / determinant, 0.0)

    return call(body, [(2, diagonal.shape[1])], [kinds, diagonal, coupling], [WHOLE] * 3)[0]


def packed_sides(sides, beside):
    def body(sides_ref, beside_ref, out_ref):
        c = lax.axis_index("c")
        mine = pl.ds(pl.multiple_of(c * HALF, 8), HALF)
        theirs = pl.ds(pl.multiple_of((1 - c) * HALF, 8), HALF)
        own = sides_ref[mine, PIVOTS:]
        other = beside_ref[mine, PIVOTS:]
        for i in range(4):
            out_ref[i, :, :PIVOTS] = sides_ref[:, :PIVOTS]
            out_ref[i, mine, PIVOTS:] = own
            out_ref[i, theirs, PIVOTS:] = other

    return call(body, [(4, SIDES, 512)], [sides, beside], [WHOLE] * 2)[0]


def level_zero_forward(first, inverse, update, factors):
    def body(first_ref, inverse_ref, update_ref, factors_ref, sent_ref, weighted_ref, upper_ref, *scratch):
        weights = Stream([inverse_ref], 0, 512, 512, *scratch[:2])
        updates = Stream([update_ref], 0, 256, 256, *scratch[2:])
        weights.start()
        updates.start()
        for q in range(4):
            upper_ref[q] = first_ref[q, :, 2 * PIVOTS :]
        gathered = jnp.concatenate([first_ref[q, :, :PIVOTS] for q in range(4)], 1)
        weights.wait(0)
        solved = dot_rows(gathered, weights.at(0))
        weighted_ref[...] = pivot_apply(solved, factors_ref[0:1, :PIVOTS], factors_ref[1:2, :PIVOTS])
        updates.wait(0)
        part = dot_cols(solved, updates.at(0))
        for c in range(2):
            for x in range(4):
                sent_ref[c * 4 + x] = part[c * HALF : (c + 1) * HALF]

    return call(
        body,
        [(8, HALF, 256), (SIDES, PIVOTS), (4, SIDES, 256)],
        [first, inverse, update, factors],
        [WHOLE, FAR, FAR, WHOLE],
        stream_scratch(1, 512, 512) + stream_scratch(1, 256, 256),
    )


def child_block(level, tables, child, k):
    own_ref, side_ref, own_beside_ref, side_beside_ref = tables
    c = lax.axis_index("c")
    if level == 1:
        return jnp.where(c == child, own_ref[0, k], own_beside_ref[0, k])
    if level == 2:
        sibling = jnp.where(c == 0, side_ref[0, 2 + k], side_beside_ref[0, 2 + k])
        return jnp.where(lax.axis_index("y0") == child, own_ref[0, 2 + k], sibling)
    sibling = jnp.where(c == 0, side_beside_ref[0, 6 + k], side_ref[0, 6 + k])
    return jnp.where(lax.axis_index("y1") == child, own_ref[0, 6 + k], sibling)


def both_factors(level, factors, beside):
    c = lax.axis_index("c")
    at = slice(level * PIVOTS, (level + 1) * PIVOTS)
    return [jnp.concatenate([factors[i : i + 1, at], beside[i : i + 1, at]], 1) for i in range(2)]


def halves(rows):
    return jnp.concatenate([rows[:HALF], rows[HALF:]], 1)


def forward(level, received, sides, tables, weights_pair, update_pair, factors, partner_factors):
    width = 1 << level
    span = 4 * PIVOTS * width
    chunks = span // 512
    start = 4 * PIVOTS * (width - 1)
    update_len = 2 * PIVOTS * width if level < 3 else 0
    update_start = 2 * PIVOTS * (width - 1)
    blocks = (2, 4, 8)[level - 1]
    n_sides = len(sides)
    n_updates = 2 if level < 3 else 0

    def body(*refs):
        refs = list(refs)

        def take(count):
            taken, refs[:] = refs[:count], refs[count:]
            return taken

        tables_refs = take(4)
        (received_ref,) = take(1)
        sides_refs = take(n_sides)
        factors_ref, beside_ref = take(2)
        inverse_refs = take(2)
        update_refs = take(n_updates)
        outs = take(2 if level == 2 else 3)
        (b_ref,) = take(1)
        weights = Stream(inverse_refs, start, span, 512, *take(2))
        weights.start()
        if level < 3:
            updates = Stream(update_refs, update_start, update_len, 256, *take(2))
            updates.start()
        y0, y1 = lax.axis_index("y0"), lax.axis_index("y1")
        if level == 1:
            for x in range(4):
                b_ref[:, x * 256 : (x + 1) * 256] = halves(sides_refs[0][x, :, PIVOTS : 2 * PIVOTS])
            near, far = sides_refs[1], sides_refs[2]
            outs[2][0] = near[:, :, PIVOTS:]
            outs[2][1] = far[:, :, PIVOTS:]
        elif level == 2:
            for flip in range(2):
                for x in range(4):
                    b_ref[:, block_at(x * 2 + (y0 ^ flip), 256)] = halves(sides_refs[flip][x, :, :PIVOTS])
        else:
            for high in range(2):
                for flip in range(2):
                    for x in range(4):
                        where = block_at(x * 4 + (y1 ^ high) * 2 + (y0 ^ flip), 256)
                        b_ref[:, where] = halves(sides_refs[high][flip, x])
        for child in range(2):
            if level == 1:
                total = sum(received_ref[child * 4 + x] for x in range(4))
            elif level == 2:
                total = sum(received_ref[x * 2 + child] for x in range(4))
            for k in range(blocks):
                if level < 3:
                    piece = total[:, k * BLOCK : (k + 1) * BLOCK]
                else:
                    piece = received_ref[(k // 2) * 4 + child * 2 + k % 2]
                where = block_at(child_block(level, tables_refs, child, k))
                b_ref[:, where] = b_ref[:, where] - piece
        solved = jnp.zeros((HALF, 2 * PIVOTS), jnp.float32)
        for k in range(chunks):
            weights.wait(k)
            solved += dot_rows(b_ref[:, k * 512 : (k + 1) * 512], weights.at(k))
        weighted = pivot_apply(solved, *both_factors(level, factors_ref, beside_ref))
        if level < 3:
            outs[1][...] = weighted
            for k in range(update_len // 256):
                updates.wait(k)
                part = dot_cols(solved, updates.at(k))
                if level == 1:
                    for i in range(8):
                        outs[0][i, :, k * 256 : (k + 1) * 256] = part
                else:
                    outs[0][2 * k] = part[:, :BLOCK]
                    outs[0][2 * k + 1] = part[:, BLOCK:]
        else:
            sent_ref, keep_ref, far_ref = outs
            for k in range(chunks):
                b_ref[:, k * 512 : (k + 1) * 512] = dot_cols(weighted, weights.at(k))
            for child in range(2):
                for k in range(8):
                    where = block_at(child_block(3, tables_refs, child, k))
                    sent_ref[(k // 2) * 4 + child * 2 + k % 2] = b_ref[:, where]
            for x in range(4):
                for low in range(2):
                    keep_ref[x, low] = b_ref[:, block_at(x * 4 + y1 * 2 + low, 256)]
                    far_ref[x, low] = b_ref[:, block_at(x * 4 + (1 - y1) * 2 + low, 256)]

    outs = {
        1: [(8, HALF, 512), (HALF, 256), (2, 4, SIDES, PIVOTS)],
        2: [(8, HALF, BLOCK), (HALF, 256)],
        3: [(16, HALF, BLOCK), (4, 2, HALF, 256), (4, 2, HALF, 256)],
    }[level]
    scratch = [pltpu.VMEM((HALF, span), jnp.float32)] + stream_scratch(2, span, 512)
    operands = [*tables, received, *sides, factors, partner_factors, *weights_pair]
    specs = [SCALARS] * 4 + [WHOLE] * (3 + n_sides) + [FAR] * 2
    if level < 3:
        scratch += stream_scratch(2, update_len, 256)
        operands += update_pair
        specs += [FAR] * 2
    return call(body, outs, operands, specs, scratch, 20)


def backward(level, received, weighted, tables, weights_pair, update_pair, answers):
    width = 1 << level
    span = 4 * PIVOTS * width
    chunks = span // 512
    start = 4 * PIVOTS * (width - 1)
    update_len = 2 * PIVOTS * width
    update_start = 2 * PIVOTS * (width - 1)
    blocks = (2, 4)[level - 1]

    def body(*refs):
        refs = list(refs)

        def take(count):
            taken, refs[:] = refs[:count], refs[count:]
            return taken

        tables_refs = take(4)
        received_ref, weighted_ref = take(2)
        answer_refs = take(len(answers))
        inverse_refs = take(2)
        update_refs = take(2)
        outs = take(2 if level == 1 else 3)
        (x_ref,) = take(1)
        weights = Stream(inverse_refs, start, span, 512, *take(2))
        updates = Stream(update_refs, update_start, update_len, 256, *take(2))
        updates.start()
        weights.start()
        target = weighted_ref[...]
        if level == 1:
            total = sum(received_ref[i] for i in range(8))
        for k in range(update_len // 256):
            if level == 1:
                chosen = total[:, k * 256 : (k + 1) * 256]
            else:
                chosen = jnp.concatenate([received_ref[2 * k], received_ref[2 * k + 1]], 1)
            updates.wait(k)
            target -= dot_rows(chosen, updates.at(k))
        for k in range(chunks):
            weights.wait(k)
            x_ref[:, k * 512 : (k + 1) * 512] = dot_cols(target, weights.at(k))
        for child in range(2):
            for k in range(blocks):
                piece = x_ref[:, block_at(child_block(level, tables_refs, child, k))]
                for x in range(4):
                    outs[0][x * 2 + child, :, k * BLOCK : (k + 1) * BLOCK] = piece
        if level == 1:
            for x in range(4):
                outs[1][x] = x_ref[:, x * 256 : (x + 1) * 256]
        else:
            y0 = lax.axis_index("y0")
            keep_ref, far_ref = outs[1:]
            own_ref, other_ref = answer_refs
            for x in range(4):
                keep_ref[0, x] = x_ref[:, block_at(x * 2 + y0, 256)]
                far_ref[0, x] = x_ref[:, block_at(x * 2 + (1 - y0), 256)]
                keep_ref[1, x] = own_ref[x, y0] + other_ref[x, y0]
                far_ref[1, x] = own_ref[x, 1 - y0] + other_ref[x, 1 - y0]

    outs = [(8, HALF, blocks * BLOCK)]
    outs += [(4, HALF, 256)] if level == 1 else [(2, 4, HALF, 256), (2, 4, HALF, 256)]
    scratch = [pltpu.VMEM((HALF, span), jnp.float32)]
    scratch += stream_scratch(2, span, 512) + stream_scratch(2, update_len, 256)
    operands = [*tables, received, weighted, *answers, *weights_pair, *update_pair]
    specs = [SCALARS] * 4 + [WHOLE] * (2 + len(answers)) + [FAR] * 4
    return call(body, outs, operands, specs, scratch, 20)


def level_zero_backward(received, weighted, inverse, update, nearest, kept, other):
    def body(received_ref, weighted_ref, nearest_ref, kept_ref, other_ref, inverse_ref, update_ref, sent_ref, *scratch):
        weights = Stream([inverse_ref], 0, 512, 512, *scratch[:2])
        updates = Stream([update_ref], 0, 256, 256, *scratch[2:])
        updates.start()
        weights.start()
        for x in range(4):
            for c in range(2):
                half = slice(c * HALF, (c + 1) * HALF)
                at = slice(c * PIVOTS, (c + 1) * PIVOTS)
                sent_ref[x, half, PIVOTS : 2 * PIVOTS] = nearest_ref[x, :, at]
                for i in range(2):
                    piece = kept_ref[i, x, :, at] + other_ref[i, x, :, at]
                    sent_ref[x, half, (2 + i) * PIVOTS : (3 + i) * PIVOTS] = piece
        chosen = jnp.concatenate([sum(received_ref[x * 2 + c] for x in range(4)) for c in range(2)], 0)
        updates.wait(0)
        target = weighted_ref[...] - dot_rows(chosen, updates.at(0))
        weights.wait(0)
        part = dot_cols(target, weights.at(0))
        for q in range(4):
            sent_ref[q, :, :PIVOTS] = part[:, q * PIVOTS : (q + 1) * PIVOTS]

    return call(
        body,
        [(4, SIDES, 512)],
        [received, weighted, nearest, kept, other, inverse, update],
        [WHOLE] * 5 + [FAR] * 2,
        stream_scratch(1, 512, 512) + stream_scratch(1, 256, 256),
    )[0]


def summed(received):
    def body(received_ref, out_ref):
        out_ref[...] = (received_ref[0] + received_ref[1]) + (received_ref[2] + received_ref[3])

    return call(body, [(SIDES, 512)], [received], [WHOLE])[0]


def unpacked(total, beside):
    def body(total_ref, beside_ref, out_ref):
        c = lax.axis_index("c")
        mine = pl.ds(pl.multiple_of(c * HALF, 8), HALF)
        theirs = pl.ds(pl.multiple_of((1 - c) * HALF, 8), HALF)
        out_ref[:, :PIVOTS] = total_ref[:, :PIVOTS]
        out_ref[mine, PIVOTS:] = total_ref[mine, PIVOTS:]
        out_ref[theirs, PIVOTS:] = beside_ref[mine, PIVOTS:]

    return call(body, [(SIDES, 512)], [total, beside], [WHOLE] * 2)[0]


def summed_copies(received, count):
    total = jnp.sum(received, 0)
    return jnp.broadcast_to(total[None], (count, *total.shape))


def sibling_tables(targets):
    pairs = []
    for y1 in range(2):
        for y0 in range(2):
            here = y1 * 4 + y0 * 2
            pairs.append((here, y1 * 4 + (1 - y0) * 2))
            pairs.append((here + 1, (1 - y1) * 4 + y0 * 2 + 1))
    side = lax.ppermute(targets, ("y1", "y0", "c"), pairs)
    return [targets, side, with_partner(targets), with_partner(side)]


def per_device(right_side, factor_inverse, update_panel, update_targets, pivot_pairs, pivot_diagonal, pivot_coupling):
    sides = right_side[0, 0]
    inverse = factor_inverse[0, 0]
    update = update_panel[0, 0]
    plane = ("x", "y1", "y0")
    pair = ("x", "y0")

    first = exchange(packed_sides(sides, with_partner(sides)), ("x",))
    tables = sibling_tables(update_targets)
    factors = pivot_factors(pivot_pairs[0], pivot_diagonal[0], pivot_coupling[0])
    partner_factors = with_partner(factors)
    weights_pair = [inverse, with_partner(inverse)]
    update_pair = [update, with_partner(update)]

    sent, weighted0, near = level_zero_forward(first, inverse, update, factors)
    far = across(near, "y0")
    received = exchange(sent, ("c", "x"))
    sent, weighted1, near3 = forward(
        1, received, [first, near, far], tables, weights_pair, update_pair, factors, partner_factors
    )
    far3 = across(near3, "y1")
    received = exchange(sent, pair)
    sent, weighted2 = forward(2, received, [near, far], tables, weights_pair, update_pair, factors, partner_factors)
    received = exchange(summed_copies(exchange(sent, pair), 16), plane)
    sent, kept3, other3 = forward(
        3, received, [near3, far3], tables, weights_pair, None, factors, partner_factors
    )
    other3 = across(other3, "y1")
    received = exchange(summed_copies(exchange(sent, plane), 8), pair)
    sent, kept, other = backward(2, received, weighted2, tables, weights_pair, update_pair, [kept3, other3])
    other = across(other, "y0")
    received = exchange(sent, pair)
    sent, nearest = backward(1, received, weighted1, tables, weights_pair, update_pair, [])
    received = exchange(sent, ("x", "c"))
    sent = level_zero_backward(received, weighted0, inverse, update, nearest, kept, other)
    total = summed(exchange(sent, ("x",)))
    return unpacked(total, with_partner(total))[None, None]


def solution(mesh):
    grid = np.array(mesh.devices).reshape(4, 2, 2, 2, 4)
    fine = Mesh(grid, AXES)
    leaf = ("z", "y1", "y0", "c")
    in_specs = (
        P(leaf, "x", None, None),
        P(leaf, "x", None, None),
        P(leaf, "x", None, None),
        P(leaf, None),
        P(leaf, "x", None),
        P(leaf, "x", None),
        P(leaf, "x", None),
    )
    out_specs = P(leaf, "x", None, None)
    return jax.shard_map(per_device, mesh=fine, in_specs=in_specs, out_specs=out_specs, check_vma=False)
```

```python
import jax
import jax.numpy as jnp
import numpy as np
from jax import lax
from jax.experimental import pallas as pl
from jax.experimental.pallas import tpu as pltpu
from jax.sharding import Mesh, PartitionSpec as P

LEVELS = 4
BLOCK = 128
PIVOTS = 128
SIDES = 96
HALF = SIDES // 2
AXES = ("z", "y1", "y0", "c", "x")

exact_mode = lax.Precision.HIGHEST


def parts(value):
    high = value.astype(jnp.bfloat16)
    return high, (value - high.astype(jnp.float32)).astype(jnp.bfloat16)


def product(left, high, low, side):
    left_high, left_low = parts(left)
    dims = (((1,), (side,)), ((), ()))

    def dot(a, b):
        return lax.dot_general(a, b, dims, preferred_element_type=jnp.float32)

    return dot(left_high, high) + (dot(left_high, low) + dot(left_low, high))


def dot_full(left, right):
    return lax.dot_general(
        left, right, (((1,), (0,)), ((), ())), precision=exact_mode, preferred_element_type=jnp.float32
    )


def exchange(value, axes):
    return lax.all_to_all(value, axes, 0, 0, tiled=True)


def with_partner(value):
    return lax.ppermute(value, "c", [(0, 1), (1, 0)])


def across(value, axis):
    return lax.ppermute(value, axis, [(0, 1), (1, 0)])


def block_at(index, size=BLOCK):
    return pl.ds(pl.multiple_of(index * size, size), size)


WHOLE = pl.BlockSpec(memory_space=pltpu.VMEM)
SCALARS = pl.BlockSpec(memory_space=pltpu.SMEM)
FAR = pl.BlockSpec(memory_space=pltpu.HBM)


def call(body, out_shapes, operands, specs, scratch=(), limit=16):
    return pl.pallas_call(
        body,
        in_specs=specs,
        out_specs=[WHOLE] * len(out_shapes),
        out_shape=[jax.ShapeDtypeStruct(s, jnp.float32) for s in out_shapes],
        scratch_shapes=list(scratch),
        compiler_params=pltpu.CompilerParams(vmem_limit_bytes=limit * 1024 * 1024),
    )(*operands)


def prepared(pair, spans, after):
    def body(*refs):
        sources = refs[: len(pair)]
        outs = refs[len(pair) + 1 :][: len(spans)]
        buffers = refs[len(pair) + 1 + len(spans) : -1]
        semaphores = refs[-1]
        moves = []
        for i, (start, width) in enumerate(spans):
            for side, source in enumerate(sources):
                move = pltpu.make_async_copy(
                    source.at[:, pl.ds(start, width)],
                    buffers[i].at[pl.ds(side * PIVOTS, PIVOTS), :],
                    semaphores.at[i, side],
                )
                move.start()
                moves.append((i, side, move))
        for i, side, move in moves:
            move.wait()
            rows = slice(side * PIVOTS, (side + 1) * PIVOTS)
            width = spans[i][1]
            step = min(width, 512)
            for at in range(0, width, step):
                high, low = parts(buffers[i][rows, at : at + step])
                outs[i][0, rows, at : at + step] = high
                outs[i][1, rows, at : at + step] = low

    count = len(pair) * PIVOTS
    return pl.pallas_call(
        body,
        in_specs=[FAR] * len(pair) + [FAR],
        out_specs=[WHOLE] * len(spans),
        out_shape=[jax.ShapeDtypeStruct((2, count, width), jnp.bfloat16) for _, width in spans],
        scratch_shapes=[pltpu.VMEM((count, width), jnp.float32) for _, width in spans]
        + [pltpu.SemaphoreType.DMA((len(spans), len(pair)))],
        compiler_params=pltpu.CompilerParams(vmem_limit_bytes=24 * 1024 * 1024),
    )(*pair, after)


def pivot_apply(solved, own, swapped):
    lane = lax.broadcasted_iota(jnp.int32, solved.shape, 1)
    width = solved.shape[1]
    beside = jnp.where(lane % 2 == 0, pltpu.roll(solved, width - 1, 1), pltpu.roll(solved, 1, 1))
    return own * solved + swapped * beside


def pivot_factors(kinds, diagonal, coupling):
    def body(kinds_ref, diagonal_ref, coupling_ref, out_ref):
        width = diagonal_ref.shape[1]
        row = lax.broadcasted_iota(jnp.int32, (width // 2, width), 0)
        col = lax.broadcasted_iota(jnp.int32, (width // 2, width), 1)
        widen = (col // 2 == row).astype(jnp.float32)
        pair = jnp.concatenate(
            [kinds_ref[...].astype(jnp.float32), coupling_ref[...], jnp.zeros((6, width // 2), jnp.float32)], 0
        )
        wide = dot_full(pair, widen)
        is_pair = wide[0:1] > 0.5
        couple = wide[1:2]
        own = jnp.broadcast_to(diagonal_ref[...], (8, width))
        lane = lax.broadcasted_iota(jnp.int32, (8, width), 1)
        other = jnp.where(lane % 2 == 0, pltpu.roll(own, width - 1, 1), pltpu.roll(own, 1, 1))[0:1]
        own = own[0:1]
        determinant = own * other - couple * couple
        out_ref[0:1, :] = jnp.where(is_pair, other / determinant, 1.0 / own)
        out_ref[1:2, :] = jnp.where(is_pair, -couple / determinant, 0.0)

    return call(body, [(2, diagonal.shape[1])], [kinds, diagonal, coupling], [WHOLE] * 3)[0]


def packed_sides(sides, beside):
    def body(sides_ref, beside_ref, out_ref):
        c = lax.axis_index("c")
        mine = pl.ds(pl.multiple_of(c * HALF, 8), HALF)
        theirs = pl.ds(pl.multiple_of((1 - c) * HALF, 8), HALF)
        out_ref[mine] = sides_ref[mine, 2 * PIVOTS :]
        out_ref[theirs] = beside_ref[mine, 2 * PIVOTS :]

    return call(body, [(SIDES, 256)], [sides, beside], [WHOLE] * 2)[0]


def level_zero_forward(first, sides, weights, updates, factors):
    def body(first_ref, sides_ref, weights_ref, updates_ref, factors_ref, sent_ref, weighted_ref):
        gathered = jnp.concatenate([first_ref[q] for q in range(4)], 1)
        solved = product(gathered, weights_ref[0], weights_ref[1], 1)
        weighted_ref[...] = pivot_apply(solved, factors_ref[0:1, :PIVOTS], factors_ref[1:2, :PIVOTS])
        part = product(solved, updates_ref[0], updates_ref[1], 0)
        for c in range(2):
            half = slice(c * HALF, (c + 1) * HALF)
            for x in range(4):
                sent_ref[c * 4 + x, :, :256] = part[half]
                sent_ref[c * 4 + x, :, 256:] = sides_ref[half, PIVOTS : 2 * PIVOTS]

    return call(
        body,
        [(8, HALF, 384), (SIDES, PIVOTS)],
        [first, sides, weights, updates, factors],
        [WHOLE] * 5,
    )


def child_block(level, tables, child, k):
    own_ref, side_ref, own_beside_ref, side_beside_ref = tables
    c = lax.axis_index("c")
    if level == 1:
        return jnp.where(c == child, own_ref[0, k], own_beside_ref[0, k])
    if level == 2:
        sibling = jnp.where(c == 0, side_ref[0, 2 + k], side_beside_ref[0, 2 + k])
        return jnp.where(lax.axis_index("y0") == child, own_ref[0, 2 + k], sibling)
    sibling = jnp.where(c == 0, side_beside_ref[0, 6 + k], side_ref[0, 6 + k])
    return jnp.where(lax.axis_index("y1") == child, own_ref[0, 6 + k], sibling)


def both_factors(level, factors, beside):
    c = lax.axis_index("c")
    at = slice(level * PIVOTS, (level + 1) * PIVOTS)
    return [jnp.concatenate([factors[i : i + 1, at], beside[i : i + 1, at]], 1) for i in range(2)]


def halves(rows):
    return jnp.concatenate([rows[:HALF], rows[HALF:]], 1)


def forward(level, received, sides, tables, weights, updates, factors, partner_factors):
    width = 1 << level
    span = 4 * PIVOTS * width
    chunks = span // 512
    update_len = 2 * PIVOTS * width if level < 3 else 0
    blocks = (2, 4, 8)[level - 1]
    n_sides = len(sides)
    n_updates = 1 if level < 3 else 0

    def body(*refs):
        refs = list(refs)

        def take(count):
            taken, refs[:] = refs[:count], refs[count:]
            return taken

        tables_refs = take(4)
        (received_ref,) = take(1)
        sides_refs = take(n_sides)
        factors_ref, beside_ref, weights_ref = take(3)
        updates_ref = take(n_updates)
        outs = take(2 if level < 3 else 3)
        (b_ref,) = take(1)
        x0, y0, y1 = lax.axis_index("x"), lax.axis_index("y0"), lax.axis_index("y1")
        if level == 1:
            for x in range(4):
                for c in range(2):
                    b_ref[:, (x * 2 + c) * PIVOTS : (x * 2 + c + 1) * PIVOTS] = received_ref[c * 4 + x, :, 256:]
        elif level == 2:
            for flip in range(2):
                for x in range(4):
                    b_ref[:, block_at((x0 ^ x) * 2 + (y0 ^ flip), 256)] = halves(sides_refs[flip][x, :, :PIVOTS])
        else:
            for high in range(2):
                for flip in range(2):
                    for x in range(4):
                        where = block_at((x0 ^ x) * 4 + (y1 ^ high) * 2 + (y0 ^ flip), 256)
                        b_ref[:, where] = halves(sides_refs[high][flip, x])
        for child in range(2):
            if level == 1:
                total = sum(received_ref[child * 4 + x, :, :256] for x in range(4))
            elif level == 2:
                total = sum(received_ref[x * 2 + child] for x in range(4))
            for k in range(blocks):
                if level < 3:
                    piece = total[:, k * BLOCK : (k + 1) * BLOCK]
                else:
                    piece = received_ref[(k // 2) * 4 + child * 2 + k % 2]
                where = block_at(child_block(level, tables_refs, child, k))
                b_ref[:, where] = b_ref[:, where] - piece
        solved = jnp.zeros((HALF, 2 * PIVOTS), jnp.float32)
        for k in range(chunks):
            at = slice(k * 512, (k + 1) * 512)
            solved += product(b_ref[:, at], weights_ref[0, :, at], weights_ref[1, :, at], 1)
        weighted = pivot_apply(solved, *both_factors(level, factors_ref, beside_ref))
        if level < 3:
            outs[1][...] = weighted
            for k in range(update_len // 256):
                at = slice(k * 256, (k + 1) * 256)
                part = product(solved, updates_ref[0][0, :, at], updates_ref[0][1, :, at], 0)
                if level == 1:
                    for i in range(8):
                        outs[0][i, :, at] = part
                else:
                    outs[0][2 * k] = part[:, :BLOCK]
                    outs[0][2 * k + 1] = part[:, BLOCK:]
        else:
            sent_ref, keep_ref, far_ref = outs
            for k in range(chunks):
                at = slice(k * 512, (k + 1) * 512)
                b_ref[:, at] = product(weighted, weights_ref[0, :, at], weights_ref[1, :, at], 0)
            for child in range(2):
                for k in range(8):
                    where = block_at(child_block(3, tables_refs, child, k))
                    sent_ref[(k // 2) * 4 + child * 2 + k % 2] = b_ref[:, where]
            for x in range(4):
                for low in range(2):
                    keep_ref[x, low] = b_ref[:, block_at(x * 4 + y1 * 2 + low, 256)]
                    far_ref[x, low] = b_ref[:, block_at(x * 4 + (1 - y1) * 2 + low, 256)]

    outs = {
        1: [(8, HALF, 512), (HALF, 256)],
        2: [(8, HALF, BLOCK), (HALF, 256)],
        3: [(16, HALF, BLOCK), (4, 2, HALF, 256), (4, 2, HALF, 256)],
    }[level]
    operands = [*tables, received, *sides, factors, partner_factors, weights]
    if level < 3:
        operands.append(updates)
    specs = [SCALARS] * 4 + [WHOLE] * (len(operands) - 4)
    return call(body, outs, operands, specs, [pltpu.VMEM((HALF, span), jnp.float32)])


def backward(level, received, weighted, tables, weights, updates, answers):
    width = 1 << level
    span = 4 * PIVOTS * width
    chunks = span // 512
    update_len = 2 * PIVOTS * width
    blocks = (2, 4)[level - 1]

    def body(*refs):
        refs = list(refs)

        def take(count):
            taken, refs[:] = refs[:count], refs[count:]
            return taken

        tables_refs = take(4)
        received_ref, weighted_ref = take(2)
        answer_refs = take(len(answers))
        weights_ref, updates_ref = take(2)
        outs = take(2 if level == 1 else 3)
        (x_ref,) = take(1)
        target = weighted_ref[...]
        if level == 1:
            total = sum(received_ref[i] for i in range(8))
        for k in range(update_len // 256):
            at = slice(k * 256, (k + 1) * 256)
            if level == 1:
                chosen = total[:, at]
            else:
                chosen = jnp.concatenate([received_ref[2 * k], received_ref[2 * k + 1]], 1)
            target -= product(chosen, updates_ref[0, :, at], updates_ref[1, :, at], 1)
        for k in range(chunks):
            at = slice(k * 512, (k + 1) * 512)
            x_ref[:, at] = product(target, weights_ref[0, :, at], weights_ref[1, :, at], 0)
        for child in range(2):
            for k in range(blocks):
                piece = x_ref[:, block_at(child_block(level, tables_refs, child, k))]
                for x in range(4):
                    outs[0][x * 2 + child, :, k * BLOCK : (k + 1) * BLOCK] = piece
        if level == 1:
            for x in range(4):
                outs[1][x] = x_ref[:, x * 256 : (x + 1) * 256]
        else:
            y0 = lax.axis_index("y0")
            keep_ref, far_ref = outs[1:]
            own_ref, other_ref = answer_refs
            for x in range(4):
                keep_ref[0, x] = x_ref[:, block_at(x * 2 + y0, 256)]
                far_ref[0, x] = x_ref[:, block_at(x * 2 + (1 - y0), 256)]
                keep_ref[1, x] = own_ref[x, y0] + other_ref[x, y0]
                far_ref[1, x] = own_ref[x, 1 - y0] + other_ref[x, 1 - y0]

    outs = [(8, HALF, blocks * BLOCK)]
    outs += [(4, HALF, 256)] if level == 1 else [(2, 4, HALF, 256), (2, 4, HALF, 256)]
    operands = [*tables, received, weighted, *answers, weights, updates]
    specs = [SCALARS] * 4 + [WHOLE] * (len(operands) - 4)
    return call(body, outs, operands, specs, [pltpu.VMEM((HALF, span), jnp.float32)])


def level_zero_backward(received, weighted, weights, updates, nearest, kept, other):
    def body(received_ref, weighted_ref, nearest_ref, kept_ref, other_ref, weights_ref, updates_ref, sent_ref):
        for x in range(4):
            for c in range(2):
                half = slice(c * HALF, (c + 1) * HALF)
                at = slice(c * PIVOTS, (c + 1) * PIVOTS)
                sent_ref[x, half, PIVOTS : 2 * PIVOTS] = nearest_ref[x, :, at]
                for i in range(2):
                    piece = kept_ref[i, x, :, at] + other_ref[i, x, :, at]
                    sent_ref[x, half, (2 + i) * PIVOTS : (3 + i) * PIVOTS] = piece
        chosen = jnp.concatenate([sum(received_ref[x * 2 + c] for x in range(4)) for c in range(2)], 0)
        target = weighted_ref[...] - product(chosen, updates_ref[0], updates_ref[1], 1)
        part = product(target, weights_ref[0], weights_ref[1], 0)
        for q in range(4):
            sent_ref[q, :, :PIVOTS] = part[:, q * PIVOTS : (q + 1) * PIVOTS]

    return call(
        body,
        [(4, SIDES, 512)],
        [received, weighted, nearest, kept, other, weights, updates],
        [WHOLE] * 7,
    )[0]


def summed(received):
    def body(received_ref, out_ref):
        out_ref[...] = (received_ref[0] + received_ref[1]) + (received_ref[2] + received_ref[3])

    return call(body, [(SIDES, 512)], [received], [WHOLE])[0]


def unpacked(total, beside):
    def body(total_ref, beside_ref, out_ref):
        c = lax.axis_index("c")
        mine = pl.ds(pl.multiple_of(c * HALF, 8), HALF)
        theirs = pl.ds(pl.multiple_of((1 - c) * HALF, 8), HALF)
        out_ref[:, :PIVOTS] = total_ref[:, :PIVOTS]
        out_ref[mine, PIVOTS:] = total_ref[mine, PIVOTS:]
        out_ref[theirs, PIVOTS:] = beside_ref[mine, PIVOTS:]

    return call(body, [(SIDES, 512)], [total, beside], [WHOLE] * 2)[0]


def summed_copies(received, count):
    total = jnp.sum(received, 0)
    return jnp.broadcast_to(total[None], (count, *total.shape))


def sibling_tables(targets):
    pairs = []
    for y1 in range(2):
        for y0 in range(2):
            here = y1 * 4 + y0 * 2
            pairs.append((here, y1 * 4 + (1 - y0) * 2))
            pairs.append((here + 1, (1 - y1) * 4 + y0 * 2 + 1))
    side = lax.ppermute(targets, ("y1", "y0", "c"), pairs)
    return [targets, side, with_partner(targets), with_partner(side)]


def per_device(right_side, factor_inverse, update_panel, update_targets, pivot_pairs, pivot_diagonal, pivot_coupling):
    sides = right_side[0, 0]
    inverse = factor_inverse[0, 0]
    update = update_panel[0, 0]
    plane = ("x", "y1", "y0")
    pair = ("x", "y0")

    copies = jnp.broadcast_to(sides[None, :, :PIVOTS], (4, SIDES, PIVOTS))
    first = exchange(copies, ("x",))
    factors = pivot_factors(pivot_pairs[0], pivot_diagonal[0], pivot_coupling[0])
    (weights0,) = prepared([inverse], [(0, 512)], copies)
    (updates0,) = prepared([update], [(0, 256)], copies)
    packed = packed_sides(sides, with_partner(sides))
    inverse_after, update_after, _ = lax.optimization_barrier((inverse, update, packed))
    partner_inverse = with_partner(inverse_after)
    partner_update = with_partner(update_after)
    two = jnp.stack([packed, lax.ppermute(packed, "x", [(0, 1), (1, 0), (2, 3), (3, 2)])])

    sent, weighted0 = level_zero_forward(first, sides, weights0, updates0, factors)
    received = exchange(sent, ("c", "x"))
    partner_factors = with_partner(factors)
    tables = sibling_tables(update_targets)
    near = jnp.concatenate([two, lax.ppermute(two, "x", [(0, 2), (2, 0), (1, 3), (3, 1)])])
    weights1, weights2, weights3 = prepared(
        [inverse, partner_inverse], [(512, 1024), (1536, 2048), (3584, 4096)], sent
    )
    updates1, updates2 = prepared([update, partner_update], [(256, 512), (768, 1024)], sent)
    sent, weighted1 = forward(1, received, [], tables, weights1, updates1, factors, partner_factors)
    far = across(near, "y0")
    near3 = jnp.stack([near[:, :, PIVOTS:], far[:, :, PIVOTS:]])
    received = exchange(sent, pair)
    sent, weighted2 = forward(2, received, [near, far], tables, weights2, updates2, factors, partner_factors)
    far3 = across(near3, "y1")
    received = exchange(summed_copies(exchange(sent, pair), 16), plane)
    sent, kept3, other3 = forward(3, received, [near3, far3], tables, weights3, None, factors, partner_factors)
    other3 = across(other3, "y1")
    received = exchange(summed_copies(exchange(sent, plane), 8), pair)
    sent, kept, other = backward(2, received, weighted2, tables, weights2, updates2, [kept3, other3])
    other = across(other, "y0")
    received = exchange(sent, pair)
    sent, nearest = backward(1, received, weighted1, tables, weights1, updates1, [])
    received = exchange(sent, ("x", "c"))
    sent = level_zero_backward(received, weighted0, weights0, updates0, nearest, kept, other)
    total = summed(exchange(sent, ("x",)))
    return unpacked(total, with_partner(total))[None, None]


def solution(mesh):
    grid = np.array(mesh.devices).reshape(4, 2, 2, 2, 4)
    fine = Mesh(grid, AXES)
    leaf = ("z", "y1", "y0", "c")
    in_specs = (
        P(leaf, "x", None, None),
        P(leaf, "x", None, None),
        P(leaf, "x", None, None),
        P(leaf, None),
        P(leaf, "x", None),
        P(leaf, "x", None),
        P(leaf, "x", None),
    )
    out_specs = P(leaf, "x", None, None)
    return jax.shard_map(per_device, mesh=fine, in_specs=in_specs, out_specs=out_specs, check_vma=False)
```

```python
import jax
import jax.numpy as jnp
import numpy as np
from jax import lax
from jax.experimental import pallas as pl
from jax.experimental.pallas import tpu as pltpu
from jax.sharding import Mesh, PartitionSpec as P

LEVELS = 4
BLOCK = 128
PIVOTS = 128
SIDES = 96
HALF = SIDES // 2
AXES = ("z", "y1", "y0", "c", "x")

exact_mode = lax.Precision.HIGHEST


def parts(value):
    high = value.astype(jnp.bfloat16)
    return high, (value - high.astype(jnp.float32)).astype(jnp.bfloat16)


def product(left, right, side):
    left_high, left_low = parts(left)
    high, low = parts(right)
    dims = (((1,), (side,)), ((), ()))

    def dot(a, b):
        return lax.dot_general(a, b, dims, preferred_element_type=jnp.float32)

    return dot(left_high, high) + (dot(left_high, low) + dot(left_low, high))


def dot_rows(left, right):
    return product(left, right, 1)


def dot_cols(left, right):
    return product(left, right, 0)


def dot_full(left, right):
    return lax.dot_general(
        left, right, (((1,), (0,)), ((), ())), precision=exact_mode, preferred_element_type=jnp.float32
    )


def exchange(value, axes):
    return lax.all_to_all(value, axes, 0, 0, tiled=True)


def with_partner(value):
    return lax.ppermute(value, "c", [(0, 1), (1, 0)])


def across(value, axis):
    return lax.ppermute(value, axis, [(0, 1), (1, 0)])


def block_at(index, size=BLOCK):
    return pl.ds(pl.multiple_of(index * size, size), size)


WHOLE = pl.BlockSpec(memory_space=pltpu.VMEM)
SCALARS = pl.BlockSpec(memory_space=pltpu.SMEM)
FAR = pl.BlockSpec(memory_space=pltpu.HBM)


def far(value):
    return pltpu.with_memory_space_constraint(value, pltpu.HBM)


def call(body, out_shapes, operands, specs, scratch=(), limit=20, out_space=pltpu.HBM):
    return pl.pallas_call(
        body,
        in_specs=specs,
        out_specs=[WHOLE] * len(out_shapes),
        out_shape=[
            out_space(s, jnp.float32) if out_space else jax.ShapeDtypeStruct(s, jnp.float32) for s in out_shapes
        ],
        scratch_shapes=list(scratch),
        compiler_params=pltpu.CompilerParams(vmem_limit_bytes=limit * 1024 * 1024),
    )(*operands)


class Stream:
    def __init__(self, pair, start, width, step, buffer, semaphores):
        self.step, self.buffer, self.moves = step, buffer, []
        for k in range(width // step):
            both = []
            for side, source in enumerate(pair):
                both.append(
                    pltpu.make_async_copy(
                        source.at[:, pl.ds(start + k * step, step)],
                        buffer.at[pl.ds(side * PIVOTS, PIVOTS), pl.ds(k * step, step)],
                        semaphores.at[k, side],
                    )
                )
            self.moves.append(both)

    def start(self):
        for both in self.moves:
            for move in both:
                move.start()

    def wait(self, k):
        for move in self.moves[k]:
            move.wait()

    def at(self, k):
        return self.buffer[:, k * self.step : (k + 1) * self.step]


def stream_scratch(pair, width, step):
    return [pltpu.VMEM((pair * PIVOTS, width), jnp.float32), pltpu.SemaphoreType.DMA((width // step, pair))]


def pivot_apply(solved, own, swapped):
    lane = lax.broadcasted_iota(jnp.int32, solved.shape, 1)
    width = solved.shape[1]
    beside = jnp.where(lane % 2 == 0, pltpu.roll(solved, width - 1, 1), pltpu.roll(solved, 1, 1))
    return own * solved + swapped * beside


def pivot_factors(kinds, diagonal, coupling):
    def body(kinds_ref, diagonal_ref, coupling_ref, out_ref):
        width = diagonal_ref.shape[1]
        row = lax.broadcasted_iota(jnp.int32, (width // 2, width), 0)
        col = lax.broadcasted_iota(jnp.int32, (width // 2, width), 1)
        widen = (col // 2 == row).astype(jnp.float32)
        pair = jnp.concatenate(
            [kinds_ref[...].astype(jnp.float32), coupling_ref[...], jnp.zeros((6, width // 2), jnp.float32)], 0
        )
        wide = dot_full(pair, widen)
        is_pair = wide[0:1] > 0.5
        couple = wide[1:2]
        own = jnp.broadcast_to(diagonal_ref[...], (8, width))
        lane = lax.broadcasted_iota(jnp.int32, (8, width), 1)
        other = jnp.where(lane % 2 == 0, pltpu.roll(own, width - 1, 1), pltpu.roll(own, 1, 1))[0:1]
        own = own[0:1]
        determinant = own * other - couple * couple
        out_ref[0:1, :] = jnp.where(is_pair, other / determinant, 1.0 / own)
        out_ref[1:2, :] = jnp.where(is_pair, -couple / determinant, 0.0)

    operands = [far(kinds), far(diagonal), far(coupling)]
    return call(body, [(2, diagonal.shape[1])], operands, [WHOLE] * 3)[0]


def packed_sides(sides, beside):
    def body(sides_ref, beside_ref, out_ref):
        c = lax.axis_index("c")
        mine = pl.ds(pl.multiple_of(c * HALF, 8), HALF)
        theirs = pl.ds(pl.multiple_of((1 - c) * HALF, 8), HALF)
        own = sides_ref[mine, PIVOTS:]
        other = beside_ref[mine, PIVOTS:]
        for i in range(4):
            out_ref[i, :, :PIVOTS] = sides_ref[:, :PIVOTS]
            out_ref[i, mine, PIVOTS:] = own
            out_ref[i, theirs, PIVOTS:] = other

    return call(body, [(4, SIDES, 512)], [far(sides), beside], [WHOLE] * 2)[0]


def level_zero_forward(first, inverse, update, factors):
    def body(first_ref, inverse_ref, update_ref, factors_ref, sent_ref, weighted_ref, one_ref, upper_ref, *scratch):
        weights = Stream([inverse_ref], 0, 512, 512, *scratch[:2])
        updates = Stream([update_ref], 0, 256, 256, *scratch[2:])
        weights.start()
        updates.start()
        for q in range(4):
            one_ref[q] = first_ref[q, :, PIVOTS : 2 * PIVOTS]
            upper_ref[q] = first_ref[q, :, 2 * PIVOTS :]
        gathered = jnp.concatenate([first_ref[q, :, :PIVOTS] for q in range(4)], 1)
        weights.wait(0)
        solved = dot_rows(gathered, weights.at(0))
        weighted_ref[...] = pivot_apply(solved, factors_ref[0:1, :PIVOTS], factors_ref[1:2, :PIVOTS])
        updates.wait(0)
        part = dot_cols(solved, updates.at(0))
        for c in range(2):
            for x in range(4):
                sent_ref[c * 4 + x] = part[c * HALF : (c + 1) * HALF]

    return call(
        body,
        [(8, HALF, 256), (SIDES, PIVOTS), (4, SIDES, PIVOTS), (4, SIDES, 256)],
        [first, far(inverse), far(update), far(factors)],
        [WHOLE, FAR, FAR, WHOLE],
        stream_scratch(1, 512, 512) + stream_scratch(1, 256, 256),
    )


def child_block(level, tables, child, k):
    own_ref, side_ref, own_beside_ref, side_beside_ref = tables
    c = lax.axis_index("c")
    if level == 1:
        return jnp.where(c == child, own_ref[0, k], own_beside_ref[0, k])
    if level == 2:
        sibling = jnp.where(c == 0, side_ref[0, 2 + k], side_beside_ref[0, 2 + k])
        return jnp.where(lax.axis_index("y0") == child, own_ref[0, 2 + k], sibling)
    sibling = jnp.where(c == 0, side_beside_ref[0, 6 + k], side_ref[0, 6 + k])
    return jnp.where(lax.axis_index("y1") == child, own_ref[0, 6 + k], sibling)


def both_factors(level, factors, beside):
    c = lax.axis_index("c")
    at = slice(level * PIVOTS, (level + 1) * PIVOTS)
    return [jnp.concatenate([factors[i : i + 1, at], beside[i : i + 1, at]], 1) for i in range(2)]


def halves(rows):
    return jnp.concatenate([rows[:HALF], rows[HALF:]], 1)


def forward(level, received, sides, tables, weights_pair, update_pair, factors, partner_factors):
    width = 1 << level
    span = 4 * PIVOTS * width
    chunks = span // 512
    start = 4 * PIVOTS * (width - 1)
    update_len = 2 * PIVOTS * width if level < 3 else 0
    update_start = 2 * PIVOTS * (width - 1)
    blocks = (2, 4, 8)[level - 1]
    n_sides = len(sides)
    n_updates = 2 if level < 3 else 0

    def body(*refs):
        refs = list(refs)

        def take(count):
            taken, refs[:] = refs[:count], refs[count:]
            return taken

        tables_refs = take(4)
        (received_ref,) = take(1)
        sides_refs = take(n_sides)
        factors_ref, beside_ref = take(2)
        inverse_refs = take(2)
        update_refs = take(n_updates)
        outs = take(2 if level == 2 else 3)
        (b_ref,) = take(1)
        weights = Stream(inverse_refs, start, span, 512, *take(2))
        weights.start()
        if level < 3:
            updates = Stream(update_refs, update_start, update_len, 256, *take(2))
            updates.start()
        y0, y1 = lax.axis_index("y0"), lax.axis_index("y1")
        if level == 1:
            for x in range(4):
                b_ref[:, x * 256 : (x + 1) * 256] = halves(sides_refs[0][x])
            near, far = sides_refs[1], sides_refs[2]
            outs[2][0] = near[:, :, PIVOTS:]
            outs[2][1] = far[:, :, PIVOTS:]
        elif level == 2:
            for flip in range(2):
                for x in range(4):
                    b_ref[:, block_at(x * 2 + (y0 ^ flip), 256)] = halves(sides_refs[flip][x, :, :PIVOTS])
        else:
            for high in range(2):
                for flip in range(2):
                    for x in range(4):
                        where = block_at(x * 4 + (y1 ^ high) * 2 + (y0 ^ flip), 256)
                        b_ref[:, where] = halves(sides_refs[high][flip, x])
        for child in range(2):
            if level == 1:
                total = sum(received_ref[child * 4 + x] for x in range(4))
            elif level == 2:
                total = sum(received_ref[x * 2 + child] for x in range(4))
            for k in range(blocks):
                if level < 3:
                    piece = total[:, k * BLOCK : (k + 1) * BLOCK]
                else:
                    piece = received_ref[(k // 2) * 4 + child * 2 + k % 2]
                where = block_at(child_block(level, tables_refs, child, k))
                b_ref[:, where] = b_ref[:, where] - piece
        solved = jnp.zeros((HALF, 2 * PIVOTS), jnp.float32)
        for k in range(chunks):
            weights.wait(k)
            solved += dot_rows(b_ref[:, k * 512 : (k + 1) * 512], weights.at(k))
        weighted = pivot_apply(solved, *both_factors(level, factors_ref, beside_ref))
        if level < 3:
            outs[1][...] = weighted
            for k in range(update_len // 256):
                updates.wait(k)
                part = dot_cols(solved, updates.at(k))
                if level == 1:
                    for i in range(8):
                        outs[0][i, :, k * 256 : (k + 1) * 256] = part
                else:
                    outs[0][2 * k] = part[:, :BLOCK]
                    outs[0][2 * k + 1] = part[:, BLOCK:]
        else:
            sent_ref, keep_ref, far_ref = outs
            for k in range(chunks):
                b_ref[:, k * 512 : (k + 1) * 512] = dot_cols(weighted, weights.at(k))
            for child in range(2):
                for k in range(8):
                    where = block_at(child_block(3, tables_refs, child, k))
                    sent_ref[(k // 2) * 4 + child * 2 + k % 2] = b_ref[:, where]
            for x in range(4):
                for low in range(2):
                    keep_ref[x, low] = b_ref[:, block_at(x * 4 + y1 * 2 + low, 256)]
                    far_ref[x, low] = b_ref[:, block_at(x * 4 + (1 - y1) * 2 + low, 256)]

    outs = {
        1: [(8, HALF, 512), (HALF, 256), (2, 4, SIDES, PIVOTS)],
        2: [(8, HALF, BLOCK), (HALF, 256)],
        3: [(16, HALF, BLOCK), (4, 2, HALF, 256), (4, 2, HALF, 256)],
    }[level]
    scratch = [pltpu.VMEM((HALF, span), jnp.float32)] + stream_scratch(2, span, 512)
    operands = [*map(far, tables), received, *map(far, sides[: 3 if level < 3 else 1]), *sides[3 if level < 3 else 1 :], far(factors), far(partner_factors)]
    operands += map(far, weights_pair)
    specs = [SCALARS] * 4 + [WHOLE] * (3 + n_sides) + [FAR] * 2
    if level < 3:
        scratch += stream_scratch(2, update_len, 256)
        operands += map(far, update_pair)
        specs += [FAR] * 2
    return call(body, outs, operands, specs, scratch, 20)


def backward(level, received, weighted, tables, weights_pair, update_pair, answers):
    width = 1 << level
    span = 4 * PIVOTS * width
    chunks = span // 512
    start = 4 * PIVOTS * (width - 1)
    update_len = 2 * PIVOTS * width
    update_start = 2 * PIVOTS * (width - 1)
    blocks = (2, 4)[level - 1]

    def body(*refs):
        refs = list(refs)

        def take(count):
            taken, refs[:] = refs[:count], refs[count:]
            return taken

        tables_refs = take(4)
        received_ref, weighted_ref = take(2)
        answer_refs = take(len(answers))
        inverse_refs = take(2)
        update_refs = take(2)
        outs = take(2 if level == 1 else 3)
        (x_ref,) = take(1)
        weights = Stream(inverse_refs, start, span, 512, *take(2))
        updates = Stream(update_refs, update_start, update_len, 256, *take(2))
        updates.start()
        weights.start()
        target = weighted_ref[...]
        if level == 1:
            total = sum(received_ref[i] for i in range(8))
        for k in range(update_len // 256):
            if level == 1:
                chosen = total[:, k * 256 : (k + 1) * 256]
            else:
                chosen = jnp.concatenate([received_ref[2 * k], received_ref[2 * k + 1]], 1)
            updates.wait(k)
            target -= dot_rows(chosen, updates.at(k))
        for k in range(chunks):
            weights.wait(k)
            x_ref[:, k * 512 : (k + 1) * 512] = dot_cols(target, weights.at(k))
        for child in range(2):
            for k in range(blocks):
                piece = x_ref[:, block_at(child_block(level, tables_refs, child, k))]
                for x in range(4):
                    outs[0][x * 2 + child, :, k * BLOCK : (k + 1) * BLOCK] = piece
        if level == 1:
            for x in range(4):
                outs[1][x] = x_ref[:, x * 256 : (x + 1) * 256]
        else:
            y0 = lax.axis_index("y0")
            keep_ref, far_ref = outs[1:]
            own_ref, other_ref = answer_refs
            for x in range(4):
                keep_ref[0, x] = x_ref[:, block_at(x * 2 + y0, 256)]
                far_ref[0, x] = x_ref[:, block_at(x * 2 + (1 - y0), 256)]
                keep_ref[1, x] = own_ref[x, y0] + other_ref[x, y0]
                far_ref[1, x] = own_ref[x, 1 - y0] + other_ref[x, 1 - y0]

    outs = [(8, HALF, blocks * BLOCK)]
    outs += [(4, HALF, 256)] if level == 1 else [(2, 4, HALF, 256), (2, 4, HALF, 256)]
    scratch = [pltpu.VMEM((HALF, span), jnp.float32)]
    scratch += stream_scratch(2, span, 512) + stream_scratch(2, update_len, 256)
    operands = [*map(far, tables), received, far(weighted), *map(far, answers[:1]), *answers[1:]]
    operands += map(far, [*weights_pair, *update_pair])
    specs = [SCALARS] * 4 + [WHOLE] * (2 + len(answers)) + [FAR] * 4
    return call(body, outs, operands, specs, scratch, 20)


def level_zero_backward(received, weighted, inverse, update, nearest, kept, other):
    def body(received_ref, weighted_ref, nearest_ref, kept_ref, other_ref, inverse_ref, update_ref, sent_ref, *scratch):
        weights = Stream([inverse_ref], 0, 512, 512, *scratch[:2])
        updates = Stream([update_ref], 0, 256, 256, *scratch[2:])
        updates.start()
        weights.start()
        for x in range(4):
            for c in range(2):
                half = slice(c * HALF, (c + 1) * HALF)
                at = slice(c * PIVOTS, (c + 1) * PIVOTS)
                sent_ref[x, half, PIVOTS : 2 * PIVOTS] = nearest_ref[x, :, at]
                for i in range(2):
                    piece = kept_ref[i, x, :, at] + other_ref[i, x, :, at]
                    sent_ref[x, half, (2 + i) * PIVOTS : (3 + i) * PIVOTS] = piece
        chosen = jnp.concatenate([sum(received_ref[x * 2 + c] for x in range(4)) for c in range(2)], 0)
        updates.wait(0)
        target = weighted_ref[...] - dot_rows(chosen, updates.at(0))
        weights.wait(0)
        part = dot_cols(target, weights.at(0))
        for q in range(4):
            sent_ref[q, :, :PIVOTS] = part[:, q * PIVOTS : (q + 1) * PIVOTS]

    return call(
        body,
        [(4, SIDES, 512)],
        [received, *map(far, [weighted, nearest, kept]), other, far(inverse), far(update)],
        [WHOLE] * 5 + [FAR] * 2,
        stream_scratch(1, 512, 512) + stream_scratch(1, 256, 256),
    )[0]


def summed(received):
    def body(received_ref, out_ref):
        out_ref[...] = (received_ref[0] + received_ref[1]) + (received_ref[2] + received_ref[3])

    return call(body, [(SIDES, 512)], [received], [WHOLE], out_space=None)[0]


def unpacked(total, beside):
    def body(total_ref, beside_ref, out_ref):
        c = lax.axis_index("c")
        mine = pl.ds(pl.multiple_of(c * HALF, 8), HALF)
        theirs = pl.ds(pl.multiple_of((1 - c) * HALF, 8), HALF)
        out_ref[:, :PIVOTS] = total_ref[:, :PIVOTS]
        out_ref[mine, PIVOTS:] = total_ref[mine, PIVOTS:]
        out_ref[theirs, PIVOTS:] = beside_ref[mine, PIVOTS:]

    return call(body, [(SIDES, 512)], [total, beside], [WHOLE] * 2, out_space=None)[0]


def summed_copies(received, count):
    total = jnp.sum(received, 0)
    return jnp.broadcast_to(total[None], (count, *total.shape))


def sibling_tables(targets):
    pairs = []
    for y1 in range(2):
        for y0 in range(2):
            here = y1 * 4 + y0 * 2
            pairs.append((here, y1 * 4 + (1 - y0) * 2))
            pairs.append((here + 1, (1 - y1) * 4 + y0 * 2 + 1))
    side = lax.ppermute(targets, ("y1", "y0", "c"), pairs)
    return [targets, side, with_partner(targets), with_partner(side)]


def per_device(right_side, factor_inverse, update_panel, update_targets, pivot_pairs, pivot_diagonal, pivot_coupling):
    sides = right_side[0, 0]
    inverse = factor_inverse[0, 0]
    update = update_panel[0, 0]
    plane = ("x", "y1", "y0")
    pair = ("x", "y0")

    packed = packed_sides(sides, with_partner(sides))
    first = exchange(packed, ("x",))
    tables = sibling_tables(update_targets)
    factors = pivot_factors(pivot_pairs[0], pivot_diagonal[0], pivot_coupling[0])
    partner_factors = with_partner(factors)
    inverse_after, update_after, _ = lax.optimization_barrier((inverse, update, packed))
    weights_pair = [inverse, with_partner(inverse_after)]
    update_pair = [update, with_partner(update_after)]

    sent, weighted0, sides1, near = level_zero_forward(first, inverse, update, factors)
    far_side = across(near, "y0")
    received = exchange(sent, ("c", "x"))
    sent, weighted1, near3 = forward(
        1, received, [sides1, near, far_side], tables, weights_pair, update_pair, factors, partner_factors
    )
    far3 = across(near3, "y1")
    received = exchange(sent, pair)
    sent, weighted2 = forward(2, received, [near, far_side], tables, weights_pair, update_pair, factors, partner_factors)
    received = exchange(summed_copies(exchange(sent, pair), 16), plane)
    sent, kept3, other3 = forward(
        3, received, [near3, far3], tables, weights_pair, None, factors, partner_factors
    )
    other3 = across(other3, "y1")
    received = exchange(summed_copies(exchange(sent, plane), 8), pair)
    sent, kept, other = backward(2, received, weighted2, tables, weights_pair, update_pair, [kept3, other3])
    other = across(other, "y0")
    received = exchange(sent, pair)
    sent, nearest = backward(1, received, weighted1, tables, weights_pair, update_pair, [])
    received = exchange(sent, ("x", "c"))
    sent = level_zero_backward(received, weighted0, inverse, update, nearest, kept, other)
    total = summed(exchange(sent, ("x",)))
    return unpacked(total, with_partner(total))[None, None]


def solution(mesh):
    grid = np.array(mesh.devices).reshape(4, 2, 2, 2, 4)
    fine = Mesh(grid, AXES)
    leaf = ("z", "y1", "y0", "c")
    in_specs = (
        P(leaf, "x", None, None),
        P(leaf, "x", None, None),
        P(leaf, "x", None, None),
        P(leaf, None),
        P(leaf, "x", None),
        P(leaf, "x", None),
        P(leaf, "x", None),
    )
    out_specs = P(leaf, "x", None, None)
    return jax.shard_map(per_device, mesh=fine, in_specs=in_specs, out_specs=out_specs, check_vma=False)
```

```python
import jax
import jax.numpy as jnp
import numpy as np
from jax import lax
from jax.experimental import pallas as pl
from jax.experimental.pallas import tpu as pltpu
from jax.sharding import Mesh, PartitionSpec as P

LEVELS = 4
BLOCK = 128
PIVOTS = 128
SIDES = 96
HALF = SIDES // 2
AXES = ("z", "y1", "y0", "c", "x")

exact_mode = lax.Precision.HIGHEST


def parts(value):
    high = value.astype(jnp.bfloat16)
    return high, (value - high.astype(jnp.float32)).astype(jnp.bfloat16)


def product(left, high, low, side):
    left_high, left_low = parts(left)
    dims = (((1,), (side,)), ((), ()))

    def dot(a, b):
        return lax.dot_general(a, b, dims, preferred_element_type=jnp.float32)

    return dot(left_high, high) + (dot(left_high, low) + dot(left_low, high))


def dot_full(left, right):
    return lax.dot_general(
        left, right, (((1,), (0,)), ((), ())), precision=exact_mode, preferred_element_type=jnp.float32
    )


def exchange(value, axes):
    return lax.all_to_all(value, axes, 0, 0, tiled=True)


def with_partner(value):
    return lax.ppermute(value, "c", [(0, 1), (1, 0)])


def across(value, axis):
    return lax.ppermute(value, axis, [(0, 1), (1, 0)])


def block_at(index, size=BLOCK):
    return pl.ds(pl.multiple_of(index * size, size), size)


WHOLE = pl.BlockSpec(memory_space=pltpu.VMEM)
SCALARS = pl.BlockSpec(memory_space=pltpu.SMEM)
FAR = pl.BlockSpec(memory_space=pltpu.HBM)


def far(value):
    return pltpu.with_memory_space_constraint(value, pltpu.HBM)


def close(value):
    return pltpu.with_memory_space_constraint(value, pltpu.VMEM)


def call(body, out_shapes, operands, specs, scratch=(), limit=20, spaces=None):
    return pl.pallas_call(
        body,
        in_specs=specs,
        out_specs=[FAR if k == "H" else WHOLE for k in spaces or "-" * len(out_shapes)],
        out_shape=[
            {"H": pltpu.HBM, "h": pltpu.HBM, "v": pltpu.VMEM, "-": jax.ShapeDtypeStruct}[k](s, jnp.float32)
            for s, k in zip(out_shapes, spaces or "-" * len(out_shapes))
        ],
        scratch_shapes=list(scratch),
        compiler_params=pltpu.CompilerParams(vmem_limit_bytes=limit * 1024 * 1024),
    )(*operands)


def prepared(pair, spans, after, space=pltpu.HBM):
    def body(*refs):
        sources = refs[: len(pair)]
        outs = refs[len(pair) + 1 :][: len(spans)]
        buffers = refs[len(pair) + 1 + len(spans) : -1]
        semaphores = refs[-1]
        moves = []
        for i, (start, width) in enumerate(spans):
            for side, source in enumerate(sources):
                move = pltpu.make_async_copy(
                    source.at[:, pl.ds(start, width)],
                    buffers[i].at[pl.ds(side * PIVOTS, PIVOTS), :],
                    semaphores.at[i, side],
                )
                move.start()
                moves.append((i, side, move))
        for i, side, move in moves:
            move.wait()
            rows = slice(side * PIVOTS, (side + 1) * PIVOTS)
            width = spans[i][1]
            step = min(width, 512)
            for at in range(0, width, step):
                high, low = parts(buffers[i][rows, at : at + step])
                outs[i][0, rows, at : at + step] = high
                outs[i][1, rows, at : at + step] = low

    count = len(pair) * PIVOTS
    return pl.pallas_call(
        body,
        in_specs=[FAR] * len(pair) + [FAR],
        out_specs=[WHOLE] * len(spans),
        out_shape=[space((2, count, width), jnp.bfloat16) for _, width in spans],
        scratch_shapes=[pltpu.VMEM((count, width), jnp.float32) for _, width in spans]
        + [pltpu.SemaphoreType.DMA((len(spans), len(pair)))],
        compiler_params=pltpu.CompilerParams(vmem_limit_bytes=24 * 1024 * 1024),
    )(*map(far, pair), after)


def pivot_apply(solved, own, swapped):
    lane = lax.broadcasted_iota(jnp.int32, solved.shape, 1)
    width = solved.shape[1]
    beside = jnp.where(lane % 2 == 0, pltpu.roll(solved, width - 1, 1), pltpu.roll(solved, 1, 1))
    return own * solved + swapped * beside


def pivot_factors(kinds, diagonal, coupling):
    def body(kinds_ref, diagonal_ref, coupling_ref, out_ref):
        width = diagonal_ref.shape[1]
        row = lax.broadcasted_iota(jnp.int32, (width // 2, width), 0)
        col = lax.broadcasted_iota(jnp.int32, (width // 2, width), 1)
        widen = (col // 2 == row).astype(jnp.float32)
        pair = jnp.concatenate(
            [kinds_ref[...].astype(jnp.float32), coupling_ref[...], jnp.zeros((6, width // 2), jnp.float32)], 0
        )
        wide = dot_full(pair, widen)
        is_pair = wide[0:1] > 0.5
        couple = wide[1:2]
        own = jnp.broadcast_to(diagonal_ref[...], (8, width))
        lane = lax.broadcasted_iota(jnp.int32, (8, width), 1)
        other = jnp.where(lane % 2 == 0, pltpu.roll(own, width - 1, 1), pltpu.roll(own, 1, 1))[0:1]
        own = own[0:1]
        determinant = own * other - couple * couple
        out_ref[0:1, :] = jnp.where(is_pair, other / determinant, 1.0 / own)
        out_ref[1:2, :] = jnp.where(is_pair, -couple / determinant, 0.0)

    operands = [far(kinds), far(diagonal), far(coupling)]
    return call(body, [(2, diagonal.shape[1])], operands, [WHOLE] * 3, spaces="v")[0]


def packed_sides(sides, beside):
    def body(sides_ref, beside_ref, out_ref):
        c = lax.axis_index("c")
        mine = pl.ds(pl.multiple_of(c * HALF, 8), HALF)
        theirs = pl.ds(pl.multiple_of((1 - c) * HALF, 8), HALF)
        own = sides_ref[mine, PIVOTS:]
        other = beside_ref[mine, PIVOTS:]
        for i in range(4):
            out_ref[i, :, :PIVOTS] = sides_ref[:, :PIVOTS]
            out_ref[i, mine, PIVOTS:] = own
            out_ref[i, theirs, PIVOTS:] = other

    return call(body, [(4, SIDES, 512)], [far(sides), beside], [WHOLE] * 2, spaces="h")[0]


class Moves:
    def __init__(self, semaphores):
        self.semaphores, self.started = semaphores, []

    def start(self, source, target):
        move = pltpu.make_async_copy(source, target, self.semaphores.at[len(self.started)])
        move.start()
        self.started.append(move)
        return move

    def columns(self, source, target, step):
        width = source.shape[2]
        spans = [pl.ds(at, step) for at in range(0, width, step)]
        return [self.start(source.at[:, :, span], target.at[:, :, span]) for span in spans]


def finish(moves):
    for move in moves:
        move.wait()


def level_zero_forward(first, weights, updates, factors):
    def body(first_ref, weights_ref, updates_ref, factors_ref, *refs):
        sent_ref, weighted_ref, one_ref, upper_ref, part_ref, own_ref, semaphores = refs
        moves = Moves(semaphores)
        leaving = [
            moves.start(first_ref.at[:, :, pl.ds(PIVOTS, PIVOTS)], one_ref),
            moves.start(first_ref.at[:, :, pl.ds(2 * PIVOTS, 2 * PIVOTS)], upper_ref),
        ]
        gathered = jnp.concatenate([first_ref[q, :, :PIVOTS] for q in range(4)], 1)
        solved = product(gathered, weights_ref[0], weights_ref[1], 1)
        part_ref[...] = product(solved, updates_ref[0], updates_ref[1], 0)
        for c in range(2):
            for x in range(4):
                leaving.append(moves.start(part_ref.at[pl.ds(c * HALF, HALF)], sent_ref.at[c * 4 + x]))
        own_ref[...] = pivot_apply(solved, factors_ref[0:1, :PIVOTS], factors_ref[1:2, :PIVOTS])
        leaving.append(moves.start(own_ref, weighted_ref))
        finish(leaving)

    return call(
        body,
        [(8, HALF, 256), (SIDES, PIVOTS), (4, SIDES, PIVOTS), (4, SIDES, 256)],
        [close(first), close(weights), close(updates), close(factors)],
        [WHOLE] * 4,
        [
            pltpu.VMEM((SIDES, 256), jnp.float32),
            pltpu.VMEM((SIDES, PIVOTS), jnp.float32),
            pltpu.SemaphoreType.DMA((16,)),
        ],
        spaces="HHHH",
    )


def child_block(level, tables, child, k):
    own_ref, side_ref, own_beside_ref, side_beside_ref = tables
    c = lax.axis_index("c")
    if level == 1:
        return jnp.where(c == child, own_ref[0, k], own_beside_ref[0, k])
    if level == 2:
        sibling = jnp.where(c == 0, side_ref[0, 2 + k], side_beside_ref[0, 2 + k])
        return jnp.where(lax.axis_index("y0") == child, own_ref[0, 2 + k], sibling)
    sibling = jnp.where(c == 0, side_beside_ref[0, 6 + k], side_ref[0, 6 + k])
    return jnp.where(lax.axis_index("y1") == child, own_ref[0, 6 + k], sibling)


def both_factors(level, factors, beside):
    c = lax.axis_index("c")
    at = slice(level * PIVOTS, (level + 1) * PIVOTS)
    return [jnp.concatenate([factors[i : i + 1, at], beside[i : i + 1, at]], 1) for i in range(2)]


def halves(rows):
    return jnp.concatenate([rows[:HALF], rows[HALF:]], 1)


def forward(level, received, sides, tables, weights, updates, factors, partner_factors):
    width = 1 << level
    span = 4 * PIVOTS * width
    chunks = span // 512
    update_len = 2 * PIVOTS * width if level < 3 else 0
    blocks = (2, 4, 8)[level - 1]
    n_sides = len(sides)
    n_updates = 1 if level < 3 else 0
    n_outs = (3, 2, 3)[level - 1]

    def body(*refs):
        refs = list(refs)

        def take(count):
            taken, refs[:] = refs[:count], refs[count:]
            return taken

        tables_refs = take(4)
        received_ref, factors_ref, beside_ref = take(3)
        sides_refs = take(n_sides)
        (weights_far,) = take(1)
        updates_far = take(n_updates)
        outs = take(n_outs)
        semaphores, b_ref, own_ref, weights_ref = take(4)
        moves = Moves(semaphores)
        x0, y0, y1 = lax.axis_index("x"), lax.axis_index("y0"), lax.axis_index("y1")

        arriving, leaving = [], []

        def bring(source, block):
            for c in range(2):
                arriving.append(moves.start(source.at[pl.ds(c * HALF, HALF)], b_ref.at[:, block_at(block * 2 + c)]))

        if level == 1:
            for x in range(4):
                bring(sides_refs[0].at[x], x)
        elif level == 2:
            for flip in range(2):
                for x in range(4):
                    bring(sides_refs[flip].at[x, :, pl.ds(0, PIVOTS)], x * 2 + (y0 ^ flip))
        else:
            for high in range(2):
                for flip in range(2):
                    for x in range(4):
                        bring(sides_refs[high].at[flip, x], x * 4 + (y1 ^ high) * 2 + (y0 ^ flip))
        columns = moves.columns(weights_far, weights_ref, 512)
        if level < 3:
            updates_ref, part_ref = refs
            update_columns = moves.columns(updates_far[0], updates_ref, 256)
        if level == 1:
            for flip in range(2):
                leaving.append(moves.start(sides_refs[1 + flip].at[:, :, pl.ds(PIVOTS, PIVOTS)], outs[2].at[flip]))
        totals = [None, None]
        for child in range(2):
            if level == 1:
                totals[child] = sum(received_ref[child * 4 + x] for x in range(4))
            elif level == 2:
                totals[child] = sum(received_ref[x * 2 + child] for x in range(4))
        finish(arriving)
        for child in range(2):
            for k in range(blocks):
                if level < 3:
                    piece = totals[child][:, k * BLOCK : (k + 1) * BLOCK]
                else:
                    piece = received_ref[(k // 2) * 4 + child * 2 + k % 2]
                where = block_at(child_block(level, tables_refs, child, k))
                b_ref[:, where] = b_ref[:, where] - piece
        solved = jnp.zeros((HALF, 2 * PIVOTS), jnp.float32)
        for k in range(chunks):
            columns[k].wait()
            at = slice(k * 512, (k + 1) * 512)
            solved += product(b_ref[:, at], weights_ref[0, :, at], weights_ref[1, :, at], 1)
        weighted = pivot_apply(solved, *both_factors(level, factors_ref, beside_ref))
        if level < 3:
            own_ref[...] = weighted
            leaving.append(moves.start(own_ref, outs[1]))
            for k in range(update_len // 256):
                update_columns[k].wait()
                at = slice(k * 256, (k + 1) * 256)
                part_ref[:, at] = product(solved, updates_ref[0, :, at], updates_ref[1, :, at], 0)
            for i in range(8):
                source = part_ref if level == 1 else part_ref.at[:, pl.ds(i * BLOCK, BLOCK)]
                leaving.append(moves.start(source, outs[0].at[i]))
        else:
            sent_ref, keep_ref, beyond_ref = outs
            for k in range(chunks):
                at = slice(k * 512, (k + 1) * 512)
                b_ref[:, at] = product(weighted, weights_ref[0, :, at], weights_ref[1, :, at], 0)
            for child in range(2):
                for k in range(8):
                    where = block_at(child_block(3, tables_refs, child, k))
                    leaving.append(
                        moves.start(b_ref.at[:, where], sent_ref.at[(k // 2) * 4 + child * 2 + k % 2])
                    )
            for out, bit in ((beyond_ref, 1 - y1), (keep_ref, y1)):
                for x in range(4):
                    for low in range(2):
                        where = block_at(x * 4 + bit * 2 + low, 256)
                        leaving.append(moves.start(b_ref.at[:, where], out.at[x, low]))
        finish(leaving)

    outs = {
        1: [(8, HALF, 512), (HALF, 256), (2, 4, SIDES, PIVOTS)],
        2: [(8, HALF, BLOCK), (HALF, 256)],
        3: [(16, HALF, BLOCK), (4, 2, HALF, 256), (4, 2, HALF, 256)],
    }[level]
    operands = [*map(far, tables), received, close(factors), close(partner_factors)]
    operands += map(far, [*sides, weights] + ([updates] if level < 3 else []))
    specs = [SCALARS] * 4 + [WHOLE] * 3 + [FAR] * (len(operands) - 7)
    scratch = [
        pltpu.SemaphoreType.DMA((80,)),
        pltpu.VMEM((HALF, span), jnp.float32),
        pltpu.VMEM((HALF, 256), jnp.float32),
        pltpu.VMEM((2, 256, span), jnp.bfloat16),
    ]
    if level < 3:
        scratch += [pltpu.VMEM((2, 256, update_len), jnp.bfloat16), pltpu.VMEM((HALF, update_len), jnp.float32)]
    return call(body, outs, operands, specs, scratch, spaces="H" * n_outs)


def backward(level, received, weighted, tables, weights, updates, answers):
    width = 1 << level
    span = 4 * PIVOTS * width
    chunks = span // 512
    update_len = 2 * PIVOTS * width
    blocks = (2, 4)[level - 1]
    n_answers = len(answers)
    n_outs = (2, 3)[level - 1]

    def body(*refs):
        refs = list(refs)

        def take(count):
            taken, refs[:] = refs[:count], refs[count:]
            return taken

        tables_refs = take(4)
        (received_ref,) = take(1)
        weighted_far, weights_far, updates_far = take(3)
        answers_far = take(n_answers)
        outs = take(n_outs)
        semaphores, x_ref, weighted_ref, weights_ref, updates_ref, pieces_ref = take(6)
        moves = Moves(semaphores)
        arriving = moves.start(weighted_far, weighted_ref)
        update_columns = moves.columns(updates_far, updates_ref, 256)
        columns = moves.columns(weights_far, weights_ref, 512)
        leaving = []
        if level == 2:
            own_ref, other_ref, sums_ref = refs
            both = [moves.start(answers_far[0], own_ref), moves.start(answers_far[1], other_ref)]
        if level == 1:
            total = sum(received_ref[i] for i in range(8))
        arriving.wait()
        target = weighted_ref[...]
        for k in range(update_len // 256):
            at = slice(k * 256, (k + 1) * 256)
            if level == 1:
                chosen = total[:, at]
            else:
                chosen = jnp.concatenate([received_ref[2 * k], received_ref[2 * k + 1]], 1)
            update_columns[k].wait()
            target -= product(chosen, updates_ref[0, :, at], updates_ref[1, :, at], 1)
        for k in range(chunks):
            columns[k].wait()
            at = slice(k * 512, (k + 1) * 512)
            x_ref[:, at] = product(target, weights_ref[0, :, at], weights_ref[1, :, at], 0)
        for child in range(2):
            for k in range(blocks):
                where = block_at(child_block(level, tables_refs, child, k))
                pieces_ref[child, :, k * BLOCK : (k + 1) * BLOCK] = x_ref[:, where]
            for x in range(4):
                leaving.append(moves.start(pieces_ref.at[child], outs[0].at[x * 2 + child]))
        if level == 1:
            for x in range(4):
                leaving.append(moves.start(x_ref.at[:, pl.ds(x * 256, 256)], outs[1].at[x]))
        else:
            y0 = lax.axis_index("y0")
            keep_out, beyond_out = outs[1:]
            for out, bit in ((beyond_out, 1 - y0), (keep_out, y0)):
                for x in range(4):
                    where = block_at(x * 2 + bit, 256)
                    leaving.append(moves.start(x_ref.at[:, where], out.at[0, x]))
            finish(both)
            for i, (out, bit) in enumerate(((beyond_out, 1 - y0), (keep_out, y0))):
                for x in range(4):
                    sums_ref[i, x] = own_ref[x, bit] + other_ref[x, bit]
                leaving.append(moves.start(sums_ref.at[i], out.at[1]))
        finish(leaving)

    outs = [(8, HALF, blocks * BLOCK)]
    outs += [(4, HALF, 256)] if level == 1 else [(2, 4, HALF, 256), (2, 4, HALF, 256)]
    operands = [*map(far, tables), received, *map(far, [weighted, weights, updates, *answers])]
    specs = [SCALARS] * 4 + [WHOLE] + [FAR] * (len(operands) - 5)
    scratch = [
        pltpu.SemaphoreType.DMA((64,)),
        pltpu.VMEM((HALF, span), jnp.float32),
        pltpu.VMEM((HALF, 256), jnp.float32),
        pltpu.VMEM((2, 256, span), jnp.bfloat16),
        pltpu.VMEM((2, 256, update_len), jnp.bfloat16),
        pltpu.VMEM((2, HALF, blocks * BLOCK), jnp.float32),
    ]
    if level == 2:
        scratch += [pltpu.VMEM((4, 2, HALF, 256), jnp.float32)] * 2 + [pltpu.VMEM((2, 4, HALF, 256), jnp.float32)]
    return call(body, outs, operands, specs, scratch, spaces="H" * n_outs)


def level_zero_backward(received, weighted, weights, updates, nearest, kept, other):
    def body(received_ref, weighted_ref, nearest_ref, kept_ref, other_ref, weights_ref, updates_ref, sent_ref):
        for x in range(4):
            for c in range(2):
                half = slice(c * HALF, (c + 1) * HALF)
                at = slice(c * PIVOTS, (c + 1) * PIVOTS)
                sent_ref[x, half, PIVOTS : 2 * PIVOTS] = nearest_ref[x, :, at]
                for i in range(2):
                    piece = kept_ref[i, x, :, at] + other_ref[i, x, :, at]
                    sent_ref[x, half, (2 + i) * PIVOTS : (3 + i) * PIVOTS] = piece
        chosen = jnp.concatenate([sum(received_ref[x * 2 + c] for x in range(4)) for c in range(2)], 0)
        target = weighted_ref[...] - product(chosen, updates_ref[0], updates_ref[1], 1)
        part = product(target, weights_ref[0], weights_ref[1], 0)
        for q in range(4):
            sent_ref[q, :, :PIVOTS] = part[:, q * PIVOTS : (q + 1) * PIVOTS]

    return call(
        body,
        [(4, SIDES, 512)],
        [received, *map(far, [weighted, nearest, kept]), other, close(weights), close(updates)],
        [WHOLE] * 7,
        spaces="h",
    )[0]


def summed(received):
    def body(received_ref, out_ref):
        out_ref[...] = (received_ref[0] + received_ref[1]) + (received_ref[2] + received_ref[3])

    return call(body, [(SIDES, 512)], [received], [WHOLE])[0]


def unpacked(total, beside):
    def body(total_ref, beside_ref, out_ref):
        c = lax.axis_index("c")
        mine = pl.ds(pl.multiple_of(c * HALF, 8), HALF)
        theirs = pl.ds(pl.multiple_of((1 - c) * HALF, 8), HALF)
        out_ref[:, :PIVOTS] = total_ref[:, :PIVOTS]
        out_ref[mine, PIVOTS:] = total_ref[mine, PIVOTS:]
        out_ref[theirs, PIVOTS:] = beside_ref[mine, PIVOTS:]

    return call(body, [(SIDES, 512)], [total, beside], [WHOLE] * 2)[0]


def summed_copies(received, count):
    total = jnp.sum(received, 0)
    return jnp.broadcast_to(total[None], (count, *total.shape))


def sibling_tables(targets):
    pairs = []
    for y1 in range(2):
        for y0 in range(2):
            here = y1 * 4 + y0 * 2
            pairs.append((here, y1 * 4 + (1 - y0) * 2))
            pairs.append((here + 1, (1 - y1) * 4 + y0 * 2 + 1))
    side = lax.ppermute(targets, ("y1", "y0", "c"), pairs)
    return [targets, side, with_partner(targets), with_partner(side)]


def per_device(right_side, factor_inverse, update_panel, update_targets, pivot_pairs, pivot_diagonal, pivot_coupling):
    sides = right_side[0, 0]
    inverse = factor_inverse[0, 0]
    update = update_panel[0, 0]
    plane = ("x", "y1", "y0")
    pair = ("x", "y0")

    packed = packed_sides(sides, with_partner(sides))
    first = exchange(packed, ("x",))
    factors = pivot_factors(pivot_pairs[0], pivot_diagonal[0], pivot_coupling[0])
    partner_factors = with_partner(factors)
    inverse_after, update_after, _ = lax.optimization_barrier((inverse, update, packed))
    partner_inverse = with_partner(inverse_after)
    partner_update = with_partner(update_after)
    (weights0,) = prepared([inverse], [(0, 512)], far(packed), pltpu.VMEM)
    (updates0,) = prepared([update], [(0, 256)], far(packed), pltpu.VMEM)
    tables = sibling_tables(update_targets)

    sent, weighted0, sides1, near = level_zero_forward(first, weights0, updates0, factors)
    beyond = across(near, "y0")
    received = exchange(sent, ("c", "x"))
    weights1, weights2, weights3 = prepared(
        [inverse, partner_inverse], [(512, 1024), (1536, 2048), (3584, 4096)], far(sent)
    )
    updates1, updates2 = prepared([update, partner_update], [(256, 512), (768, 1024)], far(sent))
    sent, weighted1, near3 = forward(
        1, received, [sides1, near, beyond], tables, weights1, updates1, factors, partner_factors
    )
    beyond3 = across(near3, "y1")
    received = exchange(sent, pair)
    sent, weighted2 = forward(2, received, [near, beyond], tables, weights2, updates2, factors, partner_factors)
    received = exchange(summed_copies(exchange(sent, pair), 16), plane)
    sent, kept3, other3 = forward(3, received, [near3, beyond3], tables, weights3, None, factors, partner_factors)
    other3 = across(other3, "y1")
    received = exchange(summed_copies(exchange(sent, plane), 8), pair)
    sent, kept, other = backward(2, received, weighted2, tables, weights2, updates2, [kept3, other3])
    other = across(other, "y0")
    received = exchange(sent, pair)
    sent, nearest = backward(1, received, weighted1, tables, weights1, updates1, [])
    received = exchange(sent, ("x", "c"))
    sent = level_zero_backward(received, weighted0, weights0, updates0, nearest, kept, other)
    total = summed(exchange(sent, ("x",)))
    return unpacked(total, with_partner(total))[None, None]


def solution(mesh):
    grid = np.array(mesh.devices).reshape(4, 2, 2, 2, 4)
    fine = Mesh(grid, AXES)
    leaf = ("z", "y1", "y0", "c")
    in_specs = (
        P(leaf, "x", None, None),
        P(leaf, "x", None, None),
        P(leaf, "x", None, None),
        P(leaf, None),
        P(leaf, "x", None),
        P(leaf, "x", None),
        P(leaf, "x", None),
    )
    out_specs = P(leaf, "x", None, None)
    return jax.shard_map(per_device, mesh=fine, in_specs=in_specs, out_specs=out_specs, check_vma=False)
```

```python
import jax
import jax.numpy as jnp
import numpy as np
from jax import lax
from jax.experimental import pallas as pl
from jax.experimental.pallas import tpu as pltpu
from jax.sharding import Mesh, PartitionSpec as P

LEVELS = 4
BLOCK = 128
PIVOTS = 128
SIDES = 96
HALF = SIDES // 2
AXES = ("z", "y1", "y0", "c", "x")

exact_mode = lax.Precision.HIGHEST


def parts(value):
    high = value.astype(jnp.bfloat16)
    return high, (value - high.astype(jnp.float32)).astype(jnp.bfloat16)


def product(left, high, low, side):
    left_high, left_low = parts(left)
    dims = (((1,), (side,)), ((), ()))

    def dot(a, b):
        return lax.dot_general(a, b, dims, preferred_element_type=jnp.float32)

    return dot(left_high, high) + (dot(left_high, low) + dot(left_low, high))


def dot_full(left, right):
    return lax.dot_general(
        left, right, (((1,), (0,)), ((), ())), precision=exact_mode, preferred_element_type=jnp.float32
    )


def exchange(value, axes):
    return lax.all_to_all(value, axes, 0, 0, tiled=True)


def with_partner(value):
    return lax.ppermute(value, "c", [(0, 1), (1, 0)])


def across(value, axis):
    return lax.ppermute(value, axis, [(0, 1), (1, 0)])


def block_at(index, size=BLOCK):
    return pl.ds(pl.multiple_of(index * size, size), size)


WHOLE = pl.BlockSpec(memory_space=pltpu.VMEM)
SCALARS = pl.BlockSpec(memory_space=pltpu.SMEM)
FAR = pl.BlockSpec(memory_space=pltpu.HBM)


def far(value):
    return pltpu.with_memory_space_constraint(value, pltpu.HBM)


def close(value):
    return pltpu.with_memory_space_constraint(value, pltpu.VMEM)


def call(body, out_shapes, operands, specs, scratch=(), limit=20, spaces=None):
    return pl.pallas_call(
        body,
        in_specs=specs,
        out_specs=[FAR if k == "H" else WHOLE for k in spaces or "-" * len(out_shapes)],
        out_shape=[
            {"H": pltpu.HBM, "h": pltpu.HBM, "v": pltpu.VMEM, "-": jax.ShapeDtypeStruct}[k](s, jnp.float32)
            for s, k in zip(out_shapes, spaces or "-" * len(out_shapes))
        ],
        scratch_shapes=list(scratch),
        compiler_params=pltpu.CompilerParams(vmem_limit_bytes=limit * 1024 * 1024),
    )(*operands)


def prepared(pair, spans, after):
    def body(*refs):
        sources = refs[: len(pair)]
        outs = refs[len(pair) + 1 :][: len(spans)]
        buffers = refs[len(pair) + 1 + len(spans) : -1]
        semaphores = refs[-1]
        moves = []
        for i, (start, width, _) in enumerate(spans):
            for side, source in enumerate(sources):
                move = pltpu.make_async_copy(
                    source.at[:, pl.ds(start, width)],
                    buffers[i].at[pl.ds(side * PIVOTS, PIVOTS), :],
                    semaphores.at[i, side],
                )
                move.start()
                moves.append((i, side, move))
        for i, side, move in moves:
            move.wait()
            rows = slice(side * PIVOTS, (side + 1) * PIVOTS)
            _, width, step = spans[i]
            for k, at in enumerate(range(0, width, step or width)):
                high, low = parts(buffers[i][rows, at : at + (step or width)])
                place = outs[i].at[k] if step else outs[i]
                place[0, rows] = high
                place[1, rows] = low

    count = len(pair) * PIVOTS
    shapes = [
        pltpu.HBM((width // step, 2, count, step), jnp.bfloat16) if step else pltpu.VMEM((2, count, width), jnp.bfloat16)
        for _, width, step in spans
    ]
    return pl.pallas_call(
        body,
        in_specs=[FAR] * (len(pair) + 1),
        out_specs=[WHOLE] * len(spans),
        out_shape=shapes,
        scratch_shapes=[pltpu.VMEM((count, width), jnp.float32) for _, width, _ in spans]
        + [pltpu.SemaphoreType.DMA((len(spans), len(pair)))],
        compiler_params=pltpu.CompilerParams(vmem_limit_bytes=28 * 1024 * 1024),
    )(*map(far, pair), far(after))


def pivot_apply(solved, own, swapped):
    lane = lax.broadcasted_iota(jnp.int32, solved.shape, 1)
    width = solved.shape[1]
    beside = jnp.where(lane % 2 == 0, pltpu.roll(solved, width - 1, 1), pltpu.roll(solved, 1, 1))
    return own * solved + swapped * beside


def pivot_factors(kinds, diagonal, coupling):
    def body(kinds_ref, diagonal_ref, coupling_ref, out_ref):
        width = diagonal_ref.shape[1]
        row = lax.broadcasted_iota(jnp.int32, (width // 2, width), 0)
        col = lax.broadcasted_iota(jnp.int32, (width // 2, width), 1)
        widen = (col // 2 == row).astype(jnp.float32)
        pair = jnp.concatenate(
            [kinds_ref[...].astype(jnp.float32), coupling_ref[...], jnp.zeros((6, width // 2), jnp.float32)], 0
        )
        wide = dot_full(pair, widen)
        is_pair = wide[0:1] > 0.5
        couple = wide[1:2]
        own = jnp.broadcast_to(diagonal_ref[...], (8, width))
        lane = lax.broadcasted_iota(jnp.int32, (8, width), 1)
        other = jnp.where(lane % 2 == 0, pltpu.roll(own, width - 1, 1), pltpu.roll(own, 1, 1))[0:1]
        own = own[0:1]
        determinant = own * other - couple * couple
        out_ref[0:1, :] = jnp.where(is_pair, other / determinant, 1.0 / own)
        out_ref[1:2, :] = jnp.where(is_pair, -couple / determinant, 0.0)

    operands = [far(kinds), far(diagonal), far(coupling)]
    return call(body, [(2, diagonal.shape[1])], operands, [WHOLE] * 3, spaces="v")[0]


def packed_sides(sides, beside):
    def body(sides_ref, beside_ref, out_ref):
        c = lax.axis_index("c")
        mine = pl.ds(pl.multiple_of(c * HALF, 8), HALF)
        theirs = pl.ds(pl.multiple_of((1 - c) * HALF, 8), HALF)
        own = sides_ref[mine, PIVOTS:]
        other = beside_ref[mine, PIVOTS:]
        for i in range(4):
            out_ref[i, :, :PIVOTS] = sides_ref[:, :PIVOTS]
            out_ref[i, mine, PIVOTS:] = own
            out_ref[i, theirs, PIVOTS:] = other

    return call(body, [(4, SIDES, 512)], [far(sides), beside], [WHOLE] * 2, spaces="h")[0]


class Moves:
    def __init__(self, semaphores):
        self.semaphores, self.started = semaphores, []

    def start(self, source, target):
        move = pltpu.make_async_copy(source, target, self.semaphores.at[len(self.started)])
        move.start()
        self.started.append(move)
        return move

    def chunks(self, source, target):
        return [self.start(source.at[k], target.at[k]) for k in range(source.shape[0])]


def finish(moves):
    for move in moves:
        move.wait()


def level_zero_forward(first, weights, updates, factors):
    def body(first_ref, weights_ref, updates_ref, factors_ref, *refs):
        sent_ref, weighted_ref, one_ref, upper_ref, part_ref, own_ref, semaphores = refs
        moves = Moves(semaphores)
        leaving = [
            moves.start(first_ref.at[:, :, pl.ds(PIVOTS, PIVOTS)], one_ref),
            moves.start(first_ref.at[:, :, pl.ds(2 * PIVOTS, 2 * PIVOTS)], upper_ref),
        ]
        gathered = jnp.concatenate([first_ref[q, :, :PIVOTS] for q in range(4)], 1)
        solved = product(gathered, weights_ref[0], weights_ref[1], 1)
        part_ref[...] = product(solved, updates_ref[0], updates_ref[1], 0)
        for c in range(2):
            for x in range(4):
                leaving.append(moves.start(part_ref.at[pl.ds(c * HALF, HALF)], sent_ref.at[c * 4 + x]))
        own_ref[...] = pivot_apply(solved, factors_ref[0:1, :PIVOTS], factors_ref[1:2, :PIVOTS])
        leaving.append(moves.start(own_ref, weighted_ref))
        finish(leaving)

    return call(
        body,
        [(8, HALF, 256), (SIDES, PIVOTS), (4, SIDES, PIVOTS), (4, SIDES, 256)],
        [close(first), close(weights), close(updates), close(factors)],
        [WHOLE] * 4,
        [
            pltpu.VMEM((SIDES, 256), jnp.float32),
            pltpu.VMEM((SIDES, PIVOTS), jnp.float32),
            pltpu.SemaphoreType.DMA((16,)),
        ],
        spaces="HHHH",
    )


def child_block(level, tables, child, k):
    own_ref, side_ref, own_beside_ref, side_beside_ref = tables
    c = lax.axis_index("c")
    if level == 1:
        return jnp.where(c == child, own_ref[0, k], own_beside_ref[0, k])
    if level == 2:
        sibling = jnp.where(c == 0, side_ref[0, 2 + k], side_beside_ref[0, 2 + k])
        return jnp.where(lax.axis_index("y0") == child, own_ref[0, 2 + k], sibling)
    sibling = jnp.where(c == 0, side_beside_ref[0, 6 + k], side_ref[0, 6 + k])
    return jnp.where(lax.axis_index("y1") == child, own_ref[0, 6 + k], sibling)


def both_factors(level, factors, beside):
    c = lax.axis_index("c")
    at = slice(level * PIVOTS, (level + 1) * PIVOTS)
    return [jnp.concatenate([factors[i : i + 1, at], beside[i : i + 1, at]], 1) for i in range(2)]


def halves(rows):
    return jnp.concatenate([rows[:HALF], rows[HALF:]], 1)


def forward(level, received, sides, tables, weights, updates, factors, partner_factors):
    width = 1 << level
    span = 4 * PIVOTS * width
    chunks = span // 512
    update_len = 2 * PIVOTS * width if level < 3 else 0
    blocks = (2, 4, 8)[level - 1]
    n_sides = len(sides)
    n_updates = 1 if level < 3 else 0
    n_outs = (3, 2, 3)[level - 1]

    def body(*refs):
        refs = list(refs)

        def take(count):
            taken, refs[:] = refs[:count], refs[count:]
            return taken

        tables_refs = take(4)
        received_ref, factors_ref, beside_ref = take(3)
        updates_ref = take(n_updates)
        sides_refs = take(n_sides)
        (weights_far,) = take(1)
        outs = take(n_outs)
        semaphores, b_ref, own_ref, weights_ref = take(4)
        moves = Moves(semaphores)
        x0, y0, y1 = lax.axis_index("x"), lax.axis_index("y0"), lax.axis_index("y1")

        arriving, leaving = [], []

        def bring(source, block):
            for c in range(2):
                arriving.append(moves.start(source.at[pl.ds(c * HALF, HALF)], b_ref.at[:, block_at(block * 2 + c)]))

        if level == 1:
            for x in range(4):
                bring(sides_refs[0].at[x], x)
        elif level == 2:
            for flip in range(2):
                for x in range(4):
                    bring(sides_refs[flip].at[x, :, pl.ds(0, PIVOTS)], x * 2 + (y0 ^ flip))
        else:
            for high in range(2):
                for flip in range(2):
                    for x in range(4):
                        bring(sides_refs[high].at[flip, x], x * 4 + (y1 ^ high) * 2 + (y0 ^ flip))
        columns = moves.chunks(weights_far, weights_ref)
        if level < 3:
            part_ref = refs[0]
        if level == 1:
            passing_ref = refs[1]
            passing = [
                moves.start(sides_refs[1 + flip].at[:, :, pl.ds(PIVOTS, PIVOTS)], passing_ref.at[flip])
                for flip in range(2)
            ]
        totals = [None, None]
        for child in range(2):
            if level == 1:
                totals[child] = sum(received_ref[child * 4 + x] for x in range(4))
            elif level == 2:
                totals[child] = sum(received_ref[x * 2 + child] for x in range(4))
        finish(arriving)
        for child in range(2):
            for k in range(blocks):
                if level < 3:
                    piece = totals[child][:, k * BLOCK : (k + 1) * BLOCK]
                else:
                    piece = received_ref[(k // 2) * 4 + child * 2 + k % 2]
                where = block_at(child_block(level, tables_refs, child, k))
                b_ref[:, where] = b_ref[:, where] - piece
        solved = jnp.zeros((HALF, 2 * PIVOTS), jnp.float32)
        for k in range(chunks):
            columns[k].wait()
            at = slice(k * 512, (k + 1) * 512)
            solved += product(b_ref[:, at], weights_ref[k, 0], weights_ref[k, 1], 1)
        weighted = pivot_apply(solved, *both_factors(level, factors_ref, beside_ref))
        if level < 3:
            own_ref[...] = weighted
            leaving.append(moves.start(own_ref, outs[1]))
            if level == 1:
                finish(passing)
                leaving.append(moves.start(passing_ref, outs[2]))
            for k in range(update_len // 256):
                at = slice(k * 256, (k + 1) * 256)
                part_ref[:, at] = product(solved, updates_ref[0][0, :, at], updates_ref[0][1, :, at], 0)
            for i in range(8):
                source = part_ref if level == 1 else part_ref.at[:, pl.ds(i * BLOCK, BLOCK)]
                leaving.append(moves.start(source, outs[0].at[i]))
        else:
            sent_ref, keep_ref, beyond_ref = outs
            for k in range(chunks):
                at = slice(k * 512, (k + 1) * 512)
                b_ref[:, at] = product(weighted, weights_ref[k, 0], weights_ref[k, 1], 0)
            for child in range(2):
                for k in range(8):
                    where = block_at(child_block(3, tables_refs, child, k))
                    leaving.append(
                        moves.start(b_ref.at[:, where], sent_ref.at[(k // 2) * 4 + child * 2 + k % 2])
                    )
            for out, bit in ((beyond_ref, 1 - y1), (keep_ref, y1)):
                for x in range(4):
                    for low in range(2):
                        where = block_at(x * 4 + bit * 2 + low, 256)
                        leaving.append(moves.start(b_ref.at[:, where], out.at[x, low]))
        finish(leaving)

    outs = {
        1: [(8, HALF, 512), (HALF, 256), (2, 4, SIDES, PIVOTS)],
        2: [(8, HALF, BLOCK), (HALF, 256)],
        3: [(16, HALF, BLOCK), (4, 2, HALF, 256), (4, 2, HALF, 256)],
    }[level]
    operands = [*map(far, tables), received, close(factors), close(partner_factors)]
    operands += [close(updates)] if level < 3 else []
    n_close = len(operands) - 4
    operands += map(far, [*sides, weights])
    specs = [SCALARS] * 4 + [WHOLE] * n_close + [FAR] * (n_sides + 1)
    scratch = [
        pltpu.SemaphoreType.DMA((80,)),
        pltpu.VMEM((HALF, span), jnp.float32),
        pltpu.VMEM((HALF, 256), jnp.float32),
        pltpu.VMEM((chunks, 2, 256, 512), jnp.bfloat16),
    ]
    if level < 3:
        scratch.append(pltpu.VMEM((HALF, update_len), jnp.float32))
    if level == 1:
        scratch.append(pltpu.VMEM((2, 4, SIDES, PIVOTS), jnp.float32))
    return call(body, outs, operands, specs, scratch, spaces="H" * n_outs)


def backward(level, received, weighted, tables, weights, updates, answers):
    width = 1 << level
    span = 4 * PIVOTS * width
    chunks = span // 512
    update_len = 2 * PIVOTS * width
    blocks = (2, 4)[level - 1]
    n_answers = len(answers)
    n_outs = (2, 3)[level - 1]

    def body(*refs):
        refs = list(refs)

        def take(count):
            taken, refs[:] = refs[:count], refs[count:]
            return taken

        tables_refs = take(4)
        received_ref, updates_ref = take(2)
        weighted_far, weights_far = take(2)
        answers_far = take(n_answers)
        outs = take(n_outs)
        semaphores, x_ref, weighted_ref, weights_ref, pieces_ref = take(5)
        moves = Moves(semaphores)
        arriving = moves.start(weighted_far, weighted_ref)
        columns = moves.chunks(weights_far, weights_ref)
        leaving = []
        if level == 2:
            own_ref, other_ref, sums_ref = refs
            both = [moves.start(answers_far[0], own_ref), moves.start(answers_far[1], other_ref)]
        if level == 1:
            total = sum(received_ref[i] for i in range(8))
        arriving.wait()
        target = weighted_ref[...]
        for k in range(update_len // 256):
            at = slice(k * 256, (k + 1) * 256)
            if level == 1:
                chosen = total[:, at]
            else:
                chosen = jnp.concatenate([received_ref[2 * k], received_ref[2 * k + 1]], 1)
            target -= product(chosen, updates_ref[0, :, at], updates_ref[1, :, at], 1)
        for k in range(chunks):
            columns[k].wait()
            at = slice(k * 512, (k + 1) * 512)
            x_ref[:, at] = product(target, weights_ref[k, 0], weights_ref[k, 1], 0)
        for child in range(2):
            for k in range(blocks):
                where = block_at(child_block(level, tables_refs, child, k))
                pieces_ref[child, :, k * BLOCK : (k + 1) * BLOCK] = x_ref[:, where]
            for x in range(4):
                leaving.append(moves.start(pieces_ref.at[child], outs[0].at[x * 2 + child]))
        if level == 1:
            for x in range(4):
                leaving.append(moves.start(x_ref.at[:, pl.ds(x * 256, 256)], outs[1].at[x]))
        else:
            y0 = lax.axis_index("y0")
            keep_out, beyond_out = outs[1:]
            for out, bit in ((beyond_out, 1 - y0), (keep_out, y0)):
                for x in range(4):
                    where = block_at(x * 2 + bit, 256)
                    leaving.append(moves.start(x_ref.at[:, where], out.at[0, x]))
            finish(both)
            for i, (out, bit) in enumerate(((beyond_out, 1 - y0), (keep_out, y0))):
                for x in range(4):
                    sums_ref[i, x] = own_ref[x, bit] + other_ref[x, bit]
                leaving.append(moves.start(sums_ref.at[i], out.at[1]))
        finish(leaving)

    outs = [(8, HALF, blocks * BLOCK)]
    outs += [(4, HALF, 256)] if level == 1 else [(2, 4, HALF, 256), (2, 4, HALF, 256)]
    operands = [*map(far, tables), received, close(updates), *map(far, [weighted, weights, *answers])]
    specs = [SCALARS] * 4 + [WHOLE] * 2 + [FAR] * (len(operands) - 6)
    scratch = [
        pltpu.SemaphoreType.DMA((64,)),
        pltpu.VMEM((HALF, span), jnp.float32),
        pltpu.VMEM((HALF, 256), jnp.float32),
        pltpu.VMEM((chunks, 2, 256, 512), jnp.bfloat16),
        pltpu.VMEM((2, HALF, blocks * BLOCK), jnp.float32),
    ]
    if level == 2:
        scratch += [pltpu.VMEM((4, 2, HALF, 256), jnp.float32)] * 2 + [pltpu.VMEM((2, 4, HALF, 256), jnp.float32)]
    return call(body, outs, operands, specs, scratch, spaces="H" * n_outs)


def level_zero_backward(received, weighted, weights, updates, nearest, kept, other):
    def body(received_ref, weighted_ref, nearest_ref, kept_ref, other_ref, weights_ref, updates_ref, sent_ref):
        for x in range(4):
            for c in range(2):
                half = slice(c * HALF, (c + 1) * HALF)
                at = slice(c * PIVOTS, (c + 1) * PIVOTS)
                sent_ref[x, half, PIVOTS : 2 * PIVOTS] = nearest_ref[x, :, at]
                for i in range(2):
                    piece = kept_ref[i, x, :, at] + other_ref[i, x, :, at]
                    sent_ref[x, half, (2 + i) * PIVOTS : (3 + i) * PIVOTS] = piece
        chosen = jnp.concatenate([sum(received_ref[x * 2 + c] for x in range(4)) for c in range(2)], 0)
        target = weighted_ref[...] - product(chosen, updates_ref[0], updates_ref[1], 1)
        part = product(target, weights_ref[0], weights_ref[1], 0)
        for q in range(4):
            sent_ref[q, :, :PIVOTS] = part[:, q * PIVOTS : (q + 1) * PIVOTS]

    return call(
        body,
        [(4, SIDES, 512)],
        [received, *map(far, [weighted, nearest, kept]), other, close(weights), close(updates)],
        [WHOLE] * 7,
        spaces="h",
    )[0]


def summed(received):
    def body(received_ref, out_ref):
        out_ref[...] = (received_ref[0] + received_ref[1]) + (received_ref[2] + received_ref[3])

    return call(body, [(SIDES, 512)], [received], [WHOLE])[0]


def unpacked(total, beside):
    def body(total_ref, beside_ref, out_ref):
        c = lax.axis_index("c")
        mine = pl.ds(pl.multiple_of(c * HALF, 8), HALF)
        theirs = pl.ds(pl.multiple_of((1 - c) * HALF, 8), HALF)
        out_ref[:, :PIVOTS] = total_ref[:, :PIVOTS]
        out_ref[mine, PIVOTS:] = total_ref[mine, PIVOTS:]
        out_ref[theirs, PIVOTS:] = beside_ref[mine, PIVOTS:]

    return call(body, [(SIDES, 512)], [total, beside], [WHOLE] * 2)[0]


def summed_copies(received, count):
    total = jnp.sum(received, 0)
    return jnp.broadcast_to(total[None], (count, *total.shape))


def sibling_tables(targets):
    pairs = []
    for y1 in range(2):
        for y0 in range(2):
            here = y1 * 4 + y0 * 2
            pairs.append((here, y1 * 4 + (1 - y0) * 2))
            pairs.append((here + 1, (1 - y1) * 4 + y0 * 2 + 1))
    side = lax.ppermute(targets, ("y1", "y0", "c"), pairs)
    return [targets, side, with_partner(targets), with_partner(side)]


def per_device(right_side, factor_inverse, update_panel, update_targets, pivot_pairs, pivot_diagonal, pivot_coupling):
    sides = right_side[0, 0]
    inverse = factor_inverse[0, 0]
    update = update_panel[0, 0]
    plane = ("x", "y1", "y0")
    pair = ("x", "y0")

    packed = packed_sides(sides, with_partner(sides))
    first = exchange(packed, ("x",))
    factors = pivot_factors(pivot_pairs[0], pivot_diagonal[0], pivot_coupling[0])
    partner_factors = with_partner(factors)
    inverse_after, update_after, _ = lax.optimization_barrier((inverse, update, packed))
    partner_inverse = with_partner(inverse_after)
    partner_update = with_partner(update_after)
    (weights0,) = prepared([inverse], [(0, 512, None)], packed)
    (updates0,) = prepared([update], [(0, 256, None)], packed)
    tables = sibling_tables(update_targets)

    sent, weighted0, sides1, near = level_zero_forward(first, weights0, updates0, factors)
    beyond = across(near, "y0")
    received = exchange(sent, ("c", "x"))
    (weights1,) = prepared([inverse, partner_inverse], [(512, 1024, 512)], sent)
    (updates1,) = prepared([update, partner_update], [(256, 512, None)], sent)
    sent, weighted1, near3 = forward(
        1, received, [sides1, near, beyond], tables, weights1, updates1, factors, partner_factors
    )
    weights2, weights3 = prepared([inverse, partner_inverse], [(1536, 2048, 512), (3584, 4096, 512)], sent)
    (updates2,) = prepared([update, partner_update], [(768, 1024, None)], sent)
    beyond3 = across(near3, "y1")
    received = exchange(sent, pair)
    sent, weighted2 = forward(2, received, [near, beyond], tables, weights2, updates2, factors, partner_factors)
    received = exchange(summed_copies(exchange(sent, pair), 16), plane)
    sent, kept3, other3 = forward(3, received, [near3, beyond3], tables, weights3, None, factors, partner_factors)
    other3 = across(other3, "y1")
    received = exchange(summed_copies(exchange(sent, plane), 8), pair)
    sent, kept, other = backward(2, received, weighted2, tables, weights2, updates2, [kept3, other3])
    other = across(other, "y0")
    received = exchange(sent, pair)
    sent, nearest = backward(1, received, weighted1, tables, weights1, updates1, [])
    received = exchange(sent, ("x", "c"))
    sent = level_zero_backward(received, weighted0, weights0, updates0, nearest, kept, other)
    total = summed(exchange(sent, ("x",)))
    return unpacked(total, with_partner(total))[None, None]


def solution(mesh):
    grid = np.array(mesh.devices).reshape(4, 2, 2, 2, 4)
    fine = Mesh(grid, AXES)
    leaf = ("z", "y1", "y0", "c")
    in_specs = (
        P(leaf, "x", None, None),
        P(leaf, "x", None, None),
        P(leaf, "x", None, None),
        P(leaf, None),
        P(leaf, "x", None),
        P(leaf, "x", None),
        P(leaf, "x", None),
    )
    out_specs = P(leaf, "x", None, None)
    return jax.shard_map(per_device, mesh=fine, in_specs=in_specs, out_specs=out_specs, check_vma=False)
```

```python
import jax
import jax.numpy as jnp
import numpy as np
from jax import lax
from jax.experimental import pallas as pl
from jax.experimental.pallas import tpu as pltpu
from jax.sharding import Mesh, PartitionSpec as P

LEVELS = 4
BLOCK = 128
PIVOTS = 128
SIDES = 96
HALF = SIDES // 2
AXES = ("z", "y1", "y0", "c", "x")

exact_mode = lax.Precision.HIGHEST


def parts(value):
    high = value.astype(jnp.bfloat16)
    return high, (value - high.astype(jnp.float32)).astype(jnp.bfloat16)


def product(left, high, low, side):
    left_high, left_low = parts(left)
    dims = (((1,), (side,)), ((), ()))

    def dot(a, b):
        return lax.dot_general(a, b, dims, preferred_element_type=jnp.float32)

    both = dot(jnp.concatenate([left_high, left_low], 0), high)
    rows = left.shape[0]
    return both[:rows] + (dot(left_high, low) + both[rows:])


def dot_full(left, right):
    return lax.dot_general(
        left, right, (((1,), (0,)), ((), ())), precision=exact_mode, preferred_element_type=jnp.float32
    )


def exchange(value, axes):
    return lax.all_to_all(value, axes, 0, 0, tiled=True)


def with_partner(value):
    return lax.ppermute(value, "c", [(0, 1), (1, 0)])


def across(value, axis):
    return lax.ppermute(value, axis, [(0, 1), (1, 0)])


def block_at(index, size=BLOCK):
    return pl.ds(pl.multiple_of(index * size, size), size)


WHOLE = pl.BlockSpec(memory_space=pltpu.VMEM)
SCALARS = pl.BlockSpec(memory_space=pltpu.SMEM)
FAR = pl.BlockSpec(memory_space=pltpu.HBM)


def far(value):
    return pltpu.with_memory_space_constraint(value, pltpu.HBM)


def close(value):
    return pltpu.with_memory_space_constraint(value, pltpu.VMEM)


def call(body, out_shapes, operands, specs, scratch=(), limit=20, spaces=None):
    return pl.pallas_call(
        body,
        in_specs=specs,
        out_specs=[FAR if k == "H" else WHOLE for k in spaces or "-" * len(out_shapes)],
        out_shape=[
            {"H": pltpu.HBM, "h": pltpu.HBM, "v": pltpu.VMEM, "-": jax.ShapeDtypeStruct}[k](s, jnp.float32)
            for s, k in zip(out_shapes, spaces or "-" * len(out_shapes))
        ],
        scratch_shapes=list(scratch),
        compiler_params=pltpu.CompilerParams(vmem_limit_bytes=limit * 1024 * 1024),
    )(*operands)


def prepared(pair, spans, after):
    def body(*refs):
        sources = refs[: len(pair)]
        outs = refs[len(pair) + 1 :][: len(spans)]
        buffers = refs[len(pair) + 1 + len(spans) : -1]
        semaphores = refs[-1]
        moves = []
        for i, (start, width, _) in enumerate(spans):
            for side, source in enumerate(sources):
                move = pltpu.make_async_copy(
                    source.at[:, pl.ds(start, width)],
                    buffers[i].at[pl.ds(side * PIVOTS, PIVOTS), :],
                    semaphores.at[i, side],
                )
                move.start()
                moves.append((i, side, move))
        for i, side, move in moves:
            move.wait()
            rows = slice(side * PIVOTS, (side + 1) * PIVOTS)
            _, width, step = spans[i]
            for k, at in enumerate(range(0, width, step or width)):
                high, low = parts(buffers[i][rows, at : at + (step or width)])
                place = outs[i].at[k] if step else outs[i]
                place[0, rows] = high
                place[1, rows] = low

    count = len(pair) * PIVOTS
    shapes = [
        pltpu.HBM((width // step, 2, count, step), jnp.bfloat16) if step else pltpu.VMEM((2, count, width), jnp.bfloat16)
        for _, width, step in spans
    ]
    return pl.pallas_call(
        body,
        in_specs=[FAR] * (len(pair) + 1),
        out_specs=[WHOLE] * len(spans),
        out_shape=shapes,
        scratch_shapes=[pltpu.VMEM((count, width), jnp.float32) for _, width, _ in spans]
        + [pltpu.SemaphoreType.DMA((len(spans), len(pair)))],
        compiler_params=pltpu.CompilerParams(vmem_limit_bytes=28 * 1024 * 1024),
    )(*map(far, pair), far(after))


def pivot_apply(solved, own, swapped):
    lane = lax.broadcasted_iota(jnp.int32, solved.shape, 1)
    width = solved.shape[1]
    beside = jnp.where(lane % 2 == 0, pltpu.roll(solved, width - 1, 1), pltpu.roll(solved, 1, 1))
    return own * solved + swapped * beside


def pivot_factors(kinds, diagonal, coupling):
    def body(kinds_ref, diagonal_ref, coupling_ref, out_ref):
        width = diagonal_ref.shape[1]
        row = lax.broadcasted_iota(jnp.int32, (width // 2, width), 0)
        col = lax.broadcasted_iota(jnp.int32, (width // 2, width), 1)
        widen = (col // 2 == row).astype(jnp.float32)
        pair = jnp.concatenate(
            [kinds_ref[...].astype(jnp.float32), coupling_ref[...], jnp.zeros((6, width // 2), jnp.float32)], 0
        )
        wide = dot_full(pair, widen)
        is_pair = wide[0:1] > 0.5
        couple = wide[1:2]
        own = jnp.broadcast_to(diagonal_ref[...], (8, width))
        lane = lax.broadcasted_iota(jnp.int32, (8, width), 1)
        other = jnp.where(lane % 2 == 0, pltpu.roll(own, width - 1, 1), pltpu.roll(own, 1, 1))[0:1]
        own = own[0:1]
        determinant = own * other - couple * couple
        out_ref[0:1, :] = jnp.where(is_pair, other / determinant, 1.0 / own)
        out_ref[1:2, :] = jnp.where(is_pair, -couple / determinant, 0.0)

    operands = [far(kinds), far(diagonal), far(coupling)]
    return call(body, [(2, diagonal.shape[1])], operands, [WHOLE] * 3, spaces="v")[0]


def packed_sides(sides, beside):
    def body(sides_ref, beside_ref, out_ref):
        c = lax.axis_index("c")
        mine = pl.ds(pl.multiple_of(c * HALF, 8), HALF)
        theirs = pl.ds(pl.multiple_of((1 - c) * HALF, 8), HALF)
        own = sides_ref[mine, PIVOTS:]
        other = beside_ref[mine, PIVOTS:]
        for i in range(4):
            out_ref[i, :, :PIVOTS] = sides_ref[:, :PIVOTS]
            out_ref[i, mine, PIVOTS:] = own
            out_ref[i, theirs, PIVOTS:] = other

    return call(body, [(4, SIDES, 512)], [far(sides), beside], [WHOLE] * 2, spaces="h")[0]


class Moves:
    def __init__(self, semaphores):
        self.semaphores, self.started = semaphores, []

    def start(self, source, target):
        move = pltpu.make_async_copy(source, target, self.semaphores.at[len(self.started)])
        move.start()
        self.started.append(move)
        return move

    def chunks(self, source, target):
        return [self.start(source.at[k], target.at[k]) for k in range(source.shape[0])]


def finish(moves):
    for move in moves:
        move.wait()


def level_zero_forward(first, weights, updates, factors):
    def body(first_ref, weights_ref, updates_ref, factors_ref, *refs):
        sent_ref, weighted_ref, one_ref, upper_ref, part_ref, own_ref, semaphores = refs
        moves = Moves(semaphores)
        leaving = [
            moves.start(first_ref.at[:, :, pl.ds(PIVOTS, PIVOTS)], one_ref),
            moves.start(first_ref.at[:, :, pl.ds(2 * PIVOTS, 2 * PIVOTS)], upper_ref),
        ]
        gathered = jnp.concatenate([first_ref[q, :, :PIVOTS] for q in range(4)], 1)
        solved = product(gathered, weights_ref[0], weights_ref[1], 1)
        part_ref[...] = product(solved, updates_ref[0], updates_ref[1], 0)
        for c in range(2):
            for x in range(4):
                leaving.append(moves.start(part_ref.at[pl.ds(c * HALF, HALF)], sent_ref.at[c * 4 + x]))
        own_ref[...] = pivot_apply(solved, factors_ref[0:1, :PIVOTS], factors_ref[1:2, :PIVOTS])
        leaving.append(moves.start(own_ref, weighted_ref))
        finish(leaving)

    return call(
        body,
        [(8, HALF, 256), (SIDES, PIVOTS), (4, SIDES, PIVOTS), (4, SIDES, 256)],
        [close(first), close(weights), close(updates), close(factors)],
        [WHOLE] * 4,
        [
            pltpu.VMEM((SIDES, 256), jnp.float32),
            pltpu.VMEM((SIDES, PIVOTS), jnp.float32),
            pltpu.SemaphoreType.DMA((16,)),
        ],
        spaces="HHHH",
    )


def child_block(level, tables, child, k):
    own_ref, side_ref, own_beside_ref, side_beside_ref = tables
    c = lax.axis_index("c")
    if level == 1:
        return jnp.where(c == child, own_ref[0, k], own_beside_ref[0, k])
    if level == 2:
        sibling = jnp.where(c == 0, side_ref[0, 2 + k], side_beside_ref[0, 2 + k])
        return jnp.where(lax.axis_index("y0") == child, own_ref[0, 2 + k], sibling)
    sibling = jnp.where(c == 0, side_beside_ref[0, 6 + k], side_ref[0, 6 + k])
    return jnp.where(lax.axis_index("y1") == child, own_ref[0, 6 + k], sibling)


def both_factors(level, factors, beside):
    c = lax.axis_index("c")
    at = slice(level * PIVOTS, (level + 1) * PIVOTS)
    return [jnp.concatenate([factors[i : i + 1, at], beside[i : i + 1, at]], 1) for i in range(2)]


def halves(rows):
    return jnp.concatenate([rows[:HALF], rows[HALF:]], 1)


def forward(level, received, sides, tables, weights, updates, factors, partner_factors):
    width = 1 << level
    span = 4 * PIVOTS * width
    chunks = span // 512
    update_len = 2 * PIVOTS * width if level < 3 else 0
    blocks = (2, 4, 8)[level - 1]
    n_sides = len(sides)
    n_updates = 1 if level < 3 else 0
    n_outs = (3, 2, 3)[level - 1]

    def body(*refs):
        refs = list(refs)

        def take(count):
            taken, refs[:] = refs[:count], refs[count:]
            return taken

        tables_refs = take(4)
        received_ref, factors_ref, beside_ref = take(3)
        updates_ref = take(n_updates)
        sides_refs = take(n_sides)
        (weights_far,) = take(1)
        outs = take(n_outs)
        semaphores, b_ref, own_ref, weights_ref = take(4)
        moves = Moves(semaphores)
        x0, y0, y1 = lax.axis_index("x"), lax.axis_index("y0"), lax.axis_index("y1")

        arriving, leaving = [], []

        def bring(source, block):
            for c in range(2):
                arriving.append(moves.start(source.at[pl.ds(c * HALF, HALF)], b_ref.at[:, block_at(block * 2 + c)]))

        if level == 1:
            for x in range(4):
                bring(sides_refs[0].at[x], x)
        elif level == 2:
            for flip in range(2):
                for x in range(4):
                    bring(sides_refs[flip].at[x, :, pl.ds(0, PIVOTS)], x * 2 + (y0 ^ flip))
        else:
            for high in range(2):
                for flip in range(2):
                    for x in range(4):
                        bring(sides_refs[high].at[flip, x], x * 4 + (y1 ^ high) * 2 + (y0 ^ flip))
        columns = moves.chunks(weights_far, weights_ref)
        if level < 3:
            part_ref = refs[0]
        if level == 1:
            passing_ref = refs[1]
            passing = [
                moves.start(sides_refs[1 + flip].at[:, :, pl.ds(PIVOTS, PIVOTS)], passing_ref.at[flip])
                for flip in range(2)
            ]
        totals = [None, None]
        for child in range(2):
            if level == 1:
                totals[child] = sum(received_ref[child * 4 + x] for x in range(4))
            elif level == 2:
                totals[child] = sum(received_ref[x * 2 + child] for x in range(4))
        finish(arriving)
        for child in range(2):
            for k in range(blocks):
                if level < 3:
                    piece = totals[child][:, k * BLOCK : (k + 1) * BLOCK]
                else:
                    piece = received_ref[(k // 2) * 4 + child * 2 + k % 2]
                where = block_at(child_block(level, tables_refs, child, k))
                b_ref[:, where] = b_ref[:, where] - piece
        solved = jnp.zeros((HALF, 2 * PIVOTS), jnp.float32)
        for k in range(chunks):
            columns[k].wait()
            at = slice(k * 512, (k + 1) * 512)
            solved += product(b_ref[:, at], weights_ref[k, 0], weights_ref[k, 1], 1)
        weighted = pivot_apply(solved, *both_factors(level, factors_ref, beside_ref))
        if level < 3:
            own_ref[...] = weighted
            leaving.append(moves.start(own_ref, outs[1]))
            if level == 1:
                finish(passing)
                leaving.append(moves.start(passing_ref, outs[2]))
            for k in range(update_len // 256):
                at = slice(k * 256, (k + 1) * 256)
                part_ref[:, at] = product(solved, updates_ref[0][0, :, at], updates_ref[0][1, :, at], 0)
            for i in range(8):
                source = part_ref if level == 1 else part_ref.at[:, pl.ds(i * BLOCK, BLOCK)]
                leaving.append(moves.start(source, outs[0].at[i]))
        else:
            sent_ref, keep_ref, beyond_ref = outs
            for k in range(chunks):
                at = slice(k * 512, (k + 1) * 512)
                b_ref[:, at] = product(weighted, weights_ref[k, 0], weights_ref[k, 1], 0)
            for child in range(2):
                for k in range(8):
                    where = block_at(child_block(3, tables_refs, child, k))
                    leaving.append(
                        moves.start(b_ref.at[:, where], sent_ref.at[(k // 2) * 4 + child * 2 + k % 2])
                    )
            for out, bit in ((beyond_ref, 1 - y1), (keep_ref, y1)):
                for x in range(4):
                    for low in range(2):
                        where = block_at(x * 4 + bit * 2 + low, 256)
                        leaving.append(moves.start(b_ref.at[:, where], out.at[x, low]))
        finish(leaving)

    outs = {
        1: [(8, HALF, 512), (HALF, 256), (2, 4, SIDES, PIVOTS)],
        2: [(8, HALF, BLOCK), (HALF, 256)],
        3: [(16, HALF, BLOCK), (4, 2, HALF, 256), (4, 2, HALF, 256)],
    }[level]
    operands = [*map(far, tables), received, close(factors), close(partner_factors)]
    operands += [close(updates)] if level < 3 else []
    n_close = len(operands) - 4
    operands += map(far, [*sides, weights])
    specs = [SCALARS] * 4 + [WHOLE] * n_close + [FAR] * (n_sides + 1)
    scratch = [
        pltpu.SemaphoreType.DMA((80,)),
        pltpu.VMEM((HALF, span), jnp.float32),
        pltpu.VMEM((HALF, 256), jnp.float32),
        pltpu.VMEM((chunks, 2, 256, 512), jnp.bfloat16),
    ]
    if level < 3:
        scratch.append(pltpu.VMEM((HALF, update_len), jnp.float32))
    if level == 1:
        scratch.append(pltpu.VMEM((2, 4, SIDES, PIVOTS), jnp.float32))
    return call(body, outs, operands, specs, scratch, spaces="H" * n_outs)


def backward(level, received, weighted, tables, weights, updates, answers):
    width = 1 << level
    span = 4 * PIVOTS * width
    chunks = span // 512
    update_len = 2 * PIVOTS * width
    blocks = (2, 4)[level - 1]
    n_answers = len(answers)
    n_outs = (2, 3)[level - 1]

    def body(*refs):
        refs = list(refs)

        def take(count):
            taken, refs[:] = refs[:count], refs[count:]
            return taken

        tables_refs = take(4)
        received_ref, updates_ref = take(2)
        weighted_far, weights_far = take(2)
        answers_far = take(n_answers)
        outs = take(n_outs)
        semaphores, x_ref, weighted_ref, weights_ref, pieces_ref = take(5)
        moves = Moves(semaphores)
        arriving = moves.start(weighted_far, weighted_ref)
        columns = moves.chunks(weights_far, weights_ref)
        leaving = []
        if level == 2:
            own_ref, other_ref, sums_ref = refs
            both = [moves.start(answers_far[0], own_ref), moves.start(answers_far[1], other_ref)]
        if level == 1:
            total = sum(received_ref[i] for i in range(8))
        arriving.wait()
        target = weighted_ref[...]
        for k in range(update_len // 256):
            at = slice(k * 256, (k + 1) * 256)
            if level == 1:
                chosen = total[:, at]
            else:
                chosen = jnp.concatenate([received_ref[2 * k], received_ref[2 * k + 1]], 1)
            target -= product(chosen, updates_ref[0, :, at], updates_ref[1, :, at], 1)
        for k in range(chunks):
            columns[k].wait()
            at = slice(k * 512, (k + 1) * 512)
            x_ref[:, at] = product(target, weights_ref[k, 0], weights_ref[k, 1], 0)
        for child in range(2):
            for k in range(blocks):
                where = block_at(child_block(level, tables_refs, child, k))
                at = slice(k * BLOCK, (k + 1) * BLOCK)
                if level == 1:
                    for x in range(4):
                        outs[0][x * 2 + child, :, at] = x_ref[:, where]
                else:
                    pieces_ref[child, :, at] = x_ref[:, where]
            if level == 2:
                for x in range(4):
                    leaving.append(moves.start(pieces_ref.at[child], outs[0].at[x * 2 + child]))
        if level == 1:
            for x in range(4):
                leaving.append(moves.start(x_ref.at[:, pl.ds(x * 256, 256)], outs[1].at[x]))
        else:
            y0 = lax.axis_index("y0")
            keep_out, beyond_out = outs[1:]
            for out, bit in ((beyond_out, 1 - y0), (keep_out, y0)):
                for x in range(4):
                    where = block_at(x * 2 + bit, 256)
                    leaving.append(moves.start(x_ref.at[:, where], out.at[0, x]))
            finish(both)
            for i, (out, bit) in enumerate(((beyond_out, 1 - y0), (keep_out, y0))):
                for x in range(4):
                    sums_ref[i, x] = own_ref[x, bit] + other_ref[x, bit]
                leaving.append(moves.start(sums_ref.at[i], out.at[1]))
        finish(leaving)

    outs = [(8, HALF, blocks * BLOCK)]
    outs += [(4, HALF, 256)] if level == 1 else [(2, 4, HALF, 256), (2, 4, HALF, 256)]
    operands = [*map(far, tables), received, close(updates), *map(far, [weighted, weights, *answers])]
    specs = [SCALARS] * 4 + [WHOLE] * 2 + [FAR] * (len(operands) - 6)
    scratch = [
        pltpu.SemaphoreType.DMA((64,)),
        pltpu.VMEM((HALF, span), jnp.float32),
        pltpu.VMEM((HALF, 256), jnp.float32),
        pltpu.VMEM((chunks, 2, 256, 512), jnp.bfloat16),
        pltpu.VMEM((2, HALF, blocks * BLOCK), jnp.float32),
    ]
    if level == 2:
        scratch += [pltpu.VMEM((4, 2, HALF, 256), jnp.float32)] * 2 + [pltpu.VMEM((2, 4, HALF, 256), jnp.float32)]
    return call(body, outs, operands, specs, scratch, spaces="vH" if level == 1 else "HHH")


def level_zero_backward(received, weighted, weights, updates, nearest, kept, other):
    def body(received_ref, weighted_ref, nearest_ref, kept_ref, other_ref, weights_ref, updates_ref, sent_ref):
        for x in range(4):
            for c in range(2):
                half = slice(c * HALF, (c + 1) * HALF)
                at = slice(c * PIVOTS, (c + 1) * PIVOTS)
                sent_ref[x, half, PIVOTS : 2 * PIVOTS] = nearest_ref[x, :, at]
                for i in range(2):
                    piece = kept_ref[i, x, :, at] + other_ref[i, x, :, at]
                    sent_ref[x, half, (2 + i) * PIVOTS : (3 + i) * PIVOTS] = piece
        chosen = jnp.concatenate([sum(received_ref[x * 2 + c] for x in range(4)) for c in range(2)], 0)
        target = weighted_ref[...] - product(chosen, updates_ref[0], updates_ref[1], 1)
        part = product(target, weights_ref[0], weights_ref[1], 0)
        for q in range(4):
            sent_ref[q, :, :PIVOTS] = part[:, q * PIVOTS : (q + 1) * PIVOTS]

    return call(
        body,
        [(4, SIDES, 512)],
        [received, *map(far, [weighted, nearest, kept]), other, close(weights), close(updates)],
        [WHOLE] * 7,
        spaces="v",
    )[0]


def summed(received):
    def body(received_ref, out_ref):
        out_ref[...] = (received_ref[0] + received_ref[1]) + (received_ref[2] + received_ref[3])

    return call(body, [(SIDES, 512)], [received], [WHOLE])[0]


def unpacked(total, beside):
    def body(total_ref, beside_ref, out_ref):
        c = lax.axis_index("c")
        mine = pl.ds(pl.multiple_of(c * HALF, 8), HALF)
        theirs = pl.ds(pl.multiple_of((1 - c) * HALF, 8), HALF)
        out_ref[:, :PIVOTS] = total_ref[:, :PIVOTS]
        out_ref[mine, PIVOTS:] = total_ref[mine, PIVOTS:]
        out_ref[theirs, PIVOTS:] = beside_ref[mine, PIVOTS:]

    return call(body, [(SIDES, 512)], [total, beside], [WHOLE] * 2)[0]


def summed_copies(received, count):
    total = jnp.sum(received, 0)
    return jnp.broadcast_to(total[None], (count, *total.shape))


def sibling_tables(targets):
    pairs = []
    for y1 in range(2):
        for y0 in range(2):
            here = y1 * 4 + y0 * 2
            pairs.append((here, y1 * 4 + (1 - y0) * 2))
            pairs.append((here + 1, (1 - y1) * 4 + y0 * 2 + 1))
    side = lax.ppermute(targets, ("y1", "y0", "c"), pairs)
    return [targets, side, with_partner(targets), with_partner(side)]


def per_device(right_side, factor_inverse, update_panel, update_targets, pivot_pairs, pivot_diagonal, pivot_coupling):
    sides = right_side[0, 0]
    inverse = factor_inverse[0, 0]
    update = update_panel[0, 0]
    plane = ("x", "y1", "y0")
    pair = ("x", "y0")

    packed = packed_sides(sides, with_partner(sides))
    first = exchange(packed, ("x",))
    factors = pivot_factors(pivot_pairs[0], pivot_diagonal[0], pivot_coupling[0])
    partner_factors = with_partner(factors)
    inverse_after, update_after, _ = lax.optimization_barrier((inverse, update, packed))
    partner_inverse = with_partner(inverse_after)
    partner_update = with_partner(update_after)
    (weights0,) = prepared([inverse], [(0, 512, None)], packed)
    (updates0,) = prepared([update], [(0, 256, None)], packed)
    first, partner_factors, *tables = lax.optimization_barrier(
        (first, partner_factors, *sibling_tables(update_targets))
    )

    sent, weighted0, sides1, near = level_zero_forward(first, weights0, updates0, factors)
    beyond = across(near, "y0")
    received = exchange(sent, ("c", "x"))
    (weights1,) = prepared([inverse, partner_inverse], [(512, 1024, 512)], sent)
    (updates1,) = prepared([update, partner_update], [(256, 512, None)], sent)
    sent, weighted1, near3 = forward(
        1, received, [sides1, near, beyond], tables, weights1, updates1, factors, partner_factors
    )
    weights2, weights3 = prepared([inverse, partner_inverse], [(1536, 2048, 512), (3584, 4096, 512)], sent)
    (updates2,) = prepared([update, partner_update], [(768, 1024, None)], sent)
    beyond3 = across(near3, "y1")
    received = exchange(sent, pair)
    sent, weighted2 = forward(2, received, [near, beyond], tables, weights2, updates2, factors, partner_factors)
    received = exchange(summed_copies(exchange(sent, pair), 16), plane)
    sent, kept3, other3 = forward(3, received, [near3, beyond3], tables, weights3, None, factors, partner_factors)
    other3 = across(other3, "y1")
    received = exchange(summed_copies(exchange(sent, plane), 8), pair)
    sent, kept, other = backward(2, received, weighted2, tables, weights2, updates2, [kept3, other3])
    other = across(other, "y0")
    received = exchange(sent, pair)
    sent, nearest = backward(1, received, weighted1, tables, weights1, updates1, [])
    sent, other = lax.optimization_barrier((sent, other))
    received = exchange(sent, ("x", "c"))
    sent = level_zero_backward(received, weighted0, weights0, updates0, nearest, kept, other)
    total = summed(exchange(sent, ("x",)))
    return unpacked(total, with_partner(total))[None, None]


def solution(mesh):
    grid = np.array(mesh.devices).reshape(4, 2, 2, 2, 4)
    fine = Mesh(grid, AXES)
    leaf = ("z", "y1", "y0", "c")
    in_specs = (
        P(leaf, "x", None, None),
        P(leaf, "x", None, None),
        P(leaf, "x", None, None),
        P(leaf, None),
        P(leaf, "x", None),
        P(leaf, "x", None),
        P(leaf, "x", None),
    )
    out_specs = P(leaf, "x", None, None)
    return jax.shard_map(per_device, mesh=fine, in_specs=in_specs, out_specs=out_specs, check_vma=False)
```

```python
import jax
import jax.numpy as jnp
import numpy as np
from jax import lax
from jax.experimental import pallas as pl
from jax.experimental.pallas import tpu as pltpu
from jax.sharding import Mesh, PartitionSpec as P

LEVELS = 4
BLOCK = 128
PIVOTS = 128
SIDES = 96
HALF = SIDES // 2
AXES = ("z", "y1", "y0", "c", "x")

exact_mode = lax.Precision.HIGHEST


def parts(value):
    high = value.astype(jnp.bfloat16)
    return high, (value - high.astype(jnp.float32)).astype(jnp.bfloat16)


def product(left, high, low, side):
    left_high, left_low = parts(left)
    dims = (((1,), (side,)), ((), ()))

    def dot(a, b):
        return lax.dot_general(a, b, dims, preferred_element_type=jnp.float32)

    both = dot(jnp.concatenate([left_high, left_low], 0), high)
    rows = left.shape[0]
    return both[:rows] + (dot(left_high, low) + both[rows:])


def dot_full(left, right):
    return lax.dot_general(
        left, right, (((1,), (0,)), ((), ())), precision=exact_mode, preferred_element_type=jnp.float32
    )


def exchange(value, axes):
    return lax.all_to_all(value, axes, 0, 0, tiled=True)


def with_partner(value):
    return lax.ppermute(value, "c", [(0, 1), (1, 0)])


def across(value, axis):
    return lax.ppermute(value, axis, [(0, 1), (1, 0)])


def block_at(index, size=BLOCK):
    return pl.ds(pl.multiple_of(index * size, size), size)


WHOLE = pl.BlockSpec(memory_space=pltpu.VMEM)
SCALARS = pl.BlockSpec(memory_space=pltpu.SMEM)
FAR = pl.BlockSpec(memory_space=pltpu.HBM)


def far(value):
    return pltpu.with_memory_space_constraint(value, pltpu.HBM)


def close(value):
    return pltpu.with_memory_space_constraint(value, pltpu.VMEM)


def call(body, out_shapes, operands, specs, scratch=(), limit=20, spaces=None):
    return pl.pallas_call(
        body,
        in_specs=specs,
        out_specs=[FAR if k == "H" else WHOLE for k in spaces or "-" * len(out_shapes)],
        out_shape=[
            {"H": pltpu.HBM, "h": pltpu.HBM, "v": pltpu.VMEM, "-": jax.ShapeDtypeStruct}[k](s, jnp.float32)
            for s, k in zip(out_shapes, spaces or "-" * len(out_shapes))
        ],
        scratch_shapes=list(scratch),
        compiler_params=pltpu.CompilerParams(vmem_limit_bytes=limit * 1024 * 1024),
    )(*operands)


def prepared(pair, spans, after):
    def body(*refs):
        sources = refs[: len(pair)]
        outs = refs[len(pair) + 1 :][: len(spans)]
        buffers = refs[len(pair) + 1 + len(spans) : -1]
        semaphores = refs[-1]
        moves = []
        for i, (start, width, _) in enumerate(spans):
            for side, source in enumerate(sources):
                move = pltpu.make_async_copy(
                    source.at[:, pl.ds(start, width)],
                    buffers[i].at[pl.ds(side * PIVOTS, PIVOTS), :],
                    semaphores.at[i, side],
                )
                move.start()
                moves.append((i, side, move))
        for i, side, move in moves:
            move.wait()
            rows = slice(side * PIVOTS, (side + 1) * PIVOTS)
            _, width, step = spans[i]
            for k, at in enumerate(range(0, width, step or width)):
                high, low = parts(buffers[i][rows, at : at + (step or width)])
                place = outs[i].at[k] if step else outs[i]
                place[0, rows] = high
                place[1, rows] = low

    count = len(pair) * PIVOTS
    shapes = [
        pltpu.HBM((width // step, 2, count, step), jnp.bfloat16) if step else pltpu.VMEM((2, count, width), jnp.bfloat16)
        for _, width, step in spans
    ]
    return pl.pallas_call(
        body,
        in_specs=[FAR] * (len(pair) + 1),
        out_specs=[WHOLE] * len(spans),
        out_shape=shapes,
        scratch_shapes=[pltpu.VMEM((count, width), jnp.float32) for _, width, _ in spans]
        + [pltpu.SemaphoreType.DMA((len(spans), len(pair)))],
        compiler_params=pltpu.CompilerParams(vmem_limit_bytes=28 * 1024 * 1024),
    )(*map(far, pair), far(after))


def pivot_apply(solved, own, swapped):
    lane = lax.broadcasted_iota(jnp.int32, solved.shape, 1)
    width = solved.shape[1]
    beside = jnp.where(lane % 2 == 0, pltpu.roll(solved, width - 1, 1), pltpu.roll(solved, 1, 1))
    return own * solved + swapped * beside


def pivot_factors(kinds, diagonal, coupling):
    def body(kinds_ref, diagonal_ref, coupling_ref, out_ref):
        width = diagonal_ref.shape[1]
        row = lax.broadcasted_iota(jnp.int32, (width // 2, width), 0)
        col = lax.broadcasted_iota(jnp.int32, (width // 2, width), 1)
        widen = (col // 2 == row).astype(jnp.float32)
        pair = jnp.concatenate(
            [kinds_ref[...].astype(jnp.float32), coupling_ref[...], jnp.zeros((6, width // 2), jnp.float32)], 0
        )
        wide = dot_full(pair, widen)
        is_pair = wide[0:1] > 0.5
        couple = wide[1:2]
        own = jnp.broadcast_to(diagonal_ref[...], (8, width))
        lane = lax.broadcasted_iota(jnp.int32, (8, width), 1)
        other = jnp.where(lane % 2 == 0, pltpu.roll(own, width - 1, 1), pltpu.roll(own, 1, 1))[0:1]
        own = own[0:1]
        determinant = own * other - couple * couple
        out_ref[0:1, :] = jnp.where(is_pair, other / determinant, 1.0 / own)
        out_ref[1:2, :] = jnp.where(is_pair, -couple / determinant, 0.0)

    operands = [far(kinds), far(diagonal), far(coupling)]
    return call(body, [(2, diagonal.shape[1])], operands, [WHOLE] * 3, spaces="v")[0]


def packed_sides(sides, beside):
    def body(sides_ref, beside_ref, out_ref):
        c = lax.axis_index("c")
        mine = pl.ds(pl.multiple_of(c * HALF, 8), HALF)
        theirs = pl.ds(pl.multiple_of((1 - c) * HALF, 8), HALF)
        own = sides_ref[mine, PIVOTS:]
        other = beside_ref[mine, PIVOTS:]
        for i in range(4):
            out_ref[i, :, :PIVOTS] = sides_ref[:, :PIVOTS]
            out_ref[i, mine, PIVOTS:] = own
            out_ref[i, theirs, PIVOTS:] = other

    return call(body, [(4, SIDES, 512)], [far(sides), beside], [WHOLE] * 2, spaces="h")[0]


class Moves:
    def __init__(self, semaphores):
        self.semaphores, self.started = semaphores, []

    def start(self, source, target):
        move = pltpu.make_async_copy(source, target, self.semaphores.at[len(self.started)])
        move.start()
        self.started.append(move)
        return move

    def chunks(self, source, target):
        return [self.start(source.at[k], target.at[k]) for k in range(source.shape[0])]


def finish(moves):
    for move in moves:
        move.wait()


def level_zero_forward(first, weights, updates, factors):
    def body(first_ref, weights_ref, updates_ref, factors_ref, *refs):
        sent_ref, weighted_ref, one_ref, upper_ref, part_ref, own_ref, semaphores = refs
        moves = Moves(semaphores)
        leaving = [
            moves.start(first_ref.at[:, :, pl.ds(PIVOTS, PIVOTS)], one_ref),
            moves.start(first_ref.at[:, :, pl.ds(2 * PIVOTS, 2 * PIVOTS)], upper_ref),
        ]
        gathered = jnp.concatenate([first_ref[q, :, :PIVOTS] for q in range(4)], 1)
        solved = product(gathered, weights_ref[0], weights_ref[1], 1)
        part_ref[...] = product(solved, updates_ref[0], updates_ref[1], 0)
        for c in range(2):
            for x in range(4):
                leaving.append(moves.start(part_ref.at[pl.ds(c * HALF, HALF)], sent_ref.at[c * 4 + x]))
        own_ref[...] = pivot_apply(solved, factors_ref[0:1, :PIVOTS], factors_ref[1:2, :PIVOTS])
        leaving.append(moves.start(own_ref, weighted_ref))
        finish(leaving)

    return call(
        body,
        [(8, HALF, 256), (SIDES, PIVOTS), (4, SIDES, PIVOTS), (4, SIDES, 256)],
        [close(first), close(weights), close(updates), close(factors)],
        [WHOLE] * 4,
        [
            pltpu.VMEM((SIDES, 256), jnp.float32),
            pltpu.VMEM((SIDES, PIVOTS), jnp.float32),
            pltpu.SemaphoreType.DMA((16,)),
        ],
        spaces="HHHH",
    )


def child_block(level, tables, child, k):
    own_ref, side_ref, own_beside_ref, side_beside_ref = tables
    c = lax.axis_index("c")
    if level == 1:
        return jnp.where(c == child, own_ref[0, k], own_beside_ref[0, k])
    if level == 2:
        sibling = jnp.where(c == 0, side_ref[0, 2 + k], side_beside_ref[0, 2 + k])
        return jnp.where(lax.axis_index("y0") == child, own_ref[0, 2 + k], sibling)
    sibling = jnp.where(c == 0, side_beside_ref[0, 6 + k], side_ref[0, 6 + k])
    return jnp.where(lax.axis_index("y1") == child, own_ref[0, 6 + k], sibling)


def both_factors(level, factors, beside):
    c = lax.axis_index("c")
    at = slice(level * PIVOTS, (level + 1) * PIVOTS)
    return [jnp.concatenate([factors[i : i + 1, at], beside[i : i + 1, at]], 1) for i in range(2)]


def halves(rows):
    return jnp.concatenate([rows[:HALF], rows[HALF:]], 1)


def forward(level, received, sides, tables, weights, updates, factors, partner_factors):
    width = 1 << level
    span = 4 * PIVOTS * width
    chunks = span // 512
    update_len = 2 * PIVOTS * width if level < 3 else 0
    blocks = (2, 4, 8)[level - 1]
    n_sides = len(sides)
    n_updates = 1 if level < 3 else 0
    n_outs = (2, 2, 3)[level - 1]

    def body(*refs):
        refs = list(refs)

        def take(count):
            taken, refs[:] = refs[:count], refs[count:]
            return taken

        tables_refs = take(4)
        received_ref, factors_ref, beside_ref = take(3)
        updates_ref = take(n_updates)
        sides_refs = take(n_sides)
        (weights_far,) = take(1)
        outs = take(n_outs)
        semaphores, b_ref, own_ref, weights_ref = take(4)
        moves = Moves(semaphores)
        x0, y0, y1 = lax.axis_index("x"), lax.axis_index("y0"), lax.axis_index("y1")

        arriving, leaving = [], []

        def bring(source, block):
            for c in range(2):
                arriving.append(moves.start(source.at[pl.ds(c * HALF, HALF)], b_ref.at[:, block_at(block * 2 + c)]))

        if level == 1:
            for x in range(4):
                bring(sides_refs[0].at[x], x)
        elif level == 2:
            for flip in range(2):
                for x in range(4):
                    bring(sides_refs[flip].at[x, :, pl.ds(0, PIVOTS)], x * 2 + (y0 ^ flip))
        else:
            for high in range(2):
                for flip in range(2):
                    for x in range(4):
                        bring(sides_refs[high].at[flip, x], x * 4 + (y1 ^ high) * 2 + (y0 ^ flip))
        columns = moves.chunks(weights_far, weights_ref)
        if level < 3:
            part_ref = refs[0]
        totals = [None, None]
        for child in range(2):
            if level == 1:
                totals[child] = sum(received_ref[child * 4 + x] for x in range(4))
            elif level == 2:
                totals[child] = sum(received_ref[x * 2 + child] for x in range(4))
        finish(arriving)
        for child in range(2):
            for k in range(blocks):
                if level < 3:
                    piece = totals[child][:, k * BLOCK : (k + 1) * BLOCK]
                else:
                    piece = received_ref[(k // 2) * 4 + child * 2 + k % 2]
                where = block_at(child_block(level, tables_refs, child, k))
                b_ref[:, where] = b_ref[:, where] - piece
        solved = jnp.zeros((HALF, 2 * PIVOTS), jnp.float32)
        for k in range(chunks):
            columns[k].wait()
            at = slice(k * 512, (k + 1) * 512)
            solved += product(b_ref[:, at], weights_ref[k, 0], weights_ref[k, 1], 1)
        weighted = pivot_apply(solved, *both_factors(level, factors_ref, beside_ref))
        if level < 3:
            own_ref[...] = weighted
            leaving.append(moves.start(own_ref, outs[1]))
            for k in range(update_len // 256):
                at = slice(k * 256, (k + 1) * 256)
                part_ref[:, at] = product(solved, updates_ref[0][0, :, at], updates_ref[0][1, :, at], 0)
            for i in range(8):
                source = part_ref if level == 1 else part_ref.at[:, pl.ds(i * BLOCK, BLOCK)]
                leaving.append(moves.start(source, outs[0].at[i]))
        else:
            sent_ref, keep_ref, beyond_ref = outs
            for k in range(chunks):
                at = slice(k * 512, (k + 1) * 512)
                b_ref[:, at] = product(weighted, weights_ref[k, 0], weights_ref[k, 1], 0)
            for child in range(2):
                for k in range(8):
                    where = block_at(child_block(3, tables_refs, child, k))
                    leaving.append(
                        moves.start(b_ref.at[:, where], sent_ref.at[(k // 2) * 4 + child * 2 + k % 2])
                    )
            for out, bit in ((beyond_ref, 1 - y1), (keep_ref, y1)):
                for x in range(4):
                    for low in range(2):
                        where = block_at(x * 4 + bit * 2 + low, 256)
                        leaving.append(moves.start(b_ref.at[:, where], out.at[x, low]))
        finish(leaving)

    outs = {
        1: [(8, HALF, 512), (HALF, 256)],
        2: [(8, HALF, BLOCK), (HALF, 256)],
        3: [(16, HALF, BLOCK), (4, 2, HALF, 256), (4, 2, HALF, 256)],
    }[level]
    operands = [*map(far, tables), received, close(factors), close(partner_factors)]
    operands += [close(updates)] if level < 3 else []
    n_close = len(operands) - 4
    operands += map(far, [*sides, weights])
    specs = [SCALARS] * 4 + [WHOLE] * n_close + [FAR] * (n_sides + 1)
    scratch = [
        pltpu.SemaphoreType.DMA((80,)),
        pltpu.VMEM((HALF, span), jnp.float32),
        pltpu.VMEM((HALF, 256), jnp.float32),
        pltpu.VMEM((chunks, 2, 256, 512), jnp.bfloat16),
    ]
    if level < 3:
        scratch.append(pltpu.VMEM((HALF, update_len), jnp.float32))
    return call(body, outs, operands, specs, scratch, spaces="H" * n_outs)


def backward(level, received, weighted, tables, weights, updates, answers):
    width = 1 << level
    span = 4 * PIVOTS * width
    chunks = span // 512
    update_len = 2 * PIVOTS * width
    blocks = (2, 4)[level - 1]
    n_answers = len(answers)
    n_outs = (2, 3)[level - 1]

    def body(*refs):
        refs = list(refs)

        def take(count):
            taken, refs[:] = refs[:count], refs[count:]
            return taken

        tables_refs = take(4)
        received_ref, updates_ref = take(2)
        weighted_far, weights_far = take(2)
        answers_far = take(n_answers)
        outs = take(n_outs)
        semaphores, x_ref, weighted_ref, weights_ref, pieces_ref = take(5)
        moves = Moves(semaphores)
        arriving = moves.start(weighted_far, weighted_ref)
        columns = moves.chunks(weights_far, weights_ref)
        leaving = []
        if level == 2:
            own_ref, other_ref, sums_ref = refs
            both = [moves.start(answers_far[0], own_ref), moves.start(answers_far[1], other_ref)]
        if level == 1:
            total = sum(received_ref[i] for i in range(8))
        arriving.wait()
        target = weighted_ref[...]
        for k in range(update_len // 256):
            at = slice(k * 256, (k + 1) * 256)
            if level == 1:
                chosen = total[:, at]
            else:
                chosen = jnp.concatenate([received_ref[2 * k], received_ref[2 * k + 1]], 1)
            target -= product(chosen, updates_ref[0, :, at], updates_ref[1, :, at], 1)
        for k in range(chunks):
            columns[k].wait()
            at = slice(k * 512, (k + 1) * 512)
            x_ref[:, at] = product(target, weights_ref[k, 0], weights_ref[k, 1], 0)
        for child in range(2):
            for k in range(blocks):
                where = block_at(child_block(level, tables_refs, child, k))
                at = slice(k * BLOCK, (k + 1) * BLOCK)
                pieces_ref[child, :, at] = x_ref[:, where]
            for x in range(4):
                leaving.append(moves.start(pieces_ref.at[child], outs[0].at[x * 2 + child]))
        if level == 1:
            for x in range(4):
                leaving.append(moves.start(x_ref.at[:, pl.ds(x * 256, 256)], outs[1].at[x]))
        else:
            y0 = lax.axis_index("y0")
            keep_out, beyond_out = outs[1:]
            for out, bit in ((beyond_out, 1 - y0), (keep_out, y0)):
                for x in range(4):
                    where = block_at(x * 2 + bit, 256)
                    leaving.append(moves.start(x_ref.at[:, where], out.at[0, x]))
            finish(both)
            for i, (out, bit) in enumerate(((beyond_out, 1 - y0), (keep_out, y0))):
                for x in range(4):
                    sums_ref[i, x] = own_ref[x, bit] + other_ref[x, bit]
                leaving.append(moves.start(sums_ref.at[i], out.at[1]))
        finish(leaving)

    outs = [(8, HALF, blocks * BLOCK)]
    outs += [(4, HALF, 256)] if level == 1 else [(2, 4, HALF, 256), (2, 4, HALF, 256)]
    operands = [*map(far, tables), received, close(updates), *map(far, [weighted, weights, *answers])]
    specs = [SCALARS] * 4 + [WHOLE] * 2 + [FAR] * (len(operands) - 6)
    scratch = [
        pltpu.SemaphoreType.DMA((64,)),
        pltpu.VMEM((HALF, span), jnp.float32),
        pltpu.VMEM((HALF, 256), jnp.float32),
        pltpu.VMEM((chunks, 2, 256, 512), jnp.bfloat16),
        pltpu.VMEM((2, HALF, blocks * BLOCK), jnp.float32),
    ]
    if level == 2:
        scratch += [pltpu.VMEM((4, 2, HALF, 256), jnp.float32)] * 2 + [pltpu.VMEM((2, 4, HALF, 256), jnp.float32)]
    return call(body, outs, operands, specs, scratch, spaces="H" * n_outs)


def level_zero_backward(received, weighted, weights, updates, nearest, kept, other):
    def body(received_ref, weighted_ref, nearest_ref, kept_ref, other_ref, weights_ref, updates_ref, sent_ref):
        for x in range(4):
            for c in range(2):
                half = slice(c * HALF, (c + 1) * HALF)
                at = slice(c * PIVOTS, (c + 1) * PIVOTS)
                sent_ref[x, half, PIVOTS : 2 * PIVOTS] = nearest_ref[x, :, at]
                for i in range(2):
                    piece = kept_ref[i, x, :, at] + other_ref[i, x, :, at]
                    sent_ref[x, half, (2 + i) * PIVOTS : (3 + i) * PIVOTS] = piece
        chosen = jnp.concatenate([sum(received_ref[x * 2 + c] for x in range(4)) for c in range(2)], 0)
        target = weighted_ref[...] - product(chosen, updates_ref[0], updates_ref[1], 1)
        part = product(target, weights_ref[0], weights_ref[1], 0)
        for q in range(4):
            sent_ref[q, :, :PIVOTS] = part[:, q * PIVOTS : (q + 1) * PIVOTS]

    return call(
        body,
        [(4, SIDES, 512)],
        [received, *map(far, [weighted, nearest, kept]), other, close(weights), close(updates)],
        [WHOLE] * 7,
        spaces="v",
    )[0]


def summed(received):
    def body(received_ref, out_ref):
        out_ref[...] = (received_ref[0] + received_ref[1]) + (received_ref[2] + received_ref[3])

    return call(body, [(SIDES, 512)], [received], [WHOLE])[0]


def unpacked(total, beside):
    def body(total_ref, beside_ref, out_ref):
        c = lax.axis_index("c")
        mine = pl.ds(pl.multiple_of(c * HALF, 8), HALF)
        theirs = pl.ds(pl.multiple_of((1 - c) * HALF, 8), HALF)
        out_ref[:, :PIVOTS] = total_ref[:, :PIVOTS]
        out_ref[mine, PIVOTS:] = total_ref[mine, PIVOTS:]
        out_ref[theirs, PIVOTS:] = beside_ref[mine, PIVOTS:]

    return call(body, [(SIDES, 512)], [total, beside], [WHOLE] * 2)[0]


def summed_copies(received, count):
    total = jnp.sum(received, 0)
    return jnp.broadcast_to(total[None], (count, *total.shape))


def sibling_tables(targets):
    pairs = []
    for y1 in range(2):
        for y0 in range(2):
            here = y1 * 4 + y0 * 2
            pairs.append((here, y1 * 4 + (1 - y0) * 2))
            pairs.append((here + 1, (1 - y1) * 4 + y0 * 2 + 1))
    side = lax.ppermute(targets, ("y1", "y0", "c"), pairs)
    return [targets, side, with_partner(targets), with_partner(side)]


def per_device(right_side, factor_inverse, update_panel, update_targets, pivot_pairs, pivot_diagonal, pivot_coupling):
    sides = right_side[0, 0]
    inverse = factor_inverse[0, 0]
    update = update_panel[0, 0]
    plane = ("x", "y1", "y0")
    pair = ("x", "y0")

    packed = packed_sides(sides, with_partner(sides))
    first = exchange(packed, ("x",))
    factors = pivot_factors(pivot_pairs[0], pivot_diagonal[0], pivot_coupling[0])
    partner_factors = with_partner(factors)
    inverse_after, update_after, _ = lax.optimization_barrier((inverse, update, packed))
    partner_inverse = with_partner(inverse_after)
    partner_update = with_partner(update_after)
    (weights0,) = prepared([inverse], [(0, 512, None)], packed)
    (updates0,) = prepared([update], [(0, 256, None)], packed)
    first, partner_factors, *tables = lax.optimization_barrier(
        (first, partner_factors, *sibling_tables(update_targets))
    )

    sent, weighted0, sides1, near = level_zero_forward(first, weights0, updates0, factors)
    beyond = across(near, "y0")
    received = exchange(sent, ("c", "x"))
    (weights1,) = prepared([inverse, partner_inverse], [(512, 1024, 512)], sent)
    (updates1,) = prepared([update, partner_update], [(256, 512, None)], sent)
    sent, weighted1 = forward(1, received, [sides1], tables, weights1, updates1, factors, partner_factors)
    sent, beyond = lax.optimization_barrier((sent, beyond))
    weights2, weights3 = prepared([inverse, partner_inverse], [(1536, 2048, 512), (3584, 4096, 512)], sent)
    (updates2,) = prepared([update, partner_update], [(768, 1024, None)], sent)
    received = exchange(sent, pair)
    near3, _ = lax.optimization_barrier((jnp.stack([near[:, :, PIVOTS:], beyond[:, :, PIVOTS:]]), sent))
    beyond3 = across(near3, "y1")
    sent, weighted2 = forward(2, received, [near, beyond], tables, weights2, updates2, factors, partner_factors)
    received = exchange(summed_copies(exchange(sent, pair), 16), plane)
    sent, kept3, other3 = forward(3, received, [near3, beyond3], tables, weights3, None, factors, partner_factors)
    other3 = across(other3, "y1")
    received = exchange(summed_copies(exchange(sent, plane), 8), pair)
    sent, kept, other = backward(2, received, weighted2, tables, weights2, updates2, [kept3, other3])
    other = across(other, "y0")
    received = exchange(sent, pair)
    sent, nearest = backward(1, received, weighted1, tables, weights1, updates1, [])
    received = exchange(sent, ("x", "c"))
    sent = level_zero_backward(received, weighted0, weights0, updates0, nearest, kept, other)
    total = summed(exchange(sent, ("x",)))
    return unpacked(total, with_partner(total))[None, None]


def solution(mesh):
    grid = np.array(mesh.devices).reshape(4, 2, 2, 2, 4)
    fine = Mesh(grid, AXES)
    leaf = ("z", "y1", "y0", "c")
    in_specs = (
        P(leaf, "x", None, None),
        P(leaf, "x", None, None),
        P(leaf, "x", None, None),
        P(leaf, None),
        P(leaf, "x", None),
        P(leaf, "x", None),
        P(leaf, "x", None),
    )
    out_specs = P(leaf, "x", None, None)
    return jax.shard_map(per_device, mesh=fine, in_specs=in_specs, out_specs=out_specs, check_vma=False)
```

```python
import jax
import jax.numpy as jnp
import numpy as np
from jax import lax
from jax.experimental import pallas as pl
from jax.experimental.pallas import tpu as pltpu
from jax.sharding import Mesh, PartitionSpec as P


BLOCK = 128
PIVOTS = 128
SIDES = 96
HALF = SIDES // 2
AXES = ("z", "y1", "y0", "c", "x")

exact_mode = lax.Precision.HIGHEST


def parts(value):
    high = value.astype(jnp.bfloat16)
    return high, (value - high.astype(jnp.float32)).astype(jnp.bfloat16)


def product(left, high, low, side):
    left_high, left_low = parts(left)
    dims = (((1,), (side,)), ((), ()))

    def dot(a, b):
        return lax.dot_general(a, b, dims, preferred_element_type=jnp.float32)

    both = dot(jnp.concatenate([left_high, left_low], 0), high)
    rows = left.shape[0]
    return both[:rows] + (dot(left_high, low) + both[rows:])


def dot_full(left, right):
    return lax.dot_general(
        left, right, (((1,), (0,)), ((), ())), precision=exact_mode, preferred_element_type=jnp.float32
    )


def exchange(value, axes):
    return lax.all_to_all(value, axes, 0, 0, tiled=True)


def with_partner(value):
    return lax.ppermute(value, "c", [(0, 1), (1, 0)])


def across(value, axis):
    return lax.ppermute(value, axis, [(0, 1), (1, 0)])


def block_at(index, size=BLOCK):
    return pl.ds(pl.multiple_of(index * size, size), size)


WHOLE = pl.BlockSpec(memory_space=pltpu.VMEM)
SCALARS = pl.BlockSpec(memory_space=pltpu.SMEM)
FAR = pl.BlockSpec(memory_space=pltpu.HBM)


def far(value):
    return pltpu.with_memory_space_constraint(value, pltpu.HBM)


def close(value):
    return pltpu.with_memory_space_constraint(value, pltpu.VMEM)


def call(body, out_shapes, operands, specs, scratch=(), limit=20, spaces=None):
    return pl.pallas_call(
        body,
        in_specs=specs,
        out_specs=[FAR if k == "H" else WHOLE for k in spaces or "-" * len(out_shapes)],
        out_shape=[
            {"H": pltpu.HBM, "h": pltpu.HBM, "v": pltpu.VMEM, "-": jax.ShapeDtypeStruct}[k](s, jnp.float32)
            for s, k in zip(out_shapes, spaces or "-" * len(out_shapes))
        ],
        scratch_shapes=list(scratch),
        compiler_params=pltpu.CompilerParams(vmem_limit_bytes=limit * 1024 * 1024),
    )(*operands)


def prepared(pair, spans, after):
    def body(*refs):
        sources = refs[: len(pair)]
        outs = refs[len(pair) + 1 :][: len(spans)]
        buffers = refs[len(pair) + 1 + len(spans) : -1]
        semaphores = refs[-1]
        moves = []
        for i, (start, width, _) in enumerate(spans):
            for side, source in enumerate(sources):
                move = pltpu.make_async_copy(
                    source.at[:, pl.ds(start, width)],
                    buffers[i].at[pl.ds(side * PIVOTS, PIVOTS), :],
                    semaphores.at[i, side],
                )
                move.start()
                moves.append((i, side, move))
        for i, side, move in moves:
            move.wait()
            rows = slice(side * PIVOTS, (side + 1) * PIVOTS)
            _, width, step = spans[i]
            for k, at in enumerate(range(0, width, step or width)):
                high, low = parts(buffers[i][rows, at : at + (step or width)])
                place = outs[i].at[k] if step else outs[i]
                place[0, rows] = high
                place[1, rows] = low

    count = len(pair) * PIVOTS
    shapes = [
        pltpu.HBM((width // step, 2, count, step), jnp.bfloat16) if step else pltpu.VMEM((2, count, width), jnp.bfloat16)
        for _, width, step in spans
    ]
    return pl.pallas_call(
        body,
        in_specs=[FAR] * (len(pair) + 1),
        out_specs=[WHOLE] * len(spans),
        out_shape=shapes,
        scratch_shapes=[pltpu.VMEM((count, width), jnp.float32) for _, width, _ in spans]
        + [pltpu.SemaphoreType.DMA((len(spans), len(pair)))],
        compiler_params=pltpu.CompilerParams(vmem_limit_bytes=28 * 1024 * 1024),
    )(*map(far, pair), far(after))


def pivot_apply(solved, own, swapped):
    lane = lax.broadcasted_iota(jnp.int32, solved.shape, 1)
    width = solved.shape[1]
    beside = jnp.where(lane % 2 == 0, pltpu.roll(solved, width - 1, 1), pltpu.roll(solved, 1, 1))
    return own * solved + swapped * beside


def pivot_factors(kinds, diagonal, coupling):
    def body(kinds_ref, diagonal_ref, coupling_ref, out_ref):
        width = diagonal_ref.shape[1]
        row = lax.broadcasted_iota(jnp.int32, (width // 2, width), 0)
        col = lax.broadcasted_iota(jnp.int32, (width // 2, width), 1)
        widen = (col // 2 == row).astype(jnp.float32)
        pair = jnp.concatenate(
            [kinds_ref[...].astype(jnp.float32), coupling_ref[...], jnp.zeros((6, width // 2), jnp.float32)], 0
        )
        wide = dot_full(pair, widen)
        is_pair = wide[0:1] > 0.5
        couple = wide[1:2]
        own = jnp.broadcast_to(diagonal_ref[...], (8, width))
        lane = lax.broadcasted_iota(jnp.int32, (8, width), 1)
        other = jnp.where(lane % 2 == 0, pltpu.roll(own, width - 1, 1), pltpu.roll(own, 1, 1))[0:1]
        own = own[0:1]
        determinant = own * other - couple * couple
        out_ref[0:1, :] = jnp.where(is_pair, other / determinant, 1.0 / own)
        out_ref[1:2, :] = jnp.where(is_pair, -couple / determinant, 0.0)

    operands = [far(kinds), far(diagonal), far(coupling)]
    return call(body, [(2, diagonal.shape[1])], operands, [WHOLE] * 3, spaces="v")[0]


def gathered_sides(own, other):
    def body(own_ref, other_ref, one_ref, near_ref):
        c = lax.axis_index("c")
        for rows, source in ((c, own_ref), (1 - c, other_ref)):
            place = pl.ds(pl.multiple_of(rows * HALF, 8), HALF)
            for x in range(4):
                one_ref[x, place] = source[x, :, :PIVOTS]
                near_ref[x, place] = source[x, :, PIVOTS:]

    return call(body, [(4, SIDES, PIVOTS), (4, SIDES, 256)], [far(own), other], [WHOLE] * 2, spaces="hh")


def upper_answers(nearest, kept, other):
    def body(nearest_ref, kept_ref, other_ref, own_ref, give_ref):
        c = lax.axis_index("c")
        for core, out in ((c, own_ref), (1 - c, give_ref)):
            at = block_at(core)
            for x in range(4):
                out[x, :, :PIVOTS] = nearest_ref[x, :, at]
                for i in range(2):
                    piece = kept_ref[i, x, :, at] + other_ref[i, x, :, at]
                    out[x, :, (1 + i) * PIVOTS : (2 + i) * PIVOTS] = piece

    return call(body, [(4, HALF, 384)] * 2, [far(nearest), far(kept), other], [WHOLE] * 3, spaces="hh")


class Moves:
    def __init__(self, semaphores):
        self.semaphores, self.started = semaphores, []

    def start(self, source, target):
        move = pltpu.make_async_copy(source, target, self.semaphores.at[len(self.started)])
        move.start()
        self.started.append(move)
        return move

    def chunks(self, source, target):
        return [self.start(source.at[k], target.at[k]) for k in range(source.shape[0])]


def finish(moves):
    for move in moves:
        move.wait()


def level_zero_forward(first, weights, updates, factors):
    def body(first_ref, weights_ref, updates_ref, factors_ref, *refs):
        sent_ref, weighted_ref, keep_ref, give_ref, part_ref, own_ref, semaphores = refs
        moves = Moves(semaphores)
        core = lax.axis_index("c")
        leaving = []
        for half, out in ((core, keep_ref), (1 - core, give_ref)):
            rows = pl.ds(pl.multiple_of(half * HALF, 8), HALF)
            leaving.append(moves.start(first_ref.at[:, rows, pl.ds(PIVOTS, 3 * PIVOTS)], out))
        gathered = jnp.concatenate([first_ref[q, :, :PIVOTS] for q in range(4)], 1)
        solved = product(gathered, weights_ref[0], weights_ref[1], 1)
        part_ref[...] = product(solved, updates_ref[0], updates_ref[1], 0)
        for c in range(2):
            for x in range(4):
                leaving.append(moves.start(part_ref.at[pl.ds(c * HALF, HALF)], sent_ref.at[c * 4 + x]))
        own_ref[...] = pivot_apply(solved, factors_ref[0:1, :PIVOTS], factors_ref[1:2, :PIVOTS])
        leaving.append(moves.start(own_ref, weighted_ref))
        finish(leaving)

    return call(
        body,
        [(8, HALF, 256), (SIDES, PIVOTS), (4, HALF, 384), (4, HALF, 384)],
        [close(first), close(weights), close(updates), close(factors)],
        [WHOLE] * 4,
        [
            pltpu.VMEM((SIDES, 256), jnp.float32),
            pltpu.VMEM((SIDES, PIVOTS), jnp.float32),
            pltpu.SemaphoreType.DMA((16,)),
        ],
        spaces="HHHH",
    )


def child_block(level, tables, child, k):
    own_ref, side_ref, own_beside_ref, side_beside_ref = tables
    c = lax.axis_index("c")
    if level == 1:
        return jnp.where(c == child, own_ref[0, k], own_beside_ref[0, k])
    if level == 2:
        sibling = jnp.where(c == 0, side_ref[0, 2 + k], side_beside_ref[0, 2 + k])
        return jnp.where(lax.axis_index("y0") == child, own_ref[0, 2 + k], sibling)
    sibling = jnp.where(c == 0, side_beside_ref[0, 6 + k], side_ref[0, 6 + k])
    return jnp.where(lax.axis_index("y1") == child, own_ref[0, 6 + k], sibling)


def both_factors(level, factors, beside):
    at = slice(level * PIVOTS, (level + 1) * PIVOTS)
    return [jnp.concatenate([factors[i : i + 1, at], beside[i : i + 1, at]], 1) for i in range(2)]


def forward(level, received, sides, tables, weights, updates, factors, partner_factors):
    width = 1 << level
    span = 4 * PIVOTS * width
    chunks = span // 512
    update_len = 2 * PIVOTS * width if level < 3 else 0
    blocks = (2, 4, 8)[level - 1]
    n_sides = len(sides)
    n_updates = 1 if level < 3 else 0
    n_outs = (2, 2, 3)[level - 1]

    def body(*refs):
        refs = list(refs)

        def take(count):
            taken, refs[:] = refs[:count], refs[count:]
            return taken

        tables_refs = take(4)
        received_ref, factors_ref, beside_ref = take(3)
        updates_ref = take(n_updates)
        sides_refs = take(n_sides)
        (weights_far,) = take(1)
        outs = take(n_outs)
        semaphores, b_ref, own_ref, weights_ref = take(4)
        moves = Moves(semaphores)
        y0, y1 = lax.axis_index("y0"), lax.axis_index("y1")

        arriving, leaving = [], []

        def bring(source, block):
            for c in range(2):
                arriving.append(moves.start(source.at[pl.ds(c * HALF, HALF)], b_ref.at[:, block_at(block * 2 + c)]))

        if level == 1:
            for x in range(4):
                bring(sides_refs[0].at[x], x)
        elif level == 2:
            for flip in range(2):
                for x in range(4):
                    bring(sides_refs[flip].at[x, :, pl.ds(0, PIVOTS)], x * 2 + (y0 ^ flip))
        else:
            for high in range(2):
                for flip in range(2):
                    for x in range(4):
                        bring(sides_refs[high].at[flip, x], x * 4 + (y1 ^ high) * 2 + (y0 ^ flip))
        columns = moves.chunks(weights_far, weights_ref)
        if level < 3:
            part_ref = refs[0]
        totals = [None, None]
        for child in range(2):
            if level == 1:
                totals[child] = sum(received_ref[child * 4 + x] for x in range(4))
            elif level == 2:
                totals[child] = sum(received_ref[x * 2 + child] for x in range(4))
        finish(arriving)
        for child in range(2):
            for k in range(blocks):
                if level < 3:
                    piece = totals[child][:, k * BLOCK : (k + 1) * BLOCK]
                else:
                    piece = received_ref[(k // 2) * 4 + child * 2 + k % 2]
                where = block_at(child_block(level, tables_refs, child, k))
                b_ref[:, where] = b_ref[:, where] - piece
        solved = jnp.zeros((HALF, 2 * PIVOTS), jnp.float32)
        for k in range(chunks):
            columns[k].wait()
            at = slice(k * 512, (k + 1) * 512)
            solved += product(b_ref[:, at], weights_ref[k, 0], weights_ref[k, 1], 1)
        weighted = pivot_apply(solved, *both_factors(level, factors_ref, beside_ref))
        if level < 3:
            own_ref[...] = weighted
            leaving.append(moves.start(own_ref, outs[1]))
            for k in range(update_len // 256):
                at = slice(k * 256, (k + 1) * 256)
                part_ref[:, at] = product(solved, updates_ref[0][0, :, at], updates_ref[0][1, :, at], 0)
            for i in range(8):
                source = part_ref if level == 1 else part_ref.at[:, pl.ds(i * BLOCK, BLOCK)]
                leaving.append(moves.start(source, outs[0].at[i]))
        else:
            sent_ref, keep_ref, beyond_ref = outs
            for k in range(chunks):
                at = slice(k * 512, (k + 1) * 512)
                b_ref[:, at] = product(weighted, weights_ref[k, 0], weights_ref[k, 1], 0)
            for child in range(2):
                for k in range(8):
                    where = block_at(child_block(3, tables_refs, child, k))
                    leaving.append(
                        moves.start(b_ref.at[:, where], sent_ref.at[(k // 2) * 4 + child * 2 + k % 2])
                    )
            for out, bit in ((beyond_ref, 1 - y1), (keep_ref, y1)):
                for x in range(4):
                    for low in range(2):
                        where = block_at(x * 4 + bit * 2 + low, 256)
                        leaving.append(moves.start(b_ref.at[:, where], out.at[x, low]))
        finish(leaving)

    outs = {
        1: [(8, HALF, 512), (HALF, 256)],
        2: [(8, HALF, BLOCK), (HALF, 256)],
        3: [(16, HALF, BLOCK), (4, 2, HALF, 256), (4, 2, HALF, 256)],
    }[level]
    operands = [*map(far, tables), received, close(factors), close(partner_factors)]
    operands += [close(updates)] if level < 3 else []
    n_close = len(operands) - 4
    operands += map(far, [*sides, weights])
    specs = [SCALARS] * 4 + [WHOLE] * n_close + [FAR] * (n_sides + 1)
    scratch = [
        pltpu.SemaphoreType.DMA((80,)),
        pltpu.VMEM((HALF, span), jnp.float32),
        pltpu.VMEM((HALF, 256), jnp.float32),
        pltpu.VMEM((chunks, 2, 256, 512), jnp.bfloat16),
    ]
    if level < 3:
        scratch.append(pltpu.VMEM((HALF, update_len), jnp.float32))
    return call(body, outs, operands, specs, scratch, spaces="H" * n_outs)


def backward(level, received, weighted, tables, weights, updates, answers):
    width = 1 << level
    span = 4 * PIVOTS * width
    chunks = span // 512
    update_len = 2 * PIVOTS * width
    blocks = (2, 4)[level - 1]
    n_answers = len(answers)
    n_outs = (2, 3)[level - 1]

    def body(*refs):
        refs = list(refs)

        def take(count):
            taken, refs[:] = refs[:count], refs[count:]
            return taken

        tables_refs = take(4)
        received_ref, updates_ref = take(2)
        weighted_far, weights_far = take(2)
        answers_far = take(n_answers)
        outs = take(n_outs)
        semaphores, x_ref, weighted_ref, weights_ref, pieces_ref = take(5)
        moves = Moves(semaphores)
        arriving = moves.start(weighted_far, weighted_ref)
        columns = moves.chunks(weights_far, weights_ref)
        leaving = []
        if level == 2:
            own_ref, other_ref, sums_ref = refs
            both = [moves.start(answers_far[0], own_ref), moves.start(answers_far[1], other_ref)]
        if level == 1:
            total = sum(received_ref[i] for i in range(8))
        arriving.wait()
        target = weighted_ref[...]
        for k in range(update_len // 256):
            at = slice(k * 256, (k + 1) * 256)
            if level == 1:
                chosen = total[:, at]
            else:
                chosen = jnp.concatenate([received_ref[2 * k], received_ref[2 * k + 1]], 1)
            target -= product(chosen, updates_ref[0, :, at], updates_ref[1, :, at], 1)
        for k in range(chunks):
            columns[k].wait()
            at = slice(k * 512, (k + 1) * 512)
            x_ref[:, at] = product(target, weights_ref[k, 0], weights_ref[k, 1], 0)
        for child in range(2):
            for k in range(blocks):
                where = block_at(child_block(level, tables_refs, child, k))
                at = slice(k * BLOCK, (k + 1) * BLOCK)
                pieces_ref[child, :, at] = x_ref[:, where]
            for x in range(4):
                leaving.append(moves.start(pieces_ref.at[child], outs[0].at[x * 2 + child]))
        if level == 1:
            for x in range(4):
                leaving.append(moves.start(x_ref.at[:, pl.ds(x * 256, 256)], outs[1].at[x]))
        else:
            y0 = lax.axis_index("y0")
            keep_out, beyond_out = outs[1:]
            for out, bit in ((beyond_out, 1 - y0), (keep_out, y0)):
                for x in range(4):
                    where = block_at(x * 2 + bit, 256)
                    leaving.append(moves.start(x_ref.at[:, where], out.at[0, x]))
            finish(both)
            for i, (out, bit) in enumerate(((beyond_out, 1 - y0), (keep_out, y0))):
                for x in range(4):
                    sums_ref[i, x] = own_ref[x, bit] + other_ref[x, bit]
                leaving.append(moves.start(sums_ref.at[i], out.at[1]))
        finish(leaving)

    outs = [(8, HALF, blocks * BLOCK)]
    outs += [(4, HALF, 256)] if level == 1 else [(2, 4, HALF, 256), (2, 4, HALF, 256)]
    operands = [*map(far, tables), received, close(updates), *map(far, [weighted, weights, *answers])]
    specs = [SCALARS] * 4 + [WHOLE] * 2 + [FAR] * (len(operands) - 6)
    scratch = [
        pltpu.SemaphoreType.DMA((64,)),
        pltpu.VMEM((HALF, span), jnp.float32),
        pltpu.VMEM((HALF, 256), jnp.float32),
        pltpu.VMEM((chunks, 2, 256, 512), jnp.bfloat16),
        pltpu.VMEM((2, HALF, blocks * BLOCK), jnp.float32),
    ]
    if level == 2:
        scratch += [pltpu.VMEM((4, 2, HALF, 256), jnp.float32)] * 2 + [pltpu.VMEM((2, 4, HALF, 256), jnp.float32)]
    return call(body, outs, operands, specs, scratch, spaces="H" * n_outs)


def level_zero_backward(received, weighted, weights, updates, own, other):
    def body(received_ref, weighted_ref, own_ref, other_ref, weights_ref, updates_ref, sent_ref):
        core = lax.axis_index("c")
        for half, source in ((core, own_ref), (1 - core, other_ref)):
            place = pl.ds(pl.multiple_of(half * HALF, 8), HALF)
            for x in range(4):
                sent_ref[x, place, PIVOTS:] = source[x]
        chosen = jnp.concatenate([sum(received_ref[x * 2 + c] for x in range(4)) for c in range(2)], 0)
        target = weighted_ref[...] - product(chosen, updates_ref[0], updates_ref[1], 1)
        part = product(target, weights_ref[0], weights_ref[1], 0)
        for q in range(4):
            sent_ref[q, :, :PIVOTS] = part[:, q * PIVOTS : (q + 1) * PIVOTS]

    return call(
        body,
        [(4, SIDES, 512)],
        [received, far(weighted), far(own), other, close(weights), close(updates)],
        [WHOLE] * 6,
        spaces="v",
    )[0]


def summed(received):
    def body(received_ref, out_ref):
        out_ref[...] = (received_ref[0] + received_ref[1]) + (received_ref[2] + received_ref[3])

    return call(body, [(SIDES, 512)], [received], [WHOLE])[0]


def summed_copies(received, count):
    total = jnp.sum(received, 0)
    return jnp.broadcast_to(total[None], (count, *total.shape))


def sibling_tables(targets):
    pairs = []
    for y1 in range(2):
        for y0 in range(2):
            here = y1 * 4 + y0 * 2
            pairs.append((here, y1 * 4 + (1 - y0) * 2))
            pairs.append((here + 1, (1 - y1) * 4 + y0 * 2 + 1))
    side = lax.ppermute(targets, ("y1", "y0", "c"), pairs)
    return [targets, side, with_partner(targets), with_partner(side)]


def per_device(right_side, factor_inverse, update_panel, update_targets, pivot_pairs, pivot_diagonal, pivot_coupling):
    sides = right_side[0, 0]
    inverse = factor_inverse[0, 0]
    update = update_panel[0, 0]
    plane = ("x", "y1", "y0")
    pair = ("x", "y0")

    packed = jnp.broadcast_to(sides[None], (4, *sides.shape))
    first = exchange(packed, ("x",))
    factors = pivot_factors(pivot_pairs[0], pivot_diagonal[0], pivot_coupling[0])
    partner_factors = with_partner(factors)
    inverse_after, update_after, _ = lax.optimization_barrier((inverse, update, packed))
    partner_inverse = with_partner(inverse_after)
    partner_update = with_partner(update_after)
    (weights0,) = prepared([inverse], [(0, 512, None)], packed)
    (updates0,) = prepared([update], [(0, 256, None)], packed)
    first, partner_factors, *tables = lax.optimization_barrier(
        (first, partner_factors, *sibling_tables(update_targets))
    )

    sent, weighted0, keep, give = level_zero_forward(first, weights0, updates0, factors)
    received = exchange(sent, ("c", "x"))
    give = with_partner(give)
    sides1, near = gathered_sides(keep, give)
    beyond = across(near, "y0")
    (weights1,) = prepared([inverse, partner_inverse], [(512, 1024, 512)], sent)
    (updates1,) = prepared([update, partner_update], [(256, 512, None)], sent)
    sent, weighted1 = forward(1, received, [sides1], tables, weights1, updates1, factors, partner_factors)
    sent, beyond = lax.optimization_barrier((sent, beyond))
    weights2, weights3 = prepared([inverse, partner_inverse], [(1536, 2048, 512), (3584, 4096, 512)], sent)
    (updates2,) = prepared([update, partner_update], [(768, 1024, None)], sent)
    received = exchange(sent, pair)
    near3, _ = lax.optimization_barrier((jnp.stack([near[:, :, PIVOTS:], beyond[:, :, PIVOTS:]]), sent))
    beyond3 = across(near3, "y1")
    sent, weighted2 = forward(2, received, [near, beyond], tables, weights2, updates2, factors, partner_factors)
    received = exchange(summed_copies(exchange(sent, pair), 16), plane)
    sent, kept3, other3 = forward(3, received, [near3, beyond3], tables, weights3, None, factors, partner_factors)
    other3 = across(other3, "y1")
    received = exchange(summed_copies(exchange(sent, plane), 8), pair)
    sent, kept, other = backward(2, received, weighted2, tables, weights2, updates2, [kept3, other3])
    other = across(other, "y0")
    received = exchange(sent, pair)
    sent, nearest = backward(1, received, weighted1, tables, weights1, updates1, [])
    received = exchange(sent, ("x", "c"))
    keep, give = upper_answers(nearest, kept, other)
    sent = level_zero_backward(received, weighted0, weights0, updates0, keep, with_partner(give))
    return summed(exchange(sent, ("x",)))[None, None]


def solution(mesh):
    grid = np.array(mesh.devices).reshape(4, 2, 2, 2, 4)
    fine = Mesh(grid, AXES)
    leaf = ("z", "y1", "y0", "c")
    in_specs = (
        P(leaf, "x", None, None),
        P(leaf, "x", None, None),
        P(leaf, "x", None, None),
        P(leaf, None),
        P(leaf, "x", None),
        P(leaf, "x", None),
        P(leaf, "x", None),
    )
    out_specs = P(leaf, "x", None, None)

    return jax.shard_map(per_device, mesh=fine, in_specs=in_specs, out_specs=out_specs, check_vma=False)
```

```python
import jax
import jax.numpy as jnp
import numpy as np
from jax import lax
from jax.experimental import pallas as pl
from jax.experimental.pallas import tpu as pltpu
from jax.sharding import Mesh, PartitionSpec as P


BLOCK = 128
PIVOTS = 128
SIDES = 96
HALF = SIDES // 2
AXES = ("z", "y1", "y0", "c", "x")

exact_mode = lax.Precision.HIGHEST


def parts(value):
    high = value.astype(jnp.bfloat16)
    return high, (value - high.astype(jnp.float32)).astype(jnp.bfloat16)


def product(left, high, low, side):
    left_high, left_low = parts(left)
    dims = (((1,), (side,)), ((), ()))

    def dot(a, b):
        return lax.dot_general(a, b, dims, preferred_element_type=jnp.float32)

    both = dot(jnp.concatenate([left_high, left_low], 0), high)
    rows = left.shape[0]
    return both[:rows] + (dot(left_high, low) + both[rows:])


def dot_full(left, right):
    return lax.dot_general(
        left, right, (((1,), (0,)), ((), ())), precision=exact_mode, preferred_element_type=jnp.float32
    )


def exchange(value, axes):
    return lax.all_to_all(value, axes, 0, 0, tiled=True)


def with_partner(value):
    return lax.ppermute(value, "c", [(0, 1), (1, 0)])


def across(value, axis):
    return lax.ppermute(value, axis, [(0, 1), (1, 0)])


def block_at(index, size=BLOCK):
    return pl.ds(pl.multiple_of(index * size, size), size)


WHOLE = pl.BlockSpec(memory_space=pltpu.VMEM)
SCALARS = pl.BlockSpec(memory_space=pltpu.SMEM)
FAR = pl.BlockSpec(memory_space=pltpu.HBM)


def far(value):
    return pltpu.with_memory_space_constraint(value, pltpu.HBM)


def close(value):
    return pltpu.with_memory_space_constraint(value, pltpu.VMEM)


def call(body, out_shapes, operands, specs, scratch=(), limit=20, spaces=None):
    return pl.pallas_call(
        body,
        in_specs=specs,
        out_specs=[FAR if k == "H" else WHOLE for k in spaces or "-" * len(out_shapes)],
        out_shape=[
            {"H": pltpu.HBM, "h": pltpu.HBM, "v": pltpu.VMEM, "-": jax.ShapeDtypeStruct}[k](s, jnp.float32)
            for s, k in zip(out_shapes, spaces or "-" * len(out_shapes))
        ],
        scratch_shapes=list(scratch),
        compiler_params=pltpu.CompilerParams(vmem_limit_bytes=limit * 1024 * 1024),
    )(*operands)


def prepared(pair, spans, after):
    def body(*refs):
        sources = refs[: len(pair)]
        outs = refs[len(pair) + 1 :][: len(spans)]
        buffers = refs[len(pair) + 1 + len(spans) : -1]
        semaphores = refs[-1]
        moves = []
        for i, (start, width, _) in enumerate(spans):
            for side, source in enumerate(sources):
                move = pltpu.make_async_copy(
                    source.at[:, pl.ds(start, width)],
                    buffers[i].at[pl.ds(side * PIVOTS, PIVOTS), :],
                    semaphores.at[i, side],
                )
                move.start()
                moves.append((i, side, move))
        for i, side, move in moves:
            move.wait()
            rows = slice(side * PIVOTS, (side + 1) * PIVOTS)
            _, width, step = spans[i]
            for k, at in enumerate(range(0, width, step or width)):
                high, low = parts(buffers[i][rows, at : at + (step or width)])
                place = outs[i].at[k] if step else outs[i]
                place[0, rows] = high
                place[1, rows] = low

    count = len(pair) * PIVOTS
    shapes = [
        pltpu.HBM((width // step, 2, count, step), jnp.bfloat16) if step else pltpu.VMEM((2, count, width), jnp.bfloat16)
        for _, width, step in spans
    ]
    return pl.pallas_call(
        body,
        in_specs=[FAR] * (len(pair) + 1),
        out_specs=[WHOLE] * len(spans),
        out_shape=shapes,
        scratch_shapes=[pltpu.VMEM((count, width), jnp.float32) for _, width, _ in spans]
        + [pltpu.SemaphoreType.DMA((len(spans), len(pair)))],
        compiler_params=pltpu.CompilerParams(vmem_limit_bytes=28 * 1024 * 1024),
    )(*map(far, pair), far(after))


def pivot_apply(solved, own, swapped):
    lane = lax.broadcasted_iota(jnp.int32, solved.shape, 1)
    width = solved.shape[1]
    beside = jnp.where(lane % 2 == 0, pltpu.roll(solved, width - 1, 1), pltpu.roll(solved, 1, 1))
    return own * solved + swapped * beside


def pivot_factors(kinds, diagonal, coupling):
    def body(kinds_ref, diagonal_ref, coupling_ref, out_ref):
        width = diagonal_ref.shape[1]
        row = lax.broadcasted_iota(jnp.int32, (width // 2, width), 0)
        col = lax.broadcasted_iota(jnp.int32, (width // 2, width), 1)
        widen = (col // 2 == row).astype(jnp.float32)
        pair = jnp.concatenate(
            [kinds_ref[...].astype(jnp.float32), coupling_ref[...], jnp.zeros((6, width // 2), jnp.float32)], 0
        )
        wide = dot_full(pair, widen)
        is_pair = wide[0:1] > 0.5
        couple = wide[1:2]
        own = jnp.broadcast_to(diagonal_ref[...], (8, width))
        lane = lax.broadcasted_iota(jnp.int32, (8, width), 1)
        other = jnp.where(lane % 2 == 0, pltpu.roll(own, width - 1, 1), pltpu.roll(own, 1, 1))[0:1]
        own = own[0:1]
        determinant = own * other - couple * couple
        out_ref[0:1, :] = jnp.where(is_pair, other / determinant, 1.0 / own)
        out_ref[1:2, :] = jnp.where(is_pair, -couple / determinant, 0.0)

    operands = [far(kinds), far(diagonal), far(coupling)]
    return call(body, [(2, diagonal.shape[1])], operands, [WHOLE] * 3, spaces="v")[0]


def gathered_sides(own, other):
    def body(own_ref, other_ref, one_ref, near_ref):
        c = lax.axis_index("c")
        for rows, source in ((c, own_ref), (1 - c, other_ref)):
            place = pl.ds(pl.multiple_of(rows * HALF, 8), HALF)
            for x in range(4):
                one_ref[x, place] = source[x, :, :PIVOTS]
                near_ref[x, place] = source[x, :, PIVOTS:]

    return call(body, [(4, SIDES, PIVOTS), (4, SIDES, 256)], [far(own), other], [WHOLE] * 2, spaces="hh")


def upper_answers(nearest, kept, other):
    def body(nearest_ref, kept_ref, other_ref, own_ref, give_ref):
        c = lax.axis_index("c")
        for core, out in ((c, own_ref), (1 - c, give_ref)):
            at = block_at(core)
            for x in range(4):
                out[x, :, :PIVOTS] = nearest_ref[x, :, at]
                for i in range(2):
                    piece = kept_ref[i, x, :, at] + other_ref[i, x, :, at]
                    out[x, :, (1 + i) * PIVOTS : (2 + i) * PIVOTS] = piece

    return call(body, [(4, HALF, 384)] * 2, [far(nearest), far(kept), other], [WHOLE] * 3, spaces="hh")


class Moves:
    def __init__(self, semaphores):
        self.semaphores, self.started = semaphores, []

    def start(self, source, target):
        move = pltpu.make_async_copy(source, target, self.semaphores.at[len(self.started)])
        move.start()
        self.started.append(move)
        return move

    def chunks(self, source, target, which):
        return [self.start(source.at[k], target.at[k]) for k in which]


def finish(moves):
    for move in moves:
        move.wait()


def level_zero_forward(first, weights, updates, factors):
    def body(first_ref, weights_ref, updates_ref, factors_ref, *refs):
        sent_ref, weighted_ref, keep_ref, give_ref, part_ref, own_ref, semaphores = refs
        moves = Moves(semaphores)
        core = lax.axis_index("c")
        leaving = []
        for half, out in ((core, keep_ref), (1 - core, give_ref)):
            rows = pl.ds(pl.multiple_of(half * HALF, 8), HALF)
            leaving.append(moves.start(first_ref.at[:, rows, pl.ds(PIVOTS, 3 * PIVOTS)], out))
        gathered = jnp.concatenate([first_ref[q, :, :PIVOTS] for q in range(4)], 1)
        solved = product(gathered, weights_ref[0], weights_ref[1], 1)
        part_ref[...] = product(solved, updates_ref[0], updates_ref[1], 0)
        for c in range(2):
            for x in range(4):
                leaving.append(moves.start(part_ref.at[pl.ds(c * HALF, HALF)], sent_ref.at[c * 4 + x]))
        own_ref[...] = pivot_apply(solved, factors_ref[0:1, :PIVOTS], factors_ref[1:2, :PIVOTS])
        leaving.append(moves.start(own_ref, weighted_ref))
        finish(leaving)

    return call(
        body,
        [(8, HALF, 256), (SIDES, PIVOTS), (4, HALF, 384), (4, HALF, 384)],
        [close(first), close(weights), close(updates), close(factors)],
        [WHOLE] * 4,
        [
            pltpu.VMEM((SIDES, 256), jnp.float32),
            pltpu.VMEM((SIDES, PIVOTS), jnp.float32),
            pltpu.SemaphoreType.DMA((16,)),
        ],
        spaces="HHHH",
    )


def child_block(level, tables, child, k):
    own_ref, side_ref, own_beside_ref, side_beside_ref = tables
    c = lax.axis_index("c")
    if level == 1:
        return jnp.where(c == child, own_ref[0, k], own_beside_ref[0, k])
    if level == 2:
        sibling = jnp.where(c == 0, side_ref[0, 2 + k], side_beside_ref[0, 2 + k])
        return jnp.where(lax.axis_index("y0") == child, own_ref[0, 2 + k], sibling)
    sibling = jnp.where(c == 0, side_beside_ref[0, 6 + k], side_ref[0, 6 + k])
    return jnp.where(lax.axis_index("y1") == child, own_ref[0, 6 + k], sibling)


def both_factors(level, factors, beside):
    at = slice(level * PIVOTS, (level + 1) * PIVOTS)
    return [jnp.concatenate([factors[i : i + 1, at], beside[i : i + 1, at]], 1) for i in range(2)]


def forward(level, received, sides, tables, weights, updates, factors, partner_factors):
    width = 1 << level
    span = 4 * PIVOTS * width
    chunks = span // 512
    update_len = 2 * PIVOTS * width if level < 3 else 0
    blocks = (2, 4, 8)[level - 1]
    n_sides = len(sides)
    n_updates = 1 if level < 3 else 0
    n_outs = (2, 2, 3)[level - 1]

    def body(*refs):
        refs = list(refs)

        def take(count):
            taken, refs[:] = refs[:count], refs[count:]
            return taken

        tables_refs = take(4)
        received_ref, factors_ref, beside_ref = take(3)
        updates_ref = take(n_updates)
        sides_refs = take(n_sides)
        (weights_far,) = take(1)
        outs = take(n_outs)
        semaphores, b_ref, own_ref, weights_ref = take(4)
        moves = Moves(semaphores)
        y0, y1 = lax.axis_index("y0"), lax.axis_index("y1")

        arriving, leaving = [], []

        def bring(source, block):
            for c in range(2):
                arriving.append(moves.start(source.at[pl.ds(c * HALF, HALF)], b_ref.at[:, block_at(block * 2 + c)]))

        if level == 1:
            for x in range(4):
                bring(sides_refs[0].at[x], x)
        elif level == 2:
            for flip in range(2):
                for x in range(4):
                    bring(sides_refs[flip].at[x, :, pl.ds(0, PIVOTS)], x * 2 + (y0 ^ flip))
        else:
            for high in range(2):
                for flip in range(2):
                    for x in range(4):
                        bring(sides_refs[high].at[flip, x], x * 4 + (y1 ^ high) * 2 + (y0 ^ flip))
        columns = moves.chunks(weights_far, weights_ref, range(min(2, chunks)))
        if level < 3:
            part_ref = refs[0]
        totals = [None, None]
        for child in range(2):
            if level == 1:
                totals[child] = sum(received_ref[child * 4 + x] for x in range(4))
            elif level == 2:
                totals[child] = sum(received_ref[x * 2 + child] for x in range(4))
        finish(arriving)
        columns += moves.chunks(weights_far, weights_ref, range(2, chunks))
        for child in range(2):
            for k in range(blocks):
                if level < 3:
                    piece = totals[child][:, k * BLOCK : (k + 1) * BLOCK]
                else:
                    piece = received_ref[(k // 2) * 4 + child * 2 + k % 2]
                where = block_at(child_block(level, tables_refs, child, k))
                b_ref[:, where] = b_ref[:, where] - piece
        solved = jnp.zeros((HALF, 2 * PIVOTS), jnp.float32)
        for k in range(chunks):
            columns[k].wait()
            at = slice(k * 512, (k + 1) * 512)
            solved += product(b_ref[:, at], weights_ref[k, 0], weights_ref[k, 1], 1)
        weighted = pivot_apply(solved, *both_factors(level, factors_ref, beside_ref))
        if level < 3:
            own_ref[...] = weighted
            leaving.append(moves.start(own_ref, outs[1]))
            for k in range(update_len // 256):
                at = slice(k * 256, (k + 1) * 256)
                part_ref[:, at] = product(solved, updates_ref[0][0, :, at], updates_ref[0][1, :, at], 0)
            for i in range(8):
                source = part_ref if level == 1 else part_ref.at[:, pl.ds(i * BLOCK, BLOCK)]
                leaving.append(moves.start(source, outs[0].at[i]))
        else:
            sent_ref, keep_ref, beyond_ref = outs
            for k in range(chunks):
                at = slice(k * 512, (k + 1) * 512)
                b_ref[:, at] = product(weighted, weights_ref[k, 0], weights_ref[k, 1], 0)
            for child in range(2):
                for k in range(8):
                    where = block_at(child_block(3, tables_refs, child, k))
                    leaving.append(
                        moves.start(b_ref.at[:, where], sent_ref.at[(k // 2) * 4 + child * 2 + k % 2])
                    )
            for out, bit in ((beyond_ref, 1 - y1), (keep_ref, y1)):
                for x in range(4):
                    for low in range(2):
                        where = block_at(x * 4 + bit * 2 + low, 256)
                        leaving.append(moves.start(b_ref.at[:, where], out.at[x, low]))
        finish(leaving)

    outs = {
        1: [(8, HALF, 512), (HALF, 256)],
        2: [(8, HALF, BLOCK), (HALF, 256)],
        3: [(16, HALF, BLOCK), (4, 2, HALF, 256), (4, 2, HALF, 256)],
    }[level]
    operands = [*map(far, tables), received, close(factors), close(partner_factors)]
    operands += [close(updates)] if level < 3 else []
    n_close = len(operands) - 4
    operands += map(far, [*sides, weights])
    specs = [SCALARS] * 4 + [WHOLE] * n_close + [FAR] * (n_sides + 1)
    scratch = [
        pltpu.SemaphoreType.DMA((80,)),
        pltpu.VMEM((HALF, span), jnp.float32),
        pltpu.VMEM((HALF, 256), jnp.float32),
        pltpu.VMEM((chunks, 2, 256, 512), jnp.bfloat16),
    ]
    if level < 3:
        scratch.append(pltpu.VMEM((HALF, update_len), jnp.float32))
    return call(body, outs, operands, specs, scratch, spaces="H" * n_outs)


def backward(level, received, weighted, tables, weights, updates, answers):
    width = 1 << level
    span = 4 * PIVOTS * width
    chunks = span // 512
    update_len = 2 * PIVOTS * width
    blocks = (2, 4)[level - 1]
    n_answers = len(answers)
    n_outs = (2, 3)[level - 1]

    def body(*refs):
        refs = list(refs)

        def take(count):
            taken, refs[:] = refs[:count], refs[count:]
            return taken

        tables_refs = take(4)
        received_ref, updates_ref = take(2)
        weighted_far, weights_far = take(2)
        answers_far = take(n_answers)
        outs = take(n_outs)
        semaphores, x_ref, weighted_ref, weights_ref, pieces_ref = take(5)
        moves = Moves(semaphores)
        arriving = moves.start(weighted_far, weighted_ref)
        columns = moves.chunks(weights_far, weights_ref, range(min(2, chunks)))
        leaving = []
        if level == 1:
            total = sum(received_ref[i] for i in range(8))
        arriving.wait()
        columns += moves.chunks(weights_far, weights_ref, range(2, chunks))
        if level == 2:
            own_ref, other_ref, sums_ref = refs
            both = [moves.start(answers_far[0], own_ref), moves.start(answers_far[1], other_ref)]
        target = weighted_ref[...]
        for k in range(update_len // 256):
            at = slice(k * 256, (k + 1) * 256)
            if level == 1:
                chosen = total[:, at]
            else:
                chosen = jnp.concatenate([received_ref[2 * k], received_ref[2 * k + 1]], 1)
            target -= product(chosen, updates_ref[0, :, at], updates_ref[1, :, at], 1)
        for k in range(chunks):
            columns[k].wait()
            at = slice(k * 512, (k + 1) * 512)
            x_ref[:, at] = product(target, weights_ref[k, 0], weights_ref[k, 1], 0)
        for child in range(2):
            for k in range(blocks):
                where = block_at(child_block(level, tables_refs, child, k))
                at = slice(k * BLOCK, (k + 1) * BLOCK)
                pieces_ref[child, :, at] = x_ref[:, where]
            for x in range(4):
                leaving.append(moves.start(pieces_ref.at[child], outs[0].at[x * 2 + child]))
        if level == 1:
            for x in range(4):
                leaving.append(moves.start(x_ref.at[:, pl.ds(x * 256, 256)], outs[1].at[x]))
        else:
            y0 = lax.axis_index("y0")
            keep_out, beyond_out = outs[1:]
            for out, bit in ((beyond_out, 1 - y0), (keep_out, y0)):
                for x in range(4):
                    where = block_at(x * 2 + bit, 256)
                    leaving.append(moves.start(x_ref.at[:, where], out.at[0, x]))
            finish(both)
            for i, (out, bit) in enumerate(((beyond_out, 1 - y0), (keep_out, y0))):
                for x in range(4):
                    sums_ref[i, x] = own_ref[x, bit] + other_ref[x, bit]
                leaving.append(moves.start(sums_ref.at[i], out.at[1]))
        finish(leaving)

    outs = [(8, HALF, blocks * BLOCK)]
    outs += [(4, HALF, 256)] if level == 1 else [(2, 4, HALF, 256), (2, 4, HALF, 256)]
    operands = [*map(far, tables), received, close(updates), *map(far, [weighted, weights, *answers])]
    specs = [SCALARS] * 4 + [WHOLE] * 2 + [FAR] * (len(operands) - 6)
    scratch = [
        pltpu.SemaphoreType.DMA((64,)),
        pltpu.VMEM((HALF, span), jnp.float32),
        pltpu.VMEM((HALF, 256), jnp.float32),
        pltpu.VMEM((chunks, 2, 256, 512), jnp.bfloat16),
        pltpu.VMEM((2, HALF, blocks * BLOCK), jnp.float32),
    ]
    if level == 2:
        scratch += [pltpu.VMEM((4, 2, HALF, 256), jnp.float32)] * 2 + [pltpu.VMEM((2, 4, HALF, 256), jnp.float32)]
    return call(body, outs, operands, specs, scratch, spaces="H" * n_outs)


def level_zero_backward(received, weighted, weights, updates, own, other):
    def body(received_ref, weighted_ref, own_ref, other_ref, weights_ref, updates_ref, sent_ref):
        core = lax.axis_index("c")
        for half, source in ((core, own_ref), (1 - core, other_ref)):
            place = pl.ds(pl.multiple_of(half * HALF, 8), HALF)
            for x in range(4):
                sent_ref[x, place, PIVOTS:] = source[x]
        chosen = jnp.concatenate([sum(received_ref[x * 2 + c] for x in range(4)) for c in range(2)], 0)
        target = weighted_ref[...] - product(chosen, updates_ref[0], updates_ref[1], 1)
        part = product(target, weights_ref[0], weights_ref[1], 0)
        for q in range(4):
            sent_ref[q, :, :PIVOTS] = part[:, q * PIVOTS : (q + 1) * PIVOTS]

    return call(
        body,
        [(4, SIDES, 512)],
        [received, far(weighted), far(own), other, close(weights), close(updates)],
        [WHOLE] * 6,
        spaces="v",
    )[0]


def summed(received):
    def body(received_ref, out_ref):
        out_ref[...] = (received_ref[0] + received_ref[1]) + (received_ref[2] + received_ref[3])

    return call(body, [(SIDES, 512)], [received], [WHOLE])[0]


def summed_copies(received, count):
    total = jnp.sum(received, 0)
    return jnp.broadcast_to(total[None], (count, *total.shape))


def sibling_tables(targets):
    pairs = []
    for y1 in range(2):
        for y0 in range(2):
            here = y1 * 4 + y0 * 2
            pairs.append((here, y1 * 4 + (1 - y0) * 2))
            pairs.append((here + 1, (1 - y1) * 4 + y0 * 2 + 1))
    side = lax.ppermute(targets, ("y1", "y0", "c"), pairs)
    return [targets, side, with_partner(targets), with_partner(side)]


def per_device(right_side, factor_inverse, update_panel, update_targets, pivot_pairs, pivot_diagonal, pivot_coupling):
    sides = right_side[0, 0]
    inverse = factor_inverse[0, 0]
    update = update_panel[0, 0]
    plane = ("x", "y1", "y0")
    pair = ("x", "y0")

    packed = jnp.broadcast_to(sides[None], (4, *sides.shape))
    first = exchange(packed, ("x",))
    factors = pivot_factors(pivot_pairs[0], pivot_diagonal[0], pivot_coupling[0])
    partner_factors = with_partner(factors)
    inverse_after, update_after, _ = lax.optimization_barrier((inverse, update, packed))
    partner_inverse = with_partner(inverse_after)
    partner_update = with_partner(update_after)
    (weights0,) = prepared([inverse], [(0, 512, None)], packed)
    (updates0,) = prepared([update], [(0, 256, None)], packed)
    first, partner_factors, *tables = lax.optimization_barrier(
        (first, partner_factors, *sibling_tables(update_targets))
    )

    sent, weighted0, keep, give = level_zero_forward(first, weights0, updates0, factors)
    received = exchange(sent, ("c", "x"))
    give = with_partner(give)
    sides1, near = gathered_sides(keep, give)
    beyond = across(near, "y0")
    (weights1,) = prepared([inverse, partner_inverse], [(512, 1024, 512)], sent)
    (updates1,) = prepared([update, partner_update], [(256, 512, None)], sent)
    sent, weighted1 = forward(1, received, [sides1], tables, weights1, updates1, factors, partner_factors)
    sent, beyond = lax.optimization_barrier((sent, beyond))
    weights2, weights3 = prepared([inverse, partner_inverse], [(1536, 2048, 512), (3584, 4096, 512)], sent)
    (updates2,) = prepared([update, partner_update], [(768, 1024, None)], sent)
    received = exchange(sent, pair)
    near3, _ = lax.optimization_barrier((jnp.stack([near[:, :, PIVOTS:], beyond[:, :, PIVOTS:]]), sent))
    beyond3 = across(near3, "y1")
    sent, weighted2 = forward(2, received, [near, beyond], tables, weights2, updates2, factors, partner_factors)
    received = exchange(summed_copies(exchange(sent, pair), 16), plane)
    sent, kept3, other3 = forward(3, received, [near3, beyond3], tables, weights3, None, factors, partner_factors)
    other3 = across(other3, "y1")
    received = exchange(summed_copies(exchange(sent, plane), 8), pair)
    sent, kept, other = backward(2, received, weighted2, tables, weights2, updates2, [kept3, other3])
    other = across(other, "y0")
    received = exchange(sent, pair)
    sent, nearest = backward(1, received, weighted1, tables, weights1, updates1, [])
    received = exchange(sent, ("x", "c"))
    keep, give = upper_answers(nearest, kept, other)
    sent = level_zero_backward(received, weighted0, weights0, updates0, keep, with_partner(give))
    return summed(exchange(sent, ("x",)))[None, None]


def solution(mesh):
    grid = np.array(mesh.devices).reshape(4, 2, 2, 2, 4)
    fine = Mesh(grid, AXES)
    leaf = ("z", "y1", "y0", "c")
    in_specs = (
        P(leaf, "x", None, None),
        P(leaf, "x", None, None),
        P(leaf, "x", None, None),
        P(leaf, None),
        P(leaf, "x", None),
        P(leaf, "x", None),
        P(leaf, "x", None),
    )
    out_specs = P(leaf, "x", None, None)

    return jax.shard_map(per_device, mesh=fine, in_specs=in_specs, out_specs=out_specs, check_vma=False)
```

```python
import jax
import jax.numpy as jnp
import numpy as np
from jax import lax
from jax.experimental import pallas as pl
from jax.experimental.pallas import tpu as pltpu
from jax.sharding import Mesh, PartitionSpec as P


BLOCK = 128
PIVOTS = 128
SIDES = 96
HALF = SIDES // 2
AXES = ("z", "y1", "y0", "c", "x")

exact_mode = lax.Precision.HIGHEST


def parts(value):
    high = value.astype(jnp.bfloat16)
    return high, (value - high.astype(jnp.float32)).astype(jnp.bfloat16)


def product(left, high, low, side):
    left_high, left_low = parts(left)
    dims = (((1,), (side,)), ((), ()))

    def dot(a, b):
        return lax.dot_general(a, b, dims, preferred_element_type=jnp.float32)

    both = dot(jnp.concatenate([left_high, left_low], 0), high)
    rows = left.shape[0]
    return both[:rows] + (dot(left_high, low) + both[rows:])


def dot_full(left, right):
    return lax.dot_general(
        left, right, (((1,), (0,)), ((), ())), precision=exact_mode, preferred_element_type=jnp.float32
    )


def exchange(value, axes):
    return lax.all_to_all(value, axes, 0, 0, tiled=True)


def with_partner(value):
    return lax.ppermute(value, "c", [(0, 1), (1, 0)])


def across(value, axis):
    return lax.ppermute(value, axis, [(0, 1), (1, 0)])


def block_at(index, size=BLOCK):
    return pl.ds(pl.multiple_of(index * size, size), size)


WHOLE = pl.BlockSpec(memory_space=pltpu.VMEM)
SCALARS = pl.BlockSpec(memory_space=pltpu.SMEM)
FAR = pl.BlockSpec(memory_space=pltpu.HBM)


def far(value):
    return pltpu.with_memory_space_constraint(value, pltpu.HBM)


def close(value):
    return pltpu.with_memory_space_constraint(value, pltpu.VMEM)


def call(body, out_shapes, operands, specs, scratch=(), limit=20, spaces=None):
    return pl.pallas_call(
        body,
        in_specs=specs,
        out_specs=[FAR if k == "H" else WHOLE for k in spaces or "-" * len(out_shapes)],
        out_shape=[
            {"H": pltpu.HBM, "h": pltpu.HBM, "v": pltpu.VMEM, "-": jax.ShapeDtypeStruct}[k](s, jnp.float32)
            for s, k in zip(out_shapes, spaces or "-" * len(out_shapes))
        ],
        scratch_shapes=list(scratch),
        compiler_params=pltpu.CompilerParams(vmem_limit_bytes=limit * 1024 * 1024),
    )(*operands)


def prepared(pair, spans, after, space=pltpu.HBM):
    def body(*refs):
        sources = refs[: len(pair)]
        outs = refs[len(pair) + 1 :][: len(spans)]
        buffers = refs[len(pair) + 1 + len(spans) : -1]
        semaphores = refs[-1]
        moves = []
        for i, (start, width, _) in enumerate(spans):
            for side, source in enumerate(sources):
                move = pltpu.make_async_copy(
                    source.at[:, pl.ds(start, width)],
                    buffers[i].at[pl.ds(side * PIVOTS, PIVOTS), :],
                    semaphores.at[i, side],
                )
                move.start()
                moves.append((i, side, move))
        for i, side, move in moves:
            move.wait()
            rows = slice(side * PIVOTS, (side + 1) * PIVOTS)
            _, width, step = spans[i]
            for k, at in enumerate(range(0, width, step or width)):
                high, low = parts(buffers[i][rows, at : at + (step or width)])
                place = outs[i].at[k] if step else outs[i]
                place[0, rows] = high
                place[1, rows] = low

    count = len(pair) * PIVOTS
    shapes = [
        space((width // step, 2, count, step), jnp.bfloat16) if step else pltpu.VMEM((2, count, width), jnp.bfloat16)
        for _, width, step in spans
    ]
    return pl.pallas_call(
        body,
        in_specs=[FAR] * (len(pair) + 1),
        out_specs=[WHOLE] * len(spans),
        out_shape=shapes,
        scratch_shapes=[pltpu.VMEM((count, width), jnp.float32) for _, width, _ in spans]
        + [pltpu.SemaphoreType.DMA((len(spans), len(pair)))],
        compiler_params=pltpu.CompilerParams(vmem_limit_bytes=28 * 1024 * 1024),
    )(*map(far, pair), far(after))


def pivot_apply(solved, own, swapped):
    lane = lax.broadcasted_iota(jnp.int32, solved.shape, 1)
    width = solved.shape[1]
    beside = jnp.where(lane % 2 == 0, pltpu.roll(solved, width - 1, 1), pltpu.roll(solved, 1, 1))
    return own * solved + swapped * beside


def pivot_factors(kinds, diagonal, coupling):
    def body(kinds_ref, diagonal_ref, coupling_ref, out_ref):
        width = diagonal_ref.shape[1]
        row = lax.broadcasted_iota(jnp.int32, (width // 2, width), 0)
        col = lax.broadcasted_iota(jnp.int32, (width // 2, width), 1)
        widen = (col // 2 == row).astype(jnp.float32)
        pair = jnp.concatenate(
            [kinds_ref[...].astype(jnp.float32), coupling_ref[...], jnp.zeros((6, width // 2), jnp.float32)], 0
        )
        wide = dot_full(pair, widen)
        is_pair = wide[0:1] > 0.5
        couple = wide[1:2]
        own = jnp.broadcast_to(diagonal_ref[...], (8, width))
        lane = lax.broadcasted_iota(jnp.int32, (8, width), 1)
        other = jnp.where(lane % 2 == 0, pltpu.roll(own, width - 1, 1), pltpu.roll(own, 1, 1))[0:1]
        own = own[0:1]
        determinant = own * other - couple * couple
        out_ref[0:1, :] = jnp.where(is_pair, other / determinant, 1.0 / own)
        out_ref[1:2, :] = jnp.where(is_pair, -couple / determinant, 0.0)

    operands = [far(kinds), far(diagonal), far(coupling)]
    return call(body, [(2, diagonal.shape[1])], operands, [WHOLE] * 3, spaces="v")[0]


def gathered_sides(own, other):
    def body(own_ref, other_ref, one_ref, near_ref):
        c = lax.axis_index("c")
        for rows, source in ((c, own_ref), (1 - c, other_ref)):
            place = pl.ds(pl.multiple_of(rows * HALF, 8), HALF)
            for x in range(4):
                one_ref[x, place] = source[x, :, :PIVOTS]
                near_ref[x, place] = source[x, :, PIVOTS:]

    return call(body, [(4, SIDES, PIVOTS), (4, SIDES, 256)], [far(own), other], [WHOLE] * 2, spaces="hh")


def upper_answers(nearest, kept, other):
    def body(nearest_ref, kept_ref, other_ref, own_ref, give_ref):
        c = lax.axis_index("c")
        for core, out in ((c, own_ref), (1 - c, give_ref)):
            at = block_at(core)
            for x in range(4):
                out[x, :, :PIVOTS] = nearest_ref[x, :, at]
                for i in range(2):
                    piece = kept_ref[i, x, :, at] + other_ref[i, x, :, at]
                    out[x, :, (1 + i) * PIVOTS : (2 + i) * PIVOTS] = piece

    return call(body, [(4, HALF, 384)] * 2, [far(nearest), far(kept), other], [WHOLE] * 3, spaces="hh")


class Moves:
    def __init__(self, semaphores):
        self.semaphores, self.started = semaphores, []

    def start(self, source, target):
        move = pltpu.make_async_copy(source, target, self.semaphores.at[len(self.started)])
        move.start()
        self.started.append(move)
        return move

    def chunks(self, source, target):
        return [self.start(source.at[k], target.at[k]) for k in range(source.shape[0])]


def finish(moves):
    for move in moves:
        move.wait()


def level_zero_forward(first, weights, updates, factors):
    def body(first_ref, weights_ref, updates_ref, factors_ref, *refs):
        sent_ref, weighted_ref, keep_ref, give_ref, part_ref, own_ref, semaphores = refs
        moves = Moves(semaphores)
        core = lax.axis_index("c")
        leaving = []
        for half, out in ((core, keep_ref), (1 - core, give_ref)):
            rows = pl.ds(pl.multiple_of(half * HALF, 8), HALF)
            leaving.append(moves.start(first_ref.at[:, rows, pl.ds(PIVOTS, 3 * PIVOTS)], out))
        gathered = jnp.concatenate([first_ref[q, :, :PIVOTS] for q in range(4)], 1)
        solved = product(gathered, weights_ref[0], weights_ref[1], 1)
        part_ref[...] = product(solved, updates_ref[0], updates_ref[1], 0)
        for c in range(2):
            for x in range(4):
                leaving.append(moves.start(part_ref.at[pl.ds(c * HALF, HALF)], sent_ref.at[c * 4 + x]))
        own_ref[...] = pivot_apply(solved, factors_ref[0:1, :PIVOTS], factors_ref[1:2, :PIVOTS])
        leaving.append(moves.start(own_ref, weighted_ref))
        finish(leaving)

    return call(
        body,
        [(8, HALF, 256), (SIDES, PIVOTS), (4, HALF, 384), (4, HALF, 384)],
        [close(first), close(weights), close(updates), close(factors)],
        [WHOLE] * 4,
        [
            pltpu.VMEM((SIDES, 256), jnp.float32),
            pltpu.VMEM((SIDES, PIVOTS), jnp.float32),
            pltpu.SemaphoreType.DMA((16,)),
        ],
        spaces="HHHH",
    )


def child_block(level, tables, child, k):
    def entry(table, at):
        return tables[0, table * 14 + at]

    c = lax.axis_index("c")
    if level == 1:
        return jnp.where(c == child, entry(0, k), entry(2, k))
    if level == 2:
        sibling = jnp.where(c == 0, entry(1, 2 + k), entry(3, 2 + k))
        return jnp.where(lax.axis_index("y0") == child, entry(0, 2 + k), sibling)
    sibling = jnp.where(c == 0, entry(3, 6 + k), entry(1, 6 + k))
    return jnp.where(lax.axis_index("y1") == child, entry(0, 6 + k), sibling)


def both_factors(level, factors, beside):
    at = slice(level * PIVOTS, (level + 1) * PIVOTS)
    return [jnp.concatenate([factors[i : i + 1, at], beside[i : i + 1, at]], 1) for i in range(2)]


def forward(level, received, sides, tables, weights, updates, factors, partner_factors):
    width = 1 << level
    span = 4 * PIVOTS * width
    chunks = span // 512
    update_len = 2 * PIVOTS * width if level < 3 else 0
    blocks = (2, 4, 8)[level - 1]
    n_sides = len(sides)
    n_updates = 1 if level < 3 else 0
    n_outs = (2, 2, 3)[level - 1]

    def body(*refs):
        refs = list(refs)

        def take(count):
            taken, refs[:] = refs[:count], refs[count:]
            return taken

        (tables_refs,) = take(1)
        received_ref, factors_ref, beside_ref = take(3)
        updates_ref = take(n_updates)
        sides_refs = take(n_sides)
        (weights_far,) = take(1)
        outs = take(n_outs)
        semaphores, b_ref, own_ref, weights_ref = take(4)
        moves = Moves(semaphores)
        y0, y1 = lax.axis_index("y0"), lax.axis_index("y1")

        arriving, leaving = [], []

        def bring(source, block):
            for c in range(2):
                arriving.append(moves.start(source.at[pl.ds(c * HALF, HALF)], b_ref.at[:, block_at(block * 2 + c)]))

        if level == 1:
            for x in range(4):
                bring(sides_refs[0].at[x], x)
        elif level == 2:
            for flip in range(2):
                for x in range(4):
                    bring(sides_refs[flip].at[x, :, pl.ds(0, PIVOTS)], x * 2 + (y0 ^ flip))
        else:
            for high in range(2):
                for flip in range(2):
                    for x in range(4):
                        bring(sides_refs[high].at[flip, x], x * 4 + (y1 ^ high) * 2 + (y0 ^ flip))
        if level == 1:
            weights_ref, columns = weights_far, []
        else:
            columns = moves.chunks(weights_far, weights_ref)
        if level < 3:
            part_ref = refs[0]
        totals = [None, None]
        for child in range(2):
            if level == 1:
                totals[child] = sum(received_ref[child * 4 + x] for x in range(4))
            elif level == 2:
                totals[child] = sum(received_ref[x * 2 + child] for x in range(4))
        finish(arriving)
        for child in range(2):
            for k in range(blocks):
                if level < 3:
                    piece = totals[child][:, k * BLOCK : (k + 1) * BLOCK]
                else:
                    piece = received_ref[(k // 2) * 4 + child * 2 + k % 2]
                where = block_at(child_block(level, tables_refs, child, k))
                b_ref[:, where] = b_ref[:, where] - piece
        solved = jnp.zeros((HALF, 2 * PIVOTS), jnp.float32)
        for k in range(chunks):
            finish(columns[k : k + 1])
            at = slice(k * 512, (k + 1) * 512)
            solved += product(b_ref[:, at], weights_ref[k, 0], weights_ref[k, 1], 1)
        weighted = pivot_apply(solved, *both_factors(level, factors_ref, beside_ref))
        if level < 3:
            own_ref[...] = weighted
            leaving.append(moves.start(own_ref, outs[1]))
            for k in range(update_len // 256):
                at = slice(k * 256, (k + 1) * 256)
                part_ref[:, at] = product(solved, updates_ref[0][0, :, at], updates_ref[0][1, :, at], 0)
            for i in range(8):
                source = part_ref if level == 1 else part_ref.at[:, pl.ds(i * BLOCK, BLOCK)]
                leaving.append(moves.start(source, outs[0].at[i]))
        else:
            sent_ref, keep_ref, beyond_ref = outs
            for k in range(chunks):
                at = slice(k * 512, (k + 1) * 512)
                b_ref[:, at] = product(weighted, weights_ref[k, 0], weights_ref[k, 1], 0)
            for child in range(2):
                for k in range(8):
                    where = block_at(child_block(3, tables_refs, child, k))
                    leaving.append(
                        moves.start(b_ref.at[:, where], sent_ref.at[(k // 2) * 4 + child * 2 + k % 2])
                    )
            for out, bit in ((beyond_ref, 1 - y1), (keep_ref, y1)):
                for x in range(4):
                    for low in range(2):
                        where = block_at(x * 4 + bit * 2 + low, 256)
                        leaving.append(moves.start(b_ref.at[:, where], out.at[x, low]))
        finish(leaving)

    outs = {
        1: [(8, HALF, 512), (HALF, 256)],
        2: [(8, HALF, BLOCK), (HALF, 256)],
        3: [(16, HALF, BLOCK), (4, 2, HALF, 256), (4, 2, HALF, 256)],
    }[level]
    operands = [far(tables), received, close(factors), close(partner_factors)]
    operands += [close(updates)] if level < 3 else []
    n_close = len(operands) - 1
    operands += [*map(far, sides), close(weights) if level == 1 else far(weights)]
    specs = [SCALARS] + [WHOLE] * n_close + [FAR] * n_sides + [WHOLE if level == 1 else FAR]
    scratch = [
        pltpu.SemaphoreType.DMA((80,)),
        pltpu.VMEM((HALF, span), jnp.float32),
        pltpu.VMEM((HALF, 256), jnp.float32),
        pltpu.VMEM((chunks, 2, 256, 512), jnp.bfloat16),
    ]
    if level < 3:
        scratch.append(pltpu.VMEM((HALF, update_len), jnp.float32))
    return call(body, outs, operands, specs, scratch, spaces="H" * n_outs)


def backward(level, received, weighted, tables, weights, updates, answers):
    width = 1 << level
    span = 4 * PIVOTS * width
    chunks = span // 512
    update_len = 2 * PIVOTS * width
    blocks = (2, 4)[level - 1]
    n_answers = len(answers)
    n_outs = (2, 3)[level - 1]

    def body(*refs):
        refs = list(refs)

        def take(count):
            taken, refs[:] = refs[:count], refs[count:]
            return taken

        (tables_refs,) = take(1)
        received_ref, updates_ref = take(2)
        weighted_far, weights_far = take(2)
        answers_far = take(n_answers)
        outs = take(n_outs)
        semaphores, x_ref, weighted_ref, weights_ref, pieces_ref = take(5)
        moves = Moves(semaphores)
        arriving = moves.start(weighted_far, weighted_ref)
        if level == 1:
            weights_ref, columns = weights_far, []
        else:
            columns = moves.chunks(weights_far, weights_ref)
        leaving = []
        if level == 2:
            own_ref, other_ref, sums_ref = refs
            both = [moves.start(answers_far[0], own_ref), moves.start(answers_far[1], other_ref)]
        if level == 1:
            total = sum(received_ref[i] for i in range(8))
        arriving.wait()
        target = weighted_ref[...]
        for k in range(update_len // 256):
            at = slice(k * 256, (k + 1) * 256)
            if level == 1:
                chosen = total[:, at]
            else:
                chosen = jnp.concatenate([received_ref[2 * k], received_ref[2 * k + 1]], 1)
            target -= product(chosen, updates_ref[0, :, at], updates_ref[1, :, at], 1)
        for k in range(chunks):
            finish(columns[k : k + 1])
            at = slice(k * 512, (k + 1) * 512)
            x_ref[:, at] = product(target, weights_ref[k, 0], weights_ref[k, 1], 0)
        for child in range(2):
            for k in range(blocks):
                where = block_at(child_block(level, tables_refs, child, k))
                at = slice(k * BLOCK, (k + 1) * BLOCK)
                pieces_ref[child, :, at] = x_ref[:, where]
            for x in range(4):
                leaving.append(moves.start(pieces_ref.at[child], outs[0].at[x * 2 + child]))
        if level == 1:
            for x in range(4):
                leaving.append(moves.start(x_ref.at[:, pl.ds(x * 256, 256)], outs[1].at[x]))
        else:
            y0 = lax.axis_index("y0")
            keep_out, beyond_out = outs[1:]
            for out, bit in ((beyond_out, 1 - y0), (keep_out, y0)):
                for x in range(4):
                    where = block_at(x * 2 + bit, 256)
                    leaving.append(moves.start(x_ref.at[:, where], out.at[0, x]))
            finish(both)
            for i, (out, bit) in enumerate(((beyond_out, 1 - y0), (keep_out, y0))):
                for x in range(4):
                    sums_ref[i, x] = own_ref[x, bit] + other_ref[x, bit]
                leaving.append(moves.start(sums_ref.at[i], out.at[1]))
        finish(leaving)

    outs = [(8, HALF, blocks * BLOCK)]
    outs += [(4, HALF, 256)] if level == 1 else [(2, 4, HALF, 256), (2, 4, HALF, 256)]
    operands = [far(tables), received, close(updates), far(weighted)]
    operands += [close(weights) if level == 1 else far(weights), *map(far, answers)]
    specs = [SCALARS] + [WHOLE] * 2 + [FAR, WHOLE if level == 1 else FAR] + [FAR] * len(answers)
    scratch = [
        pltpu.SemaphoreType.DMA((64,)),
        pltpu.VMEM((HALF, span), jnp.float32),
        pltpu.VMEM((HALF, 256), jnp.float32),
        pltpu.VMEM((chunks, 2, 256, 512), jnp.bfloat16),
        pltpu.VMEM((2, HALF, blocks * BLOCK), jnp.float32),
    ]
    if level == 2:
        scratch += [pltpu.VMEM((4, 2, HALF, 256), jnp.float32)] * 2 + [pltpu.VMEM((2, 4, HALF, 256), jnp.float32)]
    return call(body, outs, operands, specs, scratch, spaces="H" * n_outs)


def level_zero_backward(received, weighted, weights, updates, own, other):
    def body(received_ref, weighted_ref, own_ref, other_ref, weights_ref, updates_ref, sent_ref):
        core = lax.axis_index("c")
        for half, source in ((core, own_ref), (1 - core, other_ref)):
            place = pl.ds(pl.multiple_of(half * HALF, 8), HALF)
            for x in range(4):
                sent_ref[x, place, PIVOTS:] = source[x]
        chosen = jnp.concatenate([sum(received_ref[x * 2 + c] for x in range(4)) for c in range(2)], 0)
        target = weighted_ref[...] - product(chosen, updates_ref[0], updates_ref[1], 1)
        part = product(target, weights_ref[0], weights_ref[1], 0)
        for q in range(4):
            sent_ref[q, :, :PIVOTS] = part[:, q * PIVOTS : (q + 1) * PIVOTS]

    return call(
        body,
        [(4, SIDES, 512)],
        [received, far(weighted), far(own), other, close(weights), close(updates)],
        [WHOLE] * 6,
        spaces="v",
    )[0]


def summed(received):
    def body(received_ref, out_ref):
        out_ref[...] = (received_ref[0] + received_ref[1]) + (received_ref[2] + received_ref[3])

    return call(body, [(SIDES, 512)], [received], [WHOLE])[0]


def summed_copies(received, count):
    total = jnp.sum(received, 0)
    return jnp.broadcast_to(total[None], (count, *total.shape))


def sibling_tables(targets):
    pairs = []
    for y1 in range(2):
        for y0 in range(2):
            here = y1 * 4 + y0 * 2
            pairs.append((here, y1 * 4 + (1 - y0) * 2))
            pairs.append((here + 1, (1 - y1) * 4 + y0 * 2 + 1))
    side = lax.ppermute(targets, ("y1", "y0", "c"), pairs)
    return jnp.concatenate([targets, side, with_partner(targets), with_partner(side)], 1)


def per_device(right_side, factor_inverse, update_panel, update_targets, pivot_pairs, pivot_diagonal, pivot_coupling):
    sides = right_side[0, 0]
    inverse = factor_inverse[0, 0]
    update = update_panel[0, 0]
    plane = ("x", "y1", "y0")
    pair = ("x", "y0")

    packed = jnp.broadcast_to(sides[None], (4, *sides.shape))
    first = exchange(packed, ("x",))
    factors = pivot_factors(pivot_pairs[0], pivot_diagonal[0], pivot_coupling[0])
    partner_factors = with_partner(factors)
    inverse_after, update_after, _ = lax.optimization_barrier((inverse, update, packed))
    partner_inverse = with_partner(inverse_after)
    partner_update = with_partner(update_after)
    (weights0,) = prepared([inverse], [(0, 512, None)], packed)
    (updates0,) = prepared([update], [(0, 256, None)], packed)
    first, partner_factors, tables = lax.optimization_barrier(
        (first, partner_factors, sibling_tables(update_targets))
    )

    sent, weighted0, keep, give = level_zero_forward(first, weights0, updates0, factors)
    received = exchange(sent, ("c", "x"))
    give = with_partner(give)
    sides1, near = gathered_sides(keep, give)
    beyond = across(near, "y0")
    (weights1,) = prepared([inverse, partner_inverse], [(512, 1024, 512)], sent, pltpu.VMEM)
    (updates1,) = prepared([update, partner_update], [(256, 512, None)], sent)
    sent, weighted1 = forward(1, received, [sides1], tables, weights1, updates1, factors, partner_factors)
    sent, beyond = lax.optimization_barrier((sent, beyond))
    weights2, weights3 = prepared([inverse, partner_inverse], [(1536, 2048, 512), (3584, 4096, 512)], sent)
    (updates2,) = prepared([update, partner_update], [(768, 1024, None)], sent)
    received = exchange(sent, pair)
    near3, _ = lax.optimization_barrier((jnp.stack([near[:, :, PIVOTS:], beyond[:, :, PIVOTS:]]), sent))
    beyond3 = across(near3, "y1")
    sent, weighted2 = forward(2, received, [near, beyond], tables, weights2, updates2, factors, partner_factors)
    received = exchange(summed_copies(exchange(sent, pair), 16), plane)
    sent, kept3, other3 = forward(3, received, [near3, beyond3], tables, weights3, None, factors, partner_factors)
    other3 = across(other3, "y1")
    received = exchange(summed_copies(exchange(sent, plane), 8), pair)
    sent, kept, other = backward(2, received, weighted2, tables, weights2, updates2, [kept3, other3])
    other = across(other, "y0")
    received = exchange(sent, pair)
    sent, nearest = backward(1, received, weighted1, tables, weights1, updates1, [])
    received = exchange(sent, ("x", "c"))
    keep, give = upper_answers(nearest, kept, other)
    sent = level_zero_backward(received, weighted0, weights0, updates0, keep, with_partner(give))
    return summed(exchange(sent, ("x",)))[None, None]


def solution(mesh):
    grid = np.array(mesh.devices).reshape(4, 2, 2, 2, 4)
    fine = Mesh(grid, AXES)
    leaf = ("z", "y1", "y0", "c")
    in_specs = (
        P(leaf, "x", None, None),
        P(leaf, "x", None, None),
        P(leaf, "x", None, None),
        P(leaf, None),
        P(leaf, "x", None),
        P(leaf, "x", None),
        P(leaf, "x", None),
    )
    out_specs = P(leaf, "x", None, None)

    return jax.shard_map(per_device, mesh=fine, in_specs=in_specs, out_specs=out_specs, check_vma=False)
```

```python
import jax
import jax.numpy as jnp
import numpy as np
from jax import lax
from jax.experimental import pallas as pl
from jax.experimental.pallas import tpu as pltpu
from jax.sharding import Mesh, PartitionSpec as P


BLOCK = 128
PIVOTS = 128
SIDES = 96
HALF = SIDES // 2
AXES = ("z", "y1", "y0", "c", "x")

exact_mode = lax.Precision.HIGHEST


def parts(value):
    high = value.astype(jnp.bfloat16)
    return high, (value - high.astype(jnp.float32)).astype(jnp.bfloat16)


def product(left, high, low, side):
    left_high, left_low = parts(left)
    dims = (((1,), (side,)), ((), ()))

    def dot(a, b):
        return lax.dot_general(a, b, dims, preferred_element_type=jnp.float32)

    both = dot(jnp.concatenate([left_high, left_low], 0), high)
    rows = left.shape[0]
    return both[:rows] + (dot(left_high, low) + both[rows:])


def dot_full(left, right):
    return lax.dot_general(
        left, right, (((1,), (0,)), ((), ())), precision=exact_mode, preferred_element_type=jnp.float32
    )


def exchange(value, axes):
    return lax.all_to_all(value, axes, 0, 0, tiled=True)


def with_partner(value):
    return lax.ppermute(value, "c", [(0, 1), (1, 0)])


def across(value, axis):
    return lax.ppermute(value, axis, [(0, 1), (1, 0)])


def block_at(index, size=BLOCK):
    return pl.ds(pl.multiple_of(index * size, size), size)


WHOLE = pl.BlockSpec(memory_space=pltpu.VMEM)
SCALARS = pl.BlockSpec(memory_space=pltpu.SMEM)
FAR = pl.BlockSpec(memory_space=pltpu.HBM)


def far(value):
    return pltpu.with_memory_space_constraint(value, pltpu.HBM)


def close(value):
    return pltpu.with_memory_space_constraint(value, pltpu.VMEM)


def call(body, out_shapes, operands, specs, scratch=(), limit=20, spaces=None):
    return pl.pallas_call(
        body,
        in_specs=specs,
        out_specs=[FAR if k == "H" else WHOLE for k in spaces or "-" * len(out_shapes)],
        out_shape=[
            {"H": pltpu.HBM, "h": pltpu.HBM, "v": pltpu.VMEM, "-": jax.ShapeDtypeStruct}[k](s, jnp.float32)
            for s, k in zip(out_shapes, spaces or "-" * len(out_shapes))
        ],
        scratch_shapes=list(scratch),
        compiler_params=pltpu.CompilerParams(vmem_limit_bytes=limit * 1024 * 1024),
    )(*operands)


def prepared(pair, spans, after):
    def body(*refs):
        sources = refs[: len(pair)]
        outs = refs[len(pair) + 1 :][: len(spans)]
        buffers = refs[len(pair) + 1 + len(spans) : -1]
        semaphores = refs[-1]
        moves = []
        for i, (start, width, _) in enumerate(spans):
            for side, source in enumerate(sources):
                move = pltpu.make_async_copy(
                    source.at[:, pl.ds(start, width)],
                    buffers[i].at[pl.ds(side * PIVOTS, PIVOTS), :],
                    semaphores.at[i, side],
                )
                move.start()
                moves.append((i, side, move))
        for i, side, move in moves:
            move.wait()
            rows = slice(side * PIVOTS, (side + 1) * PIVOTS)
            _, width, step = spans[i]
            for k, at in enumerate(range(0, width, step or width)):
                high, low = parts(buffers[i][rows, at : at + (step or width)])
                place = outs[i].at[k] if step else outs[i]
                place[0, rows] = high
                place[1, rows] = low

    count = len(pair) * PIVOTS
    shapes = [
        pltpu.HBM((width // step, 2, count, step), jnp.bfloat16) if step else pltpu.VMEM((2, count, width), jnp.bfloat16)
        for _, width, step in spans
    ]
    return pl.pallas_call(
        body,
        in_specs=[FAR] * (len(pair) + 1),
        out_specs=[WHOLE] * len(spans),
        out_shape=shapes,
        scratch_shapes=[pltpu.VMEM((count, width), jnp.float32) for _, width, _ in spans]
        + [pltpu.SemaphoreType.DMA((len(spans), len(pair)))],
        compiler_params=pltpu.CompilerParams(vmem_limit_bytes=28 * 1024 * 1024),
    )(*map(far, pair), far(after))


def pivot_apply(solved, own, swapped):
    lane = lax.broadcasted_iota(jnp.int32, solved.shape, 1)
    width = solved.shape[1]
    beside = jnp.where(lane % 2 == 0, pltpu.roll(solved, width - 1, 1), pltpu.roll(solved, 1, 1))
    return own * solved + swapped * beside


def pivot_factors(kinds, diagonal, coupling):
    def body(kinds_ref, diagonal_ref, coupling_ref, out_ref):
        width = diagonal_ref.shape[1]
        row = lax.broadcasted_iota(jnp.int32, (width // 2, width), 0)
        col = lax.broadcasted_iota(jnp.int32, (width // 2, width), 1)
        widen = (col // 2 == row).astype(jnp.float32)
        pair = jnp.concatenate(
            [kinds_ref[...].astype(jnp.float32), coupling_ref[...], jnp.zeros((6, width // 2), jnp.float32)], 0
        )
        wide = dot_full(pair, widen)
        is_pair = wide[0:1] > 0.5
        couple = wide[1:2]
        own = jnp.broadcast_to(diagonal_ref[...], (8, width))
        lane = lax.broadcasted_iota(jnp.int32, (8, width), 1)
        other = jnp.where(lane % 2 == 0, pltpu.roll(own, width - 1, 1), pltpu.roll(own, 1, 1))[0:1]
        own = own[0:1]
        determinant = own * other - couple * couple
        out_ref[0:1, :] = jnp.where(is_pair, other / determinant, 1.0 / own)
        out_ref[1:2, :] = jnp.where(is_pair, -couple / determinant, 0.0)

    operands = [far(kinds), far(diagonal), far(coupling)]
    return call(body, [(2, diagonal.shape[1])], operands, [WHOLE] * 3, spaces="v")[0]


def gathered_sides(own, other):
    def body(own_ref, other_ref, one_ref, near_ref):
        c = lax.axis_index("c")
        for rows, source in ((c, own_ref), (1 - c, other_ref)):
            place = pl.ds(pl.multiple_of(rows * HALF, 8), HALF)
            for x in range(4):
                one_ref[x, place] = source[x, :, :PIVOTS]
                near_ref[x, place] = source[x, :, PIVOTS:]

    return call(body, [(4, SIDES, PIVOTS), (4, SIDES, 256)], [far(own), other], [WHOLE] * 2, spaces="hh")


def upper_answers(nearest, kept, other):
    def body(nearest_ref, kept_ref, other_ref, own_ref, give_ref):
        c = lax.axis_index("c")
        for core, out in ((c, own_ref), (1 - c, give_ref)):
            at = block_at(core)
            for x in range(4):
                out[x, :, :PIVOTS] = nearest_ref[x, :, at]
                for i in range(2):
                    piece = kept_ref[i, x, :, at] + other_ref[i, x, :, at]
                    out[x, :, (1 + i) * PIVOTS : (2 + i) * PIVOTS] = piece

    return call(body, [(4, HALF, 384)] * 2, [far(nearest), far(kept), other], [WHOLE] * 3, spaces="hh")


class Moves:
    def __init__(self, semaphores):
        self.semaphores, self.started = semaphores, []

    def start(self, source, target):
        move = pltpu.make_async_copy(source, target, self.semaphores.at[len(self.started)])
        move.start()
        self.started.append(move)
        return move

    def chunks(self, source, target):
        return [self.start(source.at[k], target.at[k]) for k in range(source.shape[0])]


def finish(moves):
    for move in moves:
        move.wait()


def level_zero_forward(first, weights, updates, factors):
    def body(first_ref, weights_ref, updates_ref, factors_ref, *refs):
        sent_ref, weighted_ref, keep_ref, give_ref, part_ref, own_ref, semaphores = refs
        moves = Moves(semaphores)
        core = lax.axis_index("c")
        leaving = []
        for half, out in ((core, keep_ref), (1 - core, give_ref)):
            rows = pl.ds(pl.multiple_of(half * HALF, 8), HALF)
            leaving.append(moves.start(first_ref.at[:, rows, pl.ds(PIVOTS, 3 * PIVOTS)], out))
        gathered = jnp.concatenate([first_ref[q, :, :PIVOTS] for q in range(4)], 1)
        solved = product(gathered, weights_ref[0], weights_ref[1], 1)
        part_ref[...] = product(solved, updates_ref[0], updates_ref[1], 0)
        for c in range(2):
            for x in range(4):
                leaving.append(moves.start(part_ref.at[pl.ds(c * HALF, HALF)], sent_ref.at[c * 4 + x]))
        own_ref[...] = pivot_apply(solved, factors_ref[0:1, :PIVOTS], factors_ref[1:2, :PIVOTS])
        leaving.append(moves.start(own_ref, weighted_ref))
        finish(leaving)

    return call(
        body,
        [(8, HALF, 256), (SIDES, PIVOTS), (4, HALF, 384), (4, HALF, 384)],
        [close(first), close(weights), close(updates), close(factors)],
        [WHOLE] * 4,
        [
            pltpu.VMEM((SIDES, 256), jnp.float32),
            pltpu.VMEM((SIDES, PIVOTS), jnp.float32),
            pltpu.SemaphoreType.DMA((16,)),
        ],
        spaces="HHHH",
    )


def child_block(level, tables, child, k):
    def entry(table, at):
        return tables[0, table * 14 + at]

    c = lax.axis_index("c")
    if level == 1:
        return jnp.where(c == child, entry(0, k), entry(2, k))
    if level == 2:
        sibling = jnp.where(c == 0, entry(1, 2 + k), entry(3, 2 + k))
        return jnp.where(lax.axis_index("y0") == child, entry(0, 2 + k), sibling)
    sibling = jnp.where(c == 0, entry(3, 6 + k), entry(1, 6 + k))
    return jnp.where(lax.axis_index("y1") == child, entry(0, 6 + k), sibling)


def both_factors(level, factors, beside):
    at = slice(level * PIVOTS, (level + 1) * PIVOTS)
    return [jnp.concatenate([factors[i : i + 1, at], beside[i : i + 1, at]], 1) for i in range(2)]


def forward(level, received, sides, tables, weights, updates, factors, partner_factors):
    width = 1 << level
    span = 4 * PIVOTS * width
    chunks = span // 512
    update_len = 2 * PIVOTS * width if level < 3 else 0
    blocks = (2, 4, 8)[level - 1]
    n_sides = len(sides)
    n_updates = 1 if level < 3 else 0
    n_outs = (2, 2, 3)[level - 1]

    def body(*refs):
        refs = list(refs)

        def take(count):
            taken, refs[:] = refs[:count], refs[count:]
            return taken

        (tables_refs,) = take(1)
        received_ref, factors_ref, beside_ref = take(3)
        updates_ref = take(n_updates)
        sides_refs = take(n_sides)
        (weights_far,) = take(1)
        outs = take(n_outs)
        semaphores, b_ref, own_ref, weights_ref = take(4)
        moves = Moves(semaphores)
        y0, y1 = lax.axis_index("y0"), lax.axis_index("y1")

        arriving, leaving = [], []

        def bring(source, block):
            for c in range(2):
                arriving.append(moves.start(source.at[pl.ds(c * HALF, HALF)], b_ref.at[:, block_at(block * 2 + c)]))

        if level == 1:
            for x in range(4):
                bring(sides_refs[0].at[x], x)
        elif level == 2:
            for flip in range(2):
                for x in range(4):
                    bring(sides_refs[flip].at[x, :, pl.ds(0, PIVOTS)], x * 2 + (y0 ^ flip))
        else:
            for high in range(2):
                for flip in range(2):
                    for x in range(4):
                        bring(sides_refs[high].at[flip, x], x * 4 + (y1 ^ high) * 2 + (y0 ^ flip))
        columns = moves.chunks(weights_far, weights_ref)
        if level < 3:
            part_ref = refs[0]
        totals = [None, None]
        for child in range(2):
            if level == 1:
                totals[child] = sum(received_ref[child * 4 + x] for x in range(4))
            elif level == 2:
                totals[child] = sum(received_ref[x * 2 + child] for x in range(4))
        finish(arriving)
        for child in range(2):
            for k in range(blocks):
                if level < 3:
                    piece = totals[child][:, k * BLOCK : (k + 1) * BLOCK]
                else:
                    piece = received_ref[(k // 2) * 4 + child * 2 + k % 2]
                where = block_at(child_block(level, tables_refs, child, k))
                b_ref[:, where] = b_ref[:, where] - piece
        solved = jnp.zeros((HALF, 2 * PIVOTS), jnp.float32)
        for k in range(chunks):
            columns[k].wait()
            at = slice(k * 512, (k + 1) * 512)
            solved += product(b_ref[:, at], weights_ref[k, 0], weights_ref[k, 1], 1)
        weighted = pivot_apply(solved, *both_factors(level, factors_ref, beside_ref))
        if level < 3:
            own_ref[...] = weighted
            leaving.append(moves.start(own_ref, outs[1]))
            for k in range(update_len // 256):
                at = slice(k * 256, (k + 1) * 256)
                part_ref[:, at] = product(solved, updates_ref[0][0, :, at], updates_ref[0][1, :, at], 0)
            for i in range(8):
                source = part_ref if level == 1 else part_ref.at[:, pl.ds(i * BLOCK, BLOCK)]
                leaving.append(moves.start(source, outs[0].at[i]))
        else:
            sent_ref, keep_ref, beyond_ref = outs
            for k in range(chunks):
                at = slice(k * 512, (k + 1) * 512)
                b_ref[:, at] = product(weighted, weights_ref[k, 0], weights_ref[k, 1], 0)
            for child in range(2):
                for k in range(8):
                    where = block_at(child_block(3, tables_refs, child, k))
                    leaving.append(
                        moves.start(b_ref.at[:, where], sent_ref.at[(k // 2) * 4 + child * 2 + k % 2])
                    )
            for out, bit in ((beyond_ref, 1 - y1), (keep_ref, y1)):
                for x in range(4):
                    for low in range(2):
                        where = block_at(x * 4 + bit * 2 + low, 256)
                        leaving.append(moves.start(b_ref.at[:, where], out.at[x, low]))
        finish(leaving)

    outs = {
        1: [(8, HALF, 512), (HALF, 256)],
        2: [(8, HALF, BLOCK), (HALF, 256)],
        3: [(16, HALF, BLOCK), (4, 2, HALF, 256), (4, 2, HALF, 256)],
    }[level]
    operands = [far(tables), received, close(factors), close(partner_factors)]
    operands += [close(updates)] if level < 3 else []
    n_close = len(operands) - 1
    operands += map(far, [*sides, weights])
    specs = [SCALARS] + [WHOLE] * n_close + [FAR] * (n_sides + 1)
    scratch = [
        pltpu.SemaphoreType.DMA((80,)),
        pltpu.VMEM((HALF, span), jnp.float32),
        pltpu.VMEM((HALF, 256), jnp.float32),
        pltpu.VMEM((chunks, 2, 256, 512), jnp.bfloat16),
    ]
    if level < 3:
        scratch.append(pltpu.VMEM((HALF, update_len), jnp.float32))
    return call(body, outs, operands, specs, scratch, spaces="H" * n_outs)


def backward(level, received, weighted, tables, weights, updates, answers):
    width = 1 << level
    span = 4 * PIVOTS * width
    chunks = span // 512
    update_len = 2 * PIVOTS * width
    blocks = (2, 4)[level - 1]
    n_answers = len(answers)
    n_outs = (2, 3)[level - 1]

    def body(*refs):
        refs = list(refs)

        def take(count):
            taken, refs[:] = refs[:count], refs[count:]
            return taken

        (tables_refs,) = take(1)
        received_ref, updates_ref = take(2)
        weighted_far, weights_far = take(2)
        answers_far = take(n_answers)
        outs = take(n_outs)
        semaphores, x_ref, weighted_ref, weights_ref, pieces_ref = take(5)
        moves = Moves(semaphores)
        arriving = moves.start(weighted_far, weighted_ref)
        columns = moves.chunks(weights_far, weights_ref)
        leaving = []
        if level == 2:
            own_ref, other_ref, sums_ref = refs
            both = [moves.start(answers_far[0], own_ref), moves.start(answers_far[1], other_ref)]
        if level == 1:
            total = sum(received_ref[i] for i in range(8))
        arriving.wait()
        target = weighted_ref[...]
        for k in range(update_len // 256):
            at = slice(k * 256, (k + 1) * 256)
            if level == 1:
                chosen = total[:, at]
            else:
                chosen = jnp.concatenate([received_ref[2 * k], received_ref[2 * k + 1]], 1)
            target -= product(chosen, updates_ref[0, :, at], updates_ref[1, :, at], 1)
        for k in range(chunks):
            columns[k].wait()
            at = slice(k * 512, (k + 1) * 512)
            x_ref[:, at] = product(target, weights_ref[k, 0], weights_ref[k, 1], 0)
        for child in range(2):
            for k in range(blocks):
                where = block_at(child_block(level, tables_refs, child, k))
                at = slice(k * BLOCK, (k + 1) * BLOCK)
                pieces_ref[child, :, at] = x_ref[:, where]
            for x in range(4):
                leaving.append(moves.start(pieces_ref.at[child], outs[0].at[x * 2 + child]))
        if level == 1:
            for x in range(4):
                leaving.append(moves.start(x_ref.at[:, pl.ds(x * 256, 256)], outs[1].at[x]))
        else:
            y0 = lax.axis_index("y0")
            keep_out, beyond_out = outs[1:]
            for out, bit in ((beyond_out, 1 - y0), (keep_out, y0)):
                for x in range(4):
                    where = block_at(x * 2 + bit, 256)
                    leaving.append(moves.start(x_ref.at[:, where], out.at[0, x]))
            finish(both)
            for i, (out, bit) in enumerate(((beyond_out, 1 - y0), (keep_out, y0))):
                for x in range(4):
                    sums_ref[i, x] = own_ref[x, bit] + other_ref[x, bit]
                leaving.append(moves.start(sums_ref.at[i], out.at[1]))
        finish(leaving)

    outs = [(8, HALF, blocks * BLOCK)]
    outs += [(4, HALF, 256)] if level == 1 else [(2, 4, HALF, 256), (2, 4, HALF, 256)]
    operands = [far(tables), received, close(updates), *map(far, [weighted, weights, *answers])]
    specs = [SCALARS] + [WHOLE] * 2 + [FAR] * (len(operands) - 3)
    scratch = [
        pltpu.SemaphoreType.DMA((64,)),
        pltpu.VMEM((HALF, span), jnp.float32),
        pltpu.VMEM((HALF, 256), jnp.float32),
        pltpu.VMEM((chunks, 2, 256, 512), jnp.bfloat16),
        pltpu.VMEM((2, HALF, blocks * BLOCK), jnp.float32),
    ]
    if level == 2:
        scratch += [pltpu.VMEM((4, 2, HALF, 256), jnp.float32)] * 2 + [pltpu.VMEM((2, 4, HALF, 256), jnp.float32)]
    return call(body, outs, operands, specs, scratch, spaces="H" * n_outs)


def level_zero_backward(received, weighted, weights, updates, own, other):
    def body(received_ref, weighted_ref, own_ref, other_ref, weights_ref, updates_ref, sent_ref):
        core = lax.axis_index("c")
        for half, source in ((core, own_ref), (1 - core, other_ref)):
            place = pl.ds(pl.multiple_of(half * HALF, 8), HALF)
            for x in range(4):
                sent_ref[x, place, PIVOTS:] = source[x]
        chosen = jnp.concatenate([sum(received_ref[x * 2 + c] for x in range(4)) for c in range(2)], 0)
        target = weighted_ref[...] - product(chosen, updates_ref[0], updates_ref[1], 1)
        part = product(target, weights_ref[0], weights_ref[1], 0)
        for q in range(4):
            sent_ref[q, :, :PIVOTS] = part[:, q * PIVOTS : (q + 1) * PIVOTS]

    return call(
        body,
        [(4, SIDES, 512)],
        [received, far(weighted), far(own), other, close(weights), close(updates)],
        [WHOLE] * 6,
        spaces="v",
    )[0]


def summed(received):
    def body(received_ref, out_ref):
        out_ref[...] = (received_ref[0] + received_ref[1]) + (received_ref[2] + received_ref[3])

    return call(body, [(SIDES, 512)], [received], [WHOLE])[0]


def summed_copies(received, count):
    total = jnp.sum(received, 0)
    return jnp.broadcast_to(total[None], (count, *total.shape))


def sibling_tables(targets):
    pairs = []
    for y1 in range(2):
        for y0 in range(2):
            here = y1 * 4 + y0 * 2
            pairs.append((here, y1 * 4 + (1 - y0) * 2))
            pairs.append((here + 1, (1 - y1) * 4 + y0 * 2 + 1))
    side = lax.ppermute(targets, ("y1", "y0", "c"), pairs)
    return jnp.concatenate([targets, side, with_partner(targets), with_partner(side)], 1)


def per_device(right_side, factor_inverse, update_panel, update_targets, pivot_pairs, pivot_diagonal, pivot_coupling):
    sides = right_side[0, 0]
    inverse = factor_inverse[0, 0]
    update = update_panel[0, 0]
    plane = ("x", "y1", "y0")
    pair = ("x", "y0")

    packed = jnp.broadcast_to(sides[None], (4, *sides.shape))
    first = exchange(packed, ("x",))
    factors = pivot_factors(pivot_pairs[0], pivot_diagonal[0], pivot_coupling[0])
    partner_factors = with_partner(factors)
    inverse_after, update_after, _ = lax.optimization_barrier((inverse, update, packed))
    partner_inverse = with_partner(inverse_after)
    partner_update = with_partner(update_after)
    (weights0,) = prepared([inverse], [(0, 512, None)], packed)
    (updates0,) = prepared([update], [(0, 256, None)], packed)
    first, partner_factors, tables = lax.optimization_barrier(
        (first, partner_factors, sibling_tables(update_targets))
    )

    sent, weighted0, keep, give = level_zero_forward(first, weights0, updates0, factors)
    received = exchange(sent, ("c", "x"))
    give = with_partner(give)
    sides1, near = gathered_sides(keep, give)
    beyond = across(near, "y0")
    (weights1,) = prepared([inverse, partner_inverse], [(512, 1024, 512)], sent)
    (updates1,) = prepared([update, partner_update], [(256, 512, None)], packed)
    sent, weighted1 = forward(1, received, [sides1], tables, weights1, updates1, factors, partner_factors)
    sent, beyond = lax.optimization_barrier((sent, beyond))
    weights2, weights3 = prepared([inverse, partner_inverse], [(1536, 2048, 512), (3584, 4096, 512)], sent)
    (updates2,) = prepared([update, partner_update], [(768, 1024, None)], sent)
    received = exchange(sent, pair)
    near3, _ = lax.optimization_barrier((jnp.stack([near[:, :, PIVOTS:], beyond[:, :, PIVOTS:]]), sent))
    beyond3 = across(near3, "y1")
    sent, weighted2 = forward(2, received, [near, beyond], tables, weights2, updates2, factors, partner_factors)
    received = exchange(summed_copies(exchange(sent, pair), 16), plane)
    sent, kept3, other3 = forward(3, received, [near3, beyond3], tables, weights3, None, factors, partner_factors)
    other3 = across(other3, "y1")
    received = exchange(summed_copies(exchange(sent, plane), 8), pair)
    sent, kept, other = backward(2, received, weighted2, tables, weights2, updates2, [kept3, other3])
    other = across(other, "y0")
    received = exchange(sent, pair)
    sent, nearest = backward(1, received, weighted1, tables, weights1, updates1, [])
    received = exchange(sent, ("x", "c"))
    keep, give = upper_answers(nearest, kept, other)
    sent = level_zero_backward(received, weighted0, weights0, updates0, keep, with_partner(give))
    return summed(exchange(sent, ("x",)))[None, None]


def solution(mesh):
    grid = np.array(mesh.devices).reshape(4, 2, 2, 2, 4)
    fine = Mesh(grid, AXES)
    leaf = ("z", "y1", "y0", "c")
    in_specs = (
        P(leaf, "x", None, None),
        P(leaf, "x", None, None),
        P(leaf, "x", None, None),
        P(leaf, None),
        P(leaf, "x", None),
        P(leaf, "x", None),
        P(leaf, "x", None),
    )
    out_specs = P(leaf, "x", None, None)

    return jax.shard_map(per_device, mesh=fine, in_specs=in_specs, out_specs=out_specs, check_vma=False)
```
